8 devices in a mesh: dp: 2 (over z, y), sp: 4 (over x, core).
Axes of the slice: x: 2, y: 2, z: 1, core: 2. Of those that a mesh axis runs over, the one named last changes fastest.
Arguments:
- x_rows: bfloat16 [16384, 384], P(('dp', 'sp')), parts along dimension 0
- dy_rows: bfloat16 [16384, 384], P(('dp', 'sp')), parts along dimension 0
- ln_gamma: float32 [384], replicated
- ln_beta: float32 [384], replicated
- w_qkv: bfloat16 [384, 1152], replicated
- w_out: bfloat16 [384, 384], replicated
- temperature: float32 [8], replicated
Outputs:
- output 1: bfloat16 [16384, 384], P(('dp', 'sp')), parts along dimension 0
- output 2: bfloat16 [16384, 384], P(('dp', 'sp')), parts along dimension 0
- output 3: bfloat16 [768, 1152], P(('dp', 'sp')), parts along dimension 0
- output 4: bfloat16 [768, 384], P(('dp', 'sp')), parts along dimension 0
- output 5: float32 [768], P('dp'), parts along dimension 0
- output 6: float32 [768], P('dp'), parts along dimension 0
- output 7: float32 [16], P('dp'), parts along dimension 0
There are 2 independent parts. The reference program is written for one: setup_inputs(seed, part) draws one part's arguments, and reference() takes and returns one part's arrays. A program takes and returns all parts, laid end to end along the dimension named above; an argument that names none is the same for every part.
All inputs are finite; a program needn't handle non-finite values.
Results may differ from the reference program's by a relative error of at most 0.0120056.
Values are sent between devices in bfloat16 or wider.
A program may use at most 1 GiB of HBM per device.

```python
import jax
import jax.numpy as jnp
from jax import lax

TOKENS = 8192
WIDTH = 384
N_HEADS = 8
SEGMENTS = 8
HEAD_DIM = WIDTH // N_HEADS
LN_EPS = 1e-6


def setup_inputs(seed: int = 0, part: int = 0) -> dict:
    part_keys = jax.random.split(jax.random.fold_in(jax.random.key(seed), part), 4)
    shared_keys = jax.random.split(jax.random.key(seed + 1), 5)
    seg_rows = TOKENS // SEGMENTS
    x_means = jnp.repeat(jax.random.normal(part_keys[0], (SEGMENTS, WIDTH), jnp.float32), seg_rows, axis=0)
    x_rows = jax.random.normal(part_keys[1], (TOKENS, WIDTH), jnp.float32) + 2.0 * x_means
    dy_means = jnp.repeat(jax.random.normal(part_keys[2], (SEGMENTS, WIDTH), jnp.float32), seg_rows, axis=0)
    dy_rows = 0.7 * jax.random.normal(part_keys[3], (TOKENS, WIDTH), jnp.float32) + dy_means
    fan_scale = WIDTH ** -0.5
    ln_gamma = 1.0 + 0.3 * jax.random.normal(shared_keys[0], (WIDTH,), jnp.float32)
    ln_beta = 0.3 * jax.random.normal(shared_keys[1], (WIDTH,), jnp.float32)
    w_qkv = fan_scale * jax.random.normal(shared_keys[2], (WIDTH, 3 * WIDTH), jnp.float32)
    w_out = 1.5 * fan_scale * jax.random.normal(shared_keys[3], (WIDTH, WIDTH), jnp.float32)
    temperature = jax.random.uniform(shared_keys[4], (N_HEADS,), jnp.float32, 3.0, 8.0)
    return {'x_rows': x_rows.astype(jnp.bfloat16), 'dy_rows': dy_rows.astype(jnp.bfloat16), 'ln_gamma': ln_gamma, 'ln_beta': ln_beta, 'w_qkv': w_qkv.astype(jnp.bfloat16), 'w_out': w_out.astype(jnp.bfloat16), 'temperature': temperature}


def xca_forward(x_rows, ln_gamma, ln_beta, w_qkv, w_out, temperature):
    x_f32 = x_rows.astype(jnp.float32)
    row_mean = jnp.mean(x_f32, axis=-1, keepdims=True)
    centered = x_f32 - row_mean
    row_var = jnp.mean(centered * centered, axis=-1, keepdims=True)
    normed = (centered * lax.rsqrt(row_var + LN_EPS) * ln_gamma + ln_beta).astype(jnp.bfloat16)
    qkv_all = jnp.dot(normed, w_qkv, preferred_element_type=jnp.float32).astype(jnp.bfloat16)
    qkv_heads = qkv_all.reshape(TOKENS, 3, N_HEADS, HEAD_DIM).astype(jnp.float32)
    query_h = qkv_heads[:, 0]
    key_h = qkv_heads[:, 1]
    value_h = qkv_heads[:, 2]
    gram = jnp.einsum('nhi,nhj->hij', query_h, key_h)
    q_sq = jnp.sum(query_h * query_h, axis=0)
    k_sq = jnp.sum(key_h * key_h, axis=0)
    scores = temperature[:, None, None] * gram * lax.rsqrt(q_sq)[:, :, None] * lax.rsqrt(k_sq)[:, None, :]
    attn = jax.nn.softmax(scores, axis=-1).astype(jnp.bfloat16)
    attn_out = jnp.einsum('nhj,hij->nhi', value_h, attn.astype(jnp.float32)).astype(jnp.bfloat16)
    proj = jnp.dot(attn_out.reshape(TOKENS, WIDTH), w_out, preferred_element_type=jnp.float32)
    return (x_f32 + proj).astype(jnp.bfloat16)


def reference(x_rows, dy_rows, ln_gamma, ln_beta, w_qkv, w_out, temperature):
    y_rows, backward = jax.vjp(xca_forward, x_rows, ln_gamma, ln_beta, w_qkv, w_out, temperature)
    dx_rows, d_gamma, d_beta, dw_qkv, dw_out, d_temp = backward(dy_rows)
    return (y_rows, dx_rows, dw_qkv, dw_out, d_gamma, d_beta, d_temp)
```

```python
import jax
import jax.numpy as jnp
from jax import lax
from jax.experimental import pallas as pl
from jax.experimental.pallas import tpu as pltpu
from jax.sharding import PartitionSpec as P

LN_EPS = 1e-6
F32, BF16 = jnp.float32, jnp.bfloat16
MESH = pl.DeviceIdType.MESH

C = 384
HEADS, HD = 8, 48
LANES = 128
TOK = 2048
RB = 512
NB = TOK // RB
SB = 64
OWN = C // 4
PK = 192
W0_HEADS = 5

NN = (((1,), (0,)), ((), ()))
NT = (((1,), (1,)), ((), ()))
TN = (((0,), (0,)), ((), ()))


def mm(a, b, dims=NN):
    return lax.dot_general(a, b, dims, preferred_element_type=F32)


def head_rel():
    lane = lax.broadcasted_iota(jnp.int32, (HD, LANES), 1)
    return [(lane - HD * h) & (LANES - 1) for h in range(HEADS)]


def seg_mask(rel, h, m):
    chan = rel + HD * h
    return (rel < HD) & (chan >= LANES * m) & (chan < LANES * (m + 1))


def head_window(h):
    if h < W0_HEADS:
        return 0, HD * h, (0, 1)
    return 1, HD * h - LANES, (1, 2)


def segs_of(h):
    return sorted({(HD * h) // LANES, (HD * h + HD - 1) // LANES})


def fold_windows(win_refs, out_ref):
    rels = head_rel()
    for p in range(HEADS // 2):
        acc = jnp.zeros((HD, LANES), F32)
        for h in (2 * p, 2 * p + 1):
            w, row, segs = head_window(h)
            for s, m in enumerate(segs):
                if m in segs_of(h):
                    block = win_refs[w][pl.ds(row, HD), pl.ds(LANES * s, LANES)]
                    acc = jnp.where(seg_mask(rels[h], h, m), block, acc)
        out_ref[pl.ds(HD * p, HD), :] = acc


def spread_head(value, rels, h, win_refs):
    w, row, segs = head_window(h)
    parts = []
    for m in segs:
        if m in segs_of(h):
            parts.append(jnp.where(seg_mask(rels[h], h, m), value, 0.0))
        else:
            parts.append(jnp.zeros((HD, LANES), F32))
    win_refs[w][pl.ds(row, HD), :] = jnp.concatenate(parts, axis=1).astype(BF16)


def window_mm(a, win_refs, dims):
    r0 = mm(a[:, :256], win_refs[0][...], dims)
    r1 = mm(a[:, 128:], win_refs[1][...], dims)
    return jnp.concatenate([r0[:, :128], r0[:, 128:] + r1[:, :128], r1[:, 128:]], axis=1)


def kernel(
    x_hbm, dy_hbm, g_hbm, b_hbm, wqkv_hbm, wo_hbm, tau_hbm,
    y, dx, dwqkv_ref, dwo_ref, dg_ref, db_ref, dt_ref,
    x, dy, g_ref, b_ref, wqkv, wo, tau_ref, u, ut, xhat, istd, q, k, v, do, o, ot, dqkv, du,
    g0, g1, sq, pg, rg1, sg, rg2, pa, ra1, sa, ra2,
    a0, a1, e0, e1, attn, score, qk_inv, gfull, dsq,
    wo_part, wv_part, wqk_part, wo_r1, wv_r1, wqk_r1, wo_s, wv_s, wqk_s, wo_r2, wv_r2, wqk_r2,
    dgb_all,
    in_sem, send_sem, recv_sem,
):
    me = lax.axis_index("sp")
    core = lax.rem(me, 2)
    chip = me // 2
    sib = me + 1 - 2 * core
    nbr = lax.rem(me + 2, 4)
    diag = lax.rem(sib + 2, 4)

    n_loads = [0]

    def load(src, dst):
        cp = pltpu.make_async_copy(src, dst, in_sem.at[n_loads[0]])
        n_loads[0] += 1
        cp.start()
        return cp

    def block(i):
        return pl.ds(i * RB, RB)

    ld_gb = [load(g_hbm, g_ref), load(b_hbm, b_ref)]
    ld_x = [load(x_hbm.at[block(0), :], x.at[block(0), :])]
    ld_wqk = load(wqkv_hbm.at[:, pl.ds(0, 2 * C)], wqkv.at[:, pl.ds(0, 2 * C)])
    ld_x += [load(x_hbm.at[block(i), :], x.at[block(i), :]) for i in range(1, NB)]
    ld_wv = load(wqkv_hbm.at[:, pl.ds(2 * C, C)], wqkv.at[:, pl.ds(2 * C, C)])
    ld_wo = load(wo_hbm, wo)
    ld_dy = load(dy_hbm, dy)
    ld_tau = load(tau_hbm, tau_ref)

    barrier = pltpu.get_barrier_semaphore()
    for peer in (sib, nbr, diag):
        pl.semaphore_signal(barrier, inc=1, device_id={"sp": peer}, device_id_type=MESH)

    n_sends = [0]

    def send(src, dst, peer):
        i = n_sends[0]
        n_sends[0] += 1
        cp = pltpu.make_async_remote_copy(
            src_ref=src, dst_ref=dst, send_sem=send_sem.at[i], recv_sem=recv_sem.at[i],
            device_id={"sp": peer}, device_id_type=MESH)
        cp.start()
        return cp

    def step_a(i):
        ld_x[i].wait()
        if i == 0:
            for cp in ld_gb:
                cp.wait()
        gamma = g_ref[...].reshape(1, C)
        beta = b_ref[...].reshape(1, C)
        for j in range(RB // SB):
            rows = pl.ds(i * RB + j * SB, SB)
            xf = x[rows, :].astype(F32)
            cen = xf - jnp.mean(xf, axis=-1, keepdims=True)
            inv = lax.rsqrt(jnp.mean(cen * cen, axis=-1, keepdims=True) + LN_EPS)
            xh = cen * inv
            xhat[rows, :] = xh
            istd[rows, :] = jnp.broadcast_to(inv, (SB, LANES))
            u[rows, :] = (xh * gamma + beta).astype(BF16)
        rows = block(i)
        if i == 0:
            ld_wqk.wait()
        q[rows, :] = mm(u[rows, :], wqkv[:, :C]).astype(BF16)
        k[rows, :] = mm(u[rows, :], wqkv[:, C : 2 * C]).astype(BF16)
        p0 = mm(q[rows, :256], k[rows, :256], TN)
        p1 = mm(q[rows, 128:], k[rows, 128:], TN)
        part = jnp.zeros((8, 2 * C), F32)
        for j in range(RB // SB):
            sub = pl.ds(i * RB + j * SB, SB)
            qkf = jnp.concatenate([q[sub, :], k[sub, :]], axis=1).astype(F32)
            part += jnp.sum((qkf * qkf).reshape(SB // 8, 8, 2 * C), axis=0)
        if i == 0:
            g0[...], g1[...], sq[...] = p0, p1, part
        else:
            g0[...] += p0
            g1[...] += p1
            sq[...] += part
        ut[:, rows] = u[rows, :].T

    with jax.named_scope("ln_qk"):
        for i in range(NB):
            step_a(i)
    with jax.named_scope("fold_g"):
        fold_windows((g0, g1), pg)
        sums = jnp.sum(sq[...], axis=0, keepdims=True)
        for m in range(6):
            pg[pl.ds(PK + m, 1), :] = sums[:, LANES * m : LANES * (m + 1)]
        pg[pl.ds(PK + 6, 2), :] = jnp.zeros((2, LANES), F32)
    with jax.named_scope("greet"):
        pl.semaphore_wait(barrier, 3)
    s_g1 = send(pg, rg1, sib)

    def step_b(i):
        rows = block(i)
        v[rows, :] = mm(u[rows, :], wqkv[:, 2 * C :]).astype(BF16)
        do[rows, :] = mm(dy[rows, :], wo[...], NT).astype(BF16)
        p0 = mm(do[rows, :256], v[rows, :256], TN)
        p1 = mm(do[rows, 128:], v[rows, 128:], TN)
        if i == 0:
            g0[...], g1[...] = p0, p1
        else:
            g0[...] += p0
            g1[...] += p1

    with jax.named_scope("v_do_1"):
        ld_wv.wait()
        ld_wo.wait()
        ld_dy.wait()
        ld_tau.wait()
        for i in range(NB // 2):
            step_b(i)
    with jax.named_scope("sum_g"):
        s_g1.wait()
        sg[...] = pg[...] + rg1[...]
        s_g2 = send(sg, rg2, nbr)
    with jax.named_scope("v_do_2"):
        for i in range(NB // 2, NB):
            step_b(i)
    with jax.named_scope("fold_a"):
        fold_windows((g0, g1), pa)
        s_a1 = send(pa, ra1, sib)
    with jax.named_scope("sum_a"):
        s_a1.wait()
        sa[...] = pa[...] + ra1[...]
        s_a2 = send(sa, ra2, nbr)

    with jax.named_scope("wait_g"):
        s_g2.wait()
    rels = head_rel()
    row = lax.broadcasted_iota(jnp.int32, (HD, LANES), 0)
    with jax.named_scope("softmax"):
        gfull[...] = sg[...] + rg2[...]
        for ref in (a0, a1, e0, e1):
            ref[...] = jnp.zeros_like(ref)
        for h in range(HEADS):
            rel = rels[h]
            valid = rel < HD
            tau = tau_ref[h]
            s_q = jnp.zeros((HD, LANES), F32)
            s_k = jnp.ones((HD, LANES), F32)
            for m in segs_of(h):
                mask = seg_mask(rel, h, m)
                s_q = jnp.where(mask, gfull[pl.ds(PK + m, 1), :], s_q)
                s_k = jnp.where(mask, gfull[pl.ds(PK + 3 + m, 1), :], s_k)
            s_q = jnp.sum(jnp.where(rel == row, s_q, 0.0), axis=1, keepdims=True)
            inv = jnp.where(valid, lax.rsqrt(s_q) * lax.rsqrt(s_k), 0.0)
            gram = jnp.where(valid, gfull[pl.ds(HD * (h // 2), HD), :], 0.0)
            sc = tau * gram * inv
            top = jnp.max(jnp.where(valid, sc, -jnp.inf), axis=1, keepdims=True)
            ex = jnp.where(valid, jnp.exp(sc - top), 0.0)
            at = ex / jnp.sum(ex, axis=1, keepdims=True)
            hr = pl.ds(HD * h, HD)
            score[hr, :] = sc
            qk_inv[hr, :] = inv
            attn[hr, :] = at
            spread_head(at, rels, h, (a0, a1))

    far = pl.ds(pl.multiple_of(2 * OWN * (1 - chip), 16), 2 * OWN)
    near = pl.ds(pl.multiple_of(2 * OWN * chip, 16), 2 * OWN)
    theirs = pl.ds(pl.multiple_of(OWN * (1 - core), 8), OWN)
    mine = pl.ds(pl.multiple_of(OWN * core, 8), OWN)

    def part_rows(lhs_t, rows, rhs, part, r1, slot):
        part[slot] = mm(lhs_t[rows, :], rhs)
        return send(part.at[slot, theirs, :], r1.at[slot], sib)

    def cross(cp, part, r1, s, r2):
        cp.wait()
        s[...] = part[0, mine, :] + r1[0]
        return send(s, r2, nbr)

    with jax.named_scope("o"):
        for i in range(NB):
            rows = block(i)
            o[rows, :] = window_mm(v[rows, :], (a0, a1), NT).astype(BF16)
            ot[:, rows] = o[rows, :].T
    with jax.named_scope("dwo_far"):
        f_wo = part_rows(ot, far, dy[...], wo_part, wo_r1, 0)
    with jax.named_scope("dv"):
        for i in range(NB):
            rows = block(i)
            dqkv[rows, 2 * C :] = window_mm(do[rows, :], (a0, a1), NN).astype(BF16)
    with jax.named_scope("cross_wo"):
        x_wo = cross(f_wo, wo_part, wo_r1, wo_s, wo_r2)
    with jax.named_scope("dwv_far"):
        f_wv = part_rows(ut, far, dqkv[:, 2 * C :], wv_part, wv_r1, 0)

    with jax.named_scope("wait_a"):
        s_a2.wait()
    with jax.named_scope("softmax_bwd"):
        dsum = [jnp.zeros((1, LANES), F32) for _ in range(6)]
        lane = lax.broadcasted_iota(jnp.int32, (1, LANES), 1)
        d_tau = jnp.zeros((1, LANES), F32)
        for h in range(HEADS):
            rel = rels[h]
            valid = rel < HD
            hr = pl.ds(HD * h, HD)
            pr = pl.ds(HD * (h // 2), HD)
            at = attn[hr, :]
            d_at = jnp.where(valid, sa[pr, :] + ra2[pr, :], 0.0).astype(BF16).astype(F32)
            d_sc = at * (d_at - jnp.sum(d_at * at, axis=1, keepdims=True))
            d_sc_inv = d_sc * qk_inv[hr, :]
            d_tau_h = jnp.sum(d_sc_inv * jnp.where(valid, gfull[pr, :], 0.0), axis=0, keepdims=True)
            d_tau = jnp.where(lane == h, jnp.sum(d_tau_h, axis=1, keepdims=True), d_tau)
            spread_head(d_sc_inv * tau_ref[h], rels, h, (e0, e1))
            wt = d_sc * score[hr, :]
            over_q = jnp.sum(jnp.where(rel == row, jnp.sum(wt, axis=1, keepdims=True), 0.0), axis=0, keepdims=True)
            over_k = jnp.sum(wt, axis=0, keepdims=True)
            for m in segs_of(h):
                mask = seg_mask(rel, h, m)[:1]
                dsum[m] = jnp.where(mask, over_q, dsum[m])
                dsum[3 + m] = jnp.where(mask, over_k, dsum[3 + m])
        dt_ref[...] = d_tau[:, :HEADS].reshape(HEADS)
        for m in range(6):
            dsq[:, pl.ds(LANES * m, LANES)] = -dsum[m] / gfull[pl.ds(PK + m, 1), :]
    with jax.named_scope("cross_wv"):
        x_wv = cross(f_wv, wv_part, wv_r1, wv_s, wv_r2)

    with jax.named_scope("dqk"):
        for i in range(NB):
            rows = block(i)
            dqkv[rows, :C] = (
                window_mm(k[rows, :], (e0, e1), NT) + q[rows, :].astype(F32) * dsq[:, :C]).astype(BF16)
            dqkv[rows, C : 2 * C] = (
                window_mm(q[rows, :], (e0, e1), NN) + k[rows, :].astype(F32) * dsq[:, C:]).astype(BF16)
    with jax.named_scope("dwqk_far"):
        f_wqk = part_rows(ut, far, dqkv[:, : 2 * C], wqk_part, wqk_r1, 0)
    with jax.named_scope("near"):
        l_wo = part_rows(ot, near, dy[...], wo_part, wo_r1, 1)
        l_wv = part_rows(ut, near, dqkv[:, 2 * C :], wv_part, wv_r1, 1)
    with jax.named_scope("cross_wqk"):
        x_wqk = cross(f_wqk, wqk_part, wqk_r1, wqk_s, wqk_r2)
    with jax.named_scope("near_qk"):
        l_wqk = part_rows(ut, near, dqkv[:, : 2 * C], wqk_part, wqk_r1, 1)

    gamma = g_ref[...].reshape(1, C)
    dgam = jnp.zeros((8, C), F32)
    dbet = jnp.zeros((8, C), F32)
    with jax.named_scope("ln_bwd"):
        for i in range(NB):
            rows = block(i)
            du[rows, :] = mm(dqkv[rows, :], wqkv[...], NT).astype(BF16)
            for j in range(RB // SB):
                sub = pl.ds(i * RB + j * SB, SB)
                d = du[sub, :].astype(F32)
                xh = xhat[sub, :]
                dxh = d * xh
                dgam += jnp.sum(dxh.reshape(SB // 8, 8, C), axis=0)
                dbet += jnp.sum(d.reshape(SB // 8, 8, C), axis=0)
                dh = d * gamma
                m1 = jnp.mean(dh, axis=-1, keepdims=True)
                m2 = jnp.mean(dxh * gamma, axis=-1, keepdims=True)
                inv = istd[sub, :]
                term = dh - m1 - xh * m2
                dln = term * jnp.concatenate([inv, inv, inv], axis=1)
                dx[sub, :] = (dy[sub, :].astype(F32) + dln).astype(BF16)
        dgb_all[me] = jnp.concatenate(
            [jnp.sum(dgam, axis=0, keepdims=True), jnp.sum(dbet, axis=0, keepdims=True), jnp.zeros((6, C), F32)],
            axis=0)
    c_dgb = [send(dgb_all.at[me], dgb_all.at[me], peer) for peer in (sib, nbr, diag)]
    with jax.named_scope("y"):
        for i in range(NB):
            rows = block(i)
            y[rows, :] = (x[rows, :].astype(F32) + mm(o[rows, :], wo[...])).astype(BF16)

    with jax.named_scope("wait_wo"):
        l_wo.wait()
        x_wo.wait()
        dwo_ref[...] = (wo_part[1, mine, :] + wo_r1[1] + wo_r2[...]).astype(BF16)
    with jax.named_scope("wait_wv"):
        l_wv.wait()
        x_wv.wait()
        dwqkv_ref[:, 2 * C :] = (wv_part[1, mine, :] + wv_r1[1] + wv_r2[...]).astype(BF16)
    with jax.named_scope("wait_dgb"):
        for cp in c_dgb:
            cp.wait()
        total = dgb_all[0] + dgb_all[1] + dgb_all[2] + dgb_all[3]
        dg_ref[...] = total[0:1].reshape(C)
        db_ref[...] = total[1:2].reshape(C)
    with jax.named_scope("wait_wqk"):
        l_wqk.wait()
        x_wqk.wait()
        dwqkv_ref[:, : 2 * C] = (wqk_part[1, mine, :] + wqk_r1[1] + wqk_r2[...]).astype(BF16)


def write_out(*refs):
    ins, outs, sem = refs[:7], refs[7:14], refs[14]
    copies = [pltpu.make_async_copy(ins[i], outs[i], sem.at[i]) for i in range(7)]
    for cp in copies:
        cp.start()
    for cp in copies:
        cp.wait()


def xca_local(x_rows, dy_rows, ln_gamma, ln_beta, w_qkv, w_out, temperature):
    vm = pltpu.VMEM
    hbm_spec = pl.BlockSpec(memory_space=pltpu.HBM)
    vmem_spec = pl.BlockSpec(memory_space=pltpu.VMEM)
    results = (
        ((TOK, C), BF16), ((TOK, C), BF16), ((OWN, 3 * C), BF16), ((OWN, C), BF16),
        ((C,), F32), ((C,), F32), ((HEADS,), F32),
    )
    rows_bf = vm((TOK, C), BF16)
    cols_bf = vm((C, TOK), BF16)
    win_f = vm((256, 256), F32)
    win_b = vm((256, 256), BF16)
    pk_g = vm((PK + 8, LANES), F32)
    pk_a = vm((PK, LANES), F32)
    fold = vm((C, LANES), F32)
    scratch = [
        rows_bf, rows_bf, vm((C,), F32), vm((C,), F32), vm((C, 3 * C), BF16), vm((C, C), BF16),
        pltpu.SMEM((HEADS,), F32), rows_bf, cols_bf, vm((TOK, C), F32), vm((TOK, LANES), F32),
        rows_bf, rows_bf, rows_bf, rows_bf, rows_bf, cols_bf, vm((TOK, 3 * C), BF16), rows_bf,
        win_f, win_f, vm((8, 2 * C), F32), pk_g, pk_g, pk_g, pk_g, pk_a, pk_a, pk_a, pk_a,
        win_b, win_b, win_b, win_b, fold, fold, fold, pk_g, vm((1, 2 * C), F32),
        vm((2, 2 * OWN, C), F32), vm((2, 2 * OWN, C), F32), vm((2, 2 * OWN, 2 * C), F32),
        vm((2, OWN, C), F32), vm((2, OWN, C), F32), vm((2, OWN, 2 * C), F32),
        vm((OWN, C), F32), vm((OWN, C), F32), vm((OWN, 2 * C), F32),
        vm((OWN, C), F32), vm((OWN, C), F32), vm((OWN, 2 * C), F32),
        vm((4, 8, C), F32),
        pltpu.SemaphoreType.DMA((12,)),
        pltpu.SemaphoreType.DMA((16,)), pltpu.SemaphoreType.DMA((16,)),
    ]
    parts = pl.pallas_call(
        kernel,
        name="xca",
        out_shape=tuple(pltpu.VMEM(shape, dtype) for shape, dtype in results),
        in_specs=[hbm_spec] * 7,
        out_specs=[vmem_spec] * 7,
        scratch_shapes=scratch,
        compiler_params=pltpu.CompilerParams(
            collective_id=0, has_side_effects=True, vmem_limit_bytes=60 * 1024 * 1024),
    )(x_rows, dy_rows, ln_gamma, ln_beta, w_qkv, w_out, temperature)
    return pl.pallas_call(
        write_out,
        name="xca_out",
        out_shape=tuple(jax.ShapeDtypeStruct(shape, dtype) for shape, dtype in results),
        in_specs=[vmem_spec] * 7,
        out_specs=[hbm_spec] * 7,
        scratch_shapes=[pltpu.SemaphoreType.DMA((7,))],
        compiler_params=pltpu.CompilerParams(vmem_limit_bytes=1024 * 1024),
    )(*parts)


def solution(mesh):
    row_spec = P(('dp', 'sp'), None)
    full_mat = P(None, None)
    full_vec = P(None)
    part_vec = P('dp')
    return jax.shard_map(
        xca_local, mesh=mesh,
        in_specs=(row_spec, row_spec, full_vec, full_vec, full_mat, full_mat, full_vec),
        out_specs=(row_spec, row_spec, row_spec, row_spec, part_vec, part_vec, part_vec),
        check_vma=False)
```

```python
import jax
import jax.numpy as jnp
from jax import lax
from jax.experimental import pallas as pl
from jax.experimental.pallas import tpu as pltpu
from jax.sharding import PartitionSpec as P

LN_EPS = 1e-6
F32, BF16 = jnp.float32, jnp.bfloat16
MESH = pl.DeviceIdType.MESH

C = 384
HEADS, HD = 8, 48
LANES = 128
TOK = 2048
RB = 512
NB = TOK // RB
RA = 512
NA = TOK // RA
RV = 256
NV = TOK // RV
CUT = 3
PIECES = 4
SB = 64
OWN = C // 4
PK = 144
W0_HEADS = 5

NN = (((1,), (0,)), ((), ()))
NT = (((1,), (1,)), ((), ()))
TN = (((0,), (0,)), ((), ()))


def mm(a, b, dims=NN):
    return lax.dot_general(a, b, dims, preferred_element_type=F32)


def head_rel():
    lane = lax.broadcasted_iota(jnp.int32, (HD, LANES), 1)
    return [(lane - HD * h) & (LANES - 1) for h in range(HEADS)]


def seg_mask(rel, h, m):
    chan = rel + HD * h
    return (rel < HD) & (chan >= LANES * m) & (chan < LANES * (m + 1))


def head_window(h):
    if h < W0_HEADS:
        return 0, HD * h, (0, 1)
    return 1, HD * h - LANES, (1, 2)


def segs_of(h):
    return sorted({(HD * h) // LANES, (HD * h + HD - 1) // LANES})


def spare_lanes(g):
    lane = lax.broadcasted_iota(jnp.int32, (HD, LANES), 1)
    return (lane >= 96 - 32 * g) & (lane < 128 - 32 * g)


def fold_windows(win_refs, out_ref):
    rels = head_rel()

    def put(acc, h, where):
        w, row, segs = head_window(h)
        for s, m in enumerate(segs):
            if m in segs_of(h):
                block = win_refs[w][pl.ds(row, HD), pl.ds(LANES * s, LANES)]
                mask = seg_mask(rels[h], h, m)
                acc = jnp.where(mask if where is None else mask & where, block, acc)
        return acc

    for g in range(3):
        acc = put(put(jnp.zeros((HD, LANES), F32), 2 * g, None), 2 * g + 1, None)
        spare = spare_lanes(g)
        out_ref[pl.ds(HD * g, HD), :] = put(put(acc, 6, spare), 7, spare)


def packed_head(ref, h):
    if h < 6:
        return ref[pl.ds(HD * (h // 2), HD), :]
    lane = lax.broadcasted_iota(jnp.int32, (HD, LANES), 1)
    return jnp.where(lane >= 96, ref[pl.ds(0, HD), :], jnp.where(lane >= 64, ref[pl.ds(HD, HD), :], ref[pl.ds(2 * HD, HD), :]))


def spread_head(value, rels, h, win_refs):
    w, row, segs = head_window(h)
    parts = []
    for m in segs:
        if m in segs_of(h):
            parts.append(jnp.where(seg_mask(rels[h], h, m), value, 0.0))
        else:
            parts.append(jnp.zeros((HD, LANES), F32))
    win_refs[w][pl.ds(row, HD), :] = jnp.concatenate(parts, axis=1).astype(BF16)


def window_mm(a, win_refs, dims):
    r0 = mm(a[:, :256], win_refs[0][...], dims)
    r1 = mm(a[:, 128:], win_refs[1][...], dims)
    return jnp.concatenate([r0[:, :128], r0[:, 128:] + r1[:, :128], r1[:, 128:]], axis=1)


def kernel(
    x_hbm, dy_hbm, g_hbm, b_hbm, wqkv_hbm, wo_hbm, tau_hbm,
    y, dx, dwqkv_ref, dwo_ref, dg_ref, db_ref, dt_ref,
    x, dy, g_ref, b_ref, wqkv, wo, wot, tau_ref, u, ut, xhat, istd, q, k, v, do, o, ot, dqkv, du,
    g0, g1, sq, pg, rg1, sg, rg2, pa, ra1, sa, ra2,
    a0, a1, e0, e1, attn, score, qk_inv, gfull, dsq,
    wo_part, wv_part, wqk_part, wo_r1, wv_r1, wqk_r1, wo_s, wv_s, wqk_s, wo_r2, wv_r2, wqk_r2,
    dgb_all,
    in_sem, send_sem, recv_sem,
):
    me = lax.axis_index("sp")
    core = lax.rem(me, 2)
    chip = me // 2
    sib = me + 1 - 2 * core
    nbr = lax.rem(me + 2, 4)
    diag = lax.rem(sib + 2, 4)

    n_loads = [0]

    def load(src, dst):
        cp = pltpu.make_async_copy(src, dst, in_sem.at[n_loads[0]])
        n_loads[0] += 1
        cp.start()
        return cp

    def block(i):
        return pl.ds(i * RB, RB)

    ld_gb = [load(g_hbm, g_ref), load(b_hbm, b_ref)]
    ld_x = [load(x_hbm.at[pl.ds(0, RA), :], x.at[pl.ds(0, RA), :])]
    ld_wqk = load(wqkv_hbm.at[:, pl.ds(0, 2 * C)], wqkv.at[:, pl.ds(0, 2 * C)])
    ld_x += [load(x_hbm.at[pl.ds(i * RA, RA), :], x.at[pl.ds(i * RA, RA), :]) for i in range(1, NA)]
    ld_wo = load(wo_hbm, wo)
    ld_wv = load(wqkv_hbm.at[:, pl.ds(2 * C, C)], wqkv.at[:, pl.ds(2 * C, C)])
    ld_dy = load(dy_hbm, dy)
    ld_tau = load(tau_hbm, tau_ref)

    barrier = pltpu.get_barrier_semaphore()
    for peer in (sib, nbr, diag):
        pl.semaphore_signal(barrier, inc=1, device_id={"sp": peer}, device_id_type=MESH)

    n_sends = [0]

    def send(src, dst, peer):
        i = n_sends[0]
        n_sends[0] += 1
        cp = pltpu.make_async_remote_copy(
            src_ref=src, dst_ref=dst, send_sem=send_sem.at[i], recv_sem=recv_sem.at[i],
            device_id={"sp": peer}, device_id_type=MESH)
        cp.start()
        return cp

    def step_ln(i):
        gamma = g_ref[...].reshape(1, C)
        beta = b_ref[...].reshape(1, C)
        for j in range(RA // SB):
            rows = pl.ds(i * RA + j * SB, SB)
            xf = x[rows, :].astype(F32)
            cen = xf - jnp.mean(xf, axis=-1, keepdims=True)
            inv = lax.rsqrt(jnp.mean(cen * cen, axis=-1, keepdims=True) + LN_EPS)
            xh = cen * inv
            xhat[rows, :] = xh
            istd[rows, :] = jnp.broadcast_to(inv, (SB, LANES))
            u[rows, :] = (xh * gamma + beta).astype(BF16)

    def step_qk(i):
        rows = pl.ds(i * RA, RA)
        qk = mm(u[rows, :], wqkv[:, : 2 * C]).astype(BF16)
        q[rows, :] = qk[:, :C]
        k[rows, :] = qk[:, C:]

    def step_gram(i):
        rows = pl.ds(i * RA, RA)
        p0 = mm(q[rows, :256], k[rows, :256], TN)
        p1 = mm(q[rows, 128:], k[rows, 128:], TN)
        if i == 0:
            g0[...], g1[...] = p0, p1
        else:
            g0[...] += p0
            g1[...] += p1
        for r, c0 in ((q, 0), (k, C)):
            part = jnp.zeros((8, C), F32)
            for j in range(RA // SB):
                f = r[pl.ds(i * RA + j * SB, SB), :].astype(F32)
                part += jnp.sum((f * f).reshape(SB // 8, 8, C), axis=0)
            if i == 0:
                sq[:, pl.ds(c0, C)] = part
            else:
                sq[:, pl.ds(c0, C)] += part
        ut[:, rows] = u[rows, :].T

    with jax.named_scope("ln_0"):
        ld_x[0].wait()
        for cp in ld_gb:
            cp.wait()
        step_ln(0)
    ld_wqk.wait()
    for cp in ld_x[1:]:
        cp.wait()
    ld_wo.wait()
    with jax.named_scope("ln_qk"):
        wot[...] = wo[...].T
        for i in range(1, NA + 2):
            if i < NA:
                step_ln(i)
            if 1 <= i <= NA:
                step_qk(i - 1)
            if i >= 2:
                step_gram(i - 2)
    with jax.named_scope("fold_g"):
        fold_windows((g0, g1), pg)
        sums = jnp.sum(sq[...], axis=0, keepdims=True)
        for m in range(6):
            pg[pl.ds(PK + m, 1), :] = sums[:, LANES * m : LANES * (m + 1)]
        pg[pl.ds(PK + 6, 2), :] = jnp.zeros((2, LANES), F32)
    with jax.named_scope("greet"):
        pl.semaphore_wait(barrier, 3)
    s_g1 = send(pg, rg1, sib)

    def step_b(i):
        rows = pl.ds(i * RV, RV)
        v[rows, :] = mm(u[rows, :], wqkv[:, 2 * C :]).astype(BF16)
        do[rows, :] = mm(dy[rows, :], wot[...]).astype(BF16)

    def step_da(i):
        rows = pl.ds(i * RV, RV)
        p0 = mm(do[rows, :256], v[rows, :256], TN)
        p1 = mm(do[rows, 128:], v[rows, 128:], TN)
        if i == 0:
            g0[...], g1[...] = p0, p1
        else:
            g0[...] += p0
            g1[...] += p1

    with jax.named_scope("v_do_1"):
        ld_wv.wait()
        ld_dy.wait()
        ld_tau.wait()
        for i in range(CUT + 1):
            if i < CUT:
                step_b(i)
            if i >= 1:
                step_da(i - 1)
    with jax.named_scope("sum_g"):
        s_g1.wait()
        sg[...] = pg[...] + rg1[...]
        s_g2 = send(sg, rg2, nbr)
    with jax.named_scope("v_do_2"):
        for i in range(CUT, NV + 1):
            if i < NV:
                step_b(i)
            if i >= CUT + 1:
                step_da(i - 1)
    with jax.named_scope("fold_a"):
        fold_windows((g0, g1), pa)
        s_a1 = send(pa, ra1, sib)
    with jax.named_scope("sum_a"):
        s_a1.wait()
        sa[...] = pa[...] + ra1[...]
        s_a2 = send(sa, ra2, nbr)

    with jax.named_scope("wait_g"):
        s_g2.wait()
    rels = head_rel()
    row = lax.broadcasted_iota(jnp.int32, (HD, LANES), 0)
    with jax.named_scope("softmax"):
        gfull[...] = sg[...] + rg2[...]
        for ref in (a0, a1, e0, e1):
            ref[...] = jnp.zeros_like(ref)
        for h in range(HEADS):
            rel = rels[h]
            valid = rel < HD
            tau = tau_ref[h]
            s_q = jnp.zeros((HD, LANES), F32)
            s_k = jnp.ones((HD, LANES), F32)
            for m in segs_of(h):
                mask = seg_mask(rel, h, m)
                s_q = jnp.where(mask, gfull[pl.ds(PK + m, 1), :], s_q)
                s_k = jnp.where(mask, gfull[pl.ds(PK + 3 + m, 1), :], s_k)
            s_q = jnp.sum(jnp.where(rel == row, s_q, 0.0), axis=1, keepdims=True)
            inv = jnp.where(valid, lax.rsqrt(s_q) * lax.rsqrt(s_k), 0.0)
            gram = jnp.where(valid, packed_head(gfull, h), 0.0)
            sc = tau * gram * inv
            top = jnp.max(jnp.where(valid, sc, -jnp.inf), axis=1, keepdims=True)
            ex = jnp.where(valid, jnp.exp(sc - top), 0.0)
            at = ex / jnp.sum(ex, axis=1, keepdims=True)
            hr = pl.ds(HD * h, HD)
            score[hr, :] = sc
            qk_inv[hr, :] = inv
            attn[hr, :] = at
            spread_head(at, rels, h, (a0, a1))

    far = pl.ds(pl.multiple_of(2 * OWN * (1 - chip), 16), 2 * OWN)
    near = pl.ds(pl.multiple_of(2 * OWN * chip, 16), 2 * OWN)
    theirs = pl.ds(pl.multiple_of(OWN * (1 - core), 8), OWN)
    mine = pl.ds(pl.multiple_of(OWN * core, 8), OWN)

    def part_rows(lhs_t, rows, rhs, part, r1, slot):
        part[slot] = mm(lhs_t[rows, :], rhs)
        return send(part.at[slot, theirs, :], r1.at[slot], sib)

    def cross(cp, part, r1, s, r2):
        cp.wait()
        s[...] = part[0, mine, :] + r1[0]
        return send(s, r2, nbr)

    with jax.named_scope("dv"):
        for i in range(NB):
            rows = block(i)
            dqkv[rows, 2 * C :] = window_mm(do[rows, :], (a0, a1), NN).astype(BF16)
        f_wv = part_rows(ut, far, dqkv[:, 2 * C :], wv_part, wv_r1, 0)
    with jax.named_scope("o"):
        for i in range(NB):
            rows = block(i)
            o[rows, :] = window_mm(v[rows, :], (a0, a1), NT).astype(BF16)
            ot[:, rows] = o[rows, :].T
    with jax.named_scope("cross_wv"):
        x_wv = cross(f_wv, wv_part, wv_r1, wv_s, wv_r2)
    with jax.named_scope("dwo_far"):
        f_wo = part_rows(ot, far, dy[...], wo_part, wo_r1, 0)

    with jax.named_scope("wait_a"):
        s_a2.wait()
    with jax.named_scope("softmax_bwd"):
        dsum = [jnp.zeros((1, LANES), F32) for _ in range(6)]
        lane = lax.broadcasted_iota(jnp.int32, (1, LANES), 1)
        d_tau = jnp.zeros((1, LANES), F32)
        for h in range(HEADS):
            rel = rels[h]
            valid = rel < HD
            hr = pl.ds(HD * h, HD)
            at = attn[hr, :]
            d_at = jnp.where(valid, packed_head(sa, h) + packed_head(ra2, h), 0.0).astype(BF16).astype(F32)
            d_sc = at * (d_at - jnp.sum(d_at * at, axis=1, keepdims=True))
            d_sc_inv = d_sc * qk_inv[hr, :]
            d_tau_h = jnp.sum(d_sc_inv * jnp.where(valid, packed_head(gfull, h), 0.0), axis=0, keepdims=True)
            d_tau = jnp.where(lane == h, jnp.sum(d_tau_h, axis=1, keepdims=True), d_tau)
            spread_head(d_sc_inv * tau_ref[h], rels, h, (e0, e1))
            wt = d_sc * score[hr, :]
            over_q = jnp.sum(jnp.where(rel == row, jnp.sum(wt, axis=1, keepdims=True), 0.0), axis=0, keepdims=True)
            over_k = jnp.sum(wt, axis=0, keepdims=True)
            for m in segs_of(h):
                mask = seg_mask(rel, h, m)[:1]
                dsum[m] = jnp.where(mask, over_q, dsum[m])
                dsum[3 + m] = jnp.where(mask, over_k, dsum[3 + m])
        dt_ref[...] = d_tau[:, :HEADS].reshape(HEADS)
        for m in range(6):
            dsq[:, pl.ds(LANES * m, LANES)] = -dsum[m] / gfull[pl.ds(PK + m, 1), :]
    with jax.named_scope("cross_wo"):
        x_wo = cross(f_wo, wo_part, wo_r1, wo_s, wo_r2)

    with jax.named_scope("dqk"):
        for i in range(NB):
            rows = block(i)
            dqkv[rows, :C] = (
                window_mm(k[rows, :], (e0, e1), NT) + q[rows, :].astype(F32) * dsq[:, :C]).astype(BF16)
            dqkv[rows, C : 2 * C] = (
                window_mm(q[rows, :], (e0, e1), NN) + k[rows, :].astype(F32) * dsq[:, C:]).astype(BF16)
    with jax.named_scope("dwqk_far"):
        f_wqk = part_rows(ut, far, dqkv[:, : 2 * C], wqk_part, wqk_r1, 0)
    with jax.named_scope("near"):
        l_wv = part_rows(ut, near, dqkv[:, 2 * C :], wv_part, wv_r1, 1)
    with jax.named_scope("cross_wqk"):
        x_wqk = cross(f_wqk, wqk_part, wqk_r1, wqk_s, wqk_r2)
    with jax.named_scope("near_qk"):
        l_wo = part_rows(ot, near, dy[...], wo_part, wo_r1, 1)
        l_wqk = part_rows(ut, near, dqkv[:, : 2 * C], wqk_part, wqk_r1, 1)

    gamma = g_ref[...].reshape(1, C)
    dgam = jnp.zeros((8, C), F32)
    dbet = jnp.zeros((8, C), F32)
    with jax.named_scope("ln_bwd"):
        for i in range(NB):
            rows = block(i)
            du[rows, :] = mm(dqkv[rows, :], wqkv[...], NT).astype(BF16)
            for j in range(RB // SB):
                sub = pl.ds(i * RB + j * SB, SB)
                d = du[sub, :].astype(F32)
                xh = xhat[sub, :]
                dxh = d * xh
                dgam += jnp.sum(dxh.reshape(SB // 8, 8, C), axis=0)
                dbet += jnp.sum(d.reshape(SB // 8, 8, C), axis=0)
                dh = d * gamma
                m1 = jnp.mean(dh, axis=-1, keepdims=True)
                m2 = jnp.mean(dxh * gamma, axis=-1, keepdims=True)
                inv = istd[sub, :]
                term = dh - m1 - xh * m2
                dln = term * jnp.concatenate([inv, inv, inv], axis=1)
                dx[sub, :] = (dy[sub, :].astype(F32) + dln).astype(BF16)
        dgb_all[me] = jnp.concatenate(
            [jnp.sum(dgam, axis=0, keepdims=True), jnp.sum(dbet, axis=0, keepdims=True)], axis=1)
    c_dgb = [send(dgb_all.at[me], dgb_all.at[me], peer) for peer in (sib, nbr, diag)]
    with jax.named_scope("y"):
        for i in range(NB):
            rows = block(i)
            y[rows, :] = (x[rows, :].astype(F32) + mm(o[rows, :], wo[...])).astype(BF16)

    with jax.named_scope("wait_wo"):
        l_wo.wait()
        x_wo.wait()
        dwo_ref[...] = (wo_part[1, mine, :] + wo_r1[1] + wo_r2[...]).astype(BF16)
    with jax.named_scope("wait_wv"):
        l_wv.wait()
        x_wv.wait()
        dwqkv_ref[:, 2 * C :] = (wv_part[1, mine, :] + wv_r1[1] + wv_r2[...]).astype(BF16)
    with jax.named_scope("wait_dgb"):
        for cp in c_dgb:
            cp.wait()
        total = dgb_all[0] + dgb_all[1] + dgb_all[2] + dgb_all[3]
        dg_ref[...] = total[:, :C].reshape(C)
        db_ref[...] = total[:, C:].reshape(C)
    with jax.named_scope("wait_wqk"):
        l_wqk.wait()
        x_wqk.wait()
        dwqkv_ref[:, : 2 * C] = (wqk_part[1, mine, :] + wqk_r1[1] + wqk_r2[...]).astype(BF16)


def write_out(*refs):
    ins, outs, sem = refs[:7], refs[7:14], refs[14]
    pairs = []
    for i in range(2):
        for j in range(PIECES):
            rows = pl.ds(j * (TOK // PIECES), TOK // PIECES)
            pairs.append((ins[i].at[rows, :], outs[i].at[rows, :]))
    pairs += [(ins[i], outs[i]) for i in range(2, 7)]
    copies = [pltpu.make_async_copy(src, dst, sem.at[i]) for i, (src, dst) in enumerate(pairs)]
    for cp in copies:
        cp.start()
    for cp in copies:
        cp.wait()


def xca_local(x_rows, dy_rows, ln_gamma, ln_beta, w_qkv, w_out, temperature):
    vm = pltpu.VMEM
    hbm_spec = pl.BlockSpec(memory_space=pltpu.HBM)
    vmem_spec = pl.BlockSpec(memory_space=pltpu.VMEM)
    results = (
        ((TOK, C), BF16), ((TOK, C), BF16), ((OWN, 3 * C), BF16), ((OWN, C), BF16),
        ((C,), F32), ((C,), F32), ((HEADS,), F32),
    )
    rows_bf = vm((TOK, C), BF16)
    cols_bf = vm((C, TOK), BF16)
    win_f = vm((256, 256), F32)
    win_b = vm((256, 256), BF16)
    pk_g = vm((PK + 8, LANES), F32)
    pk_a = vm((PK, LANES), F32)
    fold = vm((C, LANES), F32)
    scratch = [
        rows_bf, rows_bf, vm((C,), F32), vm((C,), F32), vm((C, 3 * C), BF16), vm((C, C), BF16), vm((C, C), BF16),
        pltpu.SMEM((HEADS,), F32), rows_bf, cols_bf, vm((TOK, C), F32), vm((TOK, LANES), F32),
        rows_bf, rows_bf, rows_bf, rows_bf, rows_bf, cols_bf, vm((TOK, 3 * C), BF16), rows_bf,
        win_f, win_f, vm((8, 2 * C), F32), pk_g, pk_g, pk_g, pk_g, pk_a, pk_a, pk_a, pk_a,
        win_b, win_b, win_b, win_b, fold, fold, fold, pk_g, vm((1, 2 * C), F32),
        vm((2, 2 * OWN, C), F32), vm((2, 2 * OWN, C), F32), vm((2, 2 * OWN, 2 * C), F32),
        vm((2, OWN, C), F32), vm((2, OWN, C), F32), vm((2, OWN, 2 * C), F32),
        vm((OWN, C), F32), vm((OWN, C), F32), vm((OWN, 2 * C), F32),
        vm((OWN, C), F32), vm((OWN, C), F32), vm((OWN, 2 * C), F32),
        vm((4, 1, 2 * C), F32),
        pltpu.SemaphoreType.DMA((16,)),
        pltpu.SemaphoreType.DMA((16,)), pltpu.SemaphoreType.DMA((16,)),
    ]
    parts = pl.pallas_call(
        kernel,
        name="xca",
        out_shape=tuple(pltpu.VMEM(shape, dtype) for shape, dtype in results),
        in_specs=[hbm_spec] * 7,
        out_specs=[vmem_spec] * 7,
        scratch_shapes=scratch,
        compiler_params=pltpu.CompilerParams(
            collective_id=0, has_side_effects=True, vmem_limit_bytes=60 * 1024 * 1024),
    )(x_rows, dy_rows, ln_gamma, ln_beta, w_qkv, w_out, temperature)
    return pl.pallas_call(
        write_out,
        name="xca_out",
        out_shape=tuple(jax.ShapeDtypeStruct(shape, dtype) for shape, dtype in results),
        in_specs=[vmem_spec] * 7,
        out_specs=[hbm_spec] * 7,
        scratch_shapes=[pltpu.SemaphoreType.DMA((2 * PIECES + 5,))],
        compiler_params=pltpu.CompilerParams(vmem_limit_bytes=1024 * 1024),
    )(*parts)


def solution(mesh):
    row_spec = P(('dp', 'sp'), None)
    full_mat = P(None, None)
    full_vec = P(None)
    part_vec = P('dp')
    return jax.shard_map(
        xca_local, mesh=mesh,
        in_specs=(row_spec, row_spec, full_vec, full_vec, full_mat, full_mat, full_vec),
        out_specs=(row_spec, row_spec, row_spec, row_spec, part_vec, part_vec, part_vec),
        check_vma=False)
```

```python
import jax
import jax.numpy as jnp
from jax import lax
from jax.experimental import pallas as pl
from jax.experimental.pallas import tpu as pltpu
from jax.sharding import PartitionSpec as P

LN_EPS = 1e-6
F32, BF16 = jnp.float32, jnp.bfloat16
MESH = pl.DeviceIdType.MESH

C = 384
HEADS, HD = 8, 48
LANES = 128
TOK = 2048
RB = 512
NB = TOK // RB
A_BLOCKS = (512, 512, 512, 512)
NA = len(A_BLOCKS)
RV = 256
NV = TOK // RV
CUT = 4
LAG = 3
PIECES = 1
SB = 64
OWN = C // 4
PK = 144
HALF = PK // 2
W0_HEADS = 5

NN = (((1,), (0,)), ((), ()))
NT = (((1,), (1,)), ((), ()))
TN = (((0,), (0,)), ((), ()))


def mm(a, b, dims=NN):
    return lax.dot_general(a, b, dims, preferred_element_type=F32)


def a_block(i):
    return sum(A_BLOCKS[:i]), A_BLOCKS[i]


def head_rel():
    lane = lax.broadcasted_iota(jnp.int32, (HD, LANES), 1)
    return [(lane - HD * h) & (LANES - 1) for h in range(HEADS)]


def seg_mask(rel, h, m):
    chan = rel + HD * h
    return (rel < HD) & (chan >= LANES * m) & (chan < LANES * (m + 1))


def head_window(h):
    if h < W0_HEADS:
        return 0, HD * h, (0, 1)
    return 1, HD * h - LANES, (1, 2)


def segs_of(h):
    return sorted({(HD * h) // LANES, (HD * h + HD - 1) // LANES})


def spare_lanes(g):
    lane = lax.broadcasted_iota(jnp.int32, (HD, LANES), 1)
    return (lane >= 96 - 32 * g) & (lane < 128 - 32 * g)


def fold_windows(win_refs, out_ref):
    rels = head_rel()

    def put(acc, h, where):
        w, row, segs = head_window(h)
        for s, m in enumerate(segs):
            if m in segs_of(h):
                block = win_refs[w][pl.ds(row, HD), pl.ds(LANES * s, LANES)]
                mask = seg_mask(rels[h], h, m)
                acc = jnp.where(mask if where is None else mask & where, block, acc)
        return acc

    for g in range(3):
        acc = put(put(jnp.zeros((HD, LANES), F32), 2 * g, None), 2 * g + 1, None)
        spare = spare_lanes(g)
        put_rows(out_ref, g, put(put(acc, 6, spare), 7, spare))


def put_rows(ref, g, value):
    if len(ref.shape) == 2:
        ref[pl.ds(HD * g, HD), :] = value
    elif g == 1:
        ref[0, pl.ds(HD, HALF - HD), :] = value[: HALF - HD]
        ref[1, pl.ds(0, HALF - HD), :] = value[HALF - HD :]
    else:
        ref[g // 2, pl.ds((HALF - HD) * (g // 2), HD), :] = value


def get_rows(ref, g):
    if len(ref.shape) == 2:
        return ref[pl.ds(HD * g, HD), :]
    if g == 1:
        return jnp.concatenate([ref[0, pl.ds(HD, HALF - HD), :], ref[1, pl.ds(0, HALF - HD), :]], axis=0)
    return ref[g // 2, pl.ds((HALF - HD) * (g // 2), HD), :]


def packed_head(ref, h):
    if h < 6:
        return get_rows(ref, h // 2)
    lane = lax.broadcasted_iota(jnp.int32, (HD, LANES), 1)
    return jnp.where(lane >= 96, get_rows(ref, 0), jnp.where(lane >= 64, get_rows(ref, 1), get_rows(ref, 2)))


def spread_head(value, rels, h, win_refs):
    w, row, segs = head_window(h)
    parts = []
    for m in segs:
        if m in segs_of(h):
            parts.append(jnp.where(seg_mask(rels[h], h, m), value, 0.0))
        else:
            parts.append(jnp.zeros((HD, LANES), F32))
    win_refs[w][pl.ds(row, HD), :] = jnp.concatenate(parts, axis=1).astype(BF16)


def window_mm(a, win_refs, dims):
    r0 = mm(a[:, :256], win_refs[0][...], dims)
    r1 = mm(a[:, 128:], win_refs[1][...], dims)
    return jnp.concatenate([r0[:, :128], r0[:, 128:] + r1[:, :128], r1[:, 128:]], axis=1)


def kernel(
    x_hbm, dy_hbm, g_hbm, b_hbm, wqkv_hbm, wo_hbm, tau_hbm,
    y, dx, dwqkv_ref, dwo_ref, dg_ref, db_ref, dt_ref,
    x, dy, g_ref, b_ref, wqkv, wo, wot, tau_ref, u, ut, xhat, istd, q, k, v, do, o, ot, dqkv, du,
    g0, g1, sq, pg, rg1, sg, rg2, pa, ra1, sa,
    a0, a1, e0, e1, attn, score, qk_inv, gfull, dsq,
    wo_part, wv_part, wq_part, wk_part, wo_r1, wv_r1, wq_r1, wk_r1,
    wo_s, wv_s, wq_s, wk_s, wo_r2, wv_r2, wq_r2, wk_r2,
    dgb_all,
    in_sem, send_sem, recv_sem,
):
    me = lax.axis_index("sp")
    core = lax.rem(me, 2)
    chip = me // 2
    sib = me + 1 - 2 * core
    nbr = lax.rem(me + 2, 4)
    diag = lax.rem(sib + 2, 4)

    n_loads = [0]

    def load(src, dst):
        cp = pltpu.make_async_copy(src, dst, in_sem.at[n_loads[0]])
        n_loads[0] += 1
        cp.start()
        return cp

    def block(i):
        return pl.ds(i * RB, RB)

    ld_gb = [load(g_hbm, g_ref), load(b_hbm, b_ref)]
    ld_x = [load(x_hbm.at[pl.ds(*a_block(0)), :], x.at[pl.ds(*a_block(0)), :])]
    ld_wqk = load(wqkv_hbm.at[:, pl.ds(0, 2 * C)], wqkv.at[:, pl.ds(0, 2 * C)])
    ld_x += [load(x_hbm.at[pl.ds(*a_block(i)), :], x.at[pl.ds(*a_block(i)), :]) for i in range(1, NA)]
    ld_wo = load(wo_hbm, wo)
    ld_wv = load(wqkv_hbm.at[:, pl.ds(2 * C, C)], wqkv.at[:, pl.ds(2 * C, C)])
    ld_dy = load(dy_hbm, dy)
    ld_tau = load(tau_hbm, tau_ref)

    barrier = pltpu.get_barrier_semaphore()
    for peer in (sib, nbr, diag):
        pl.semaphore_signal(barrier, inc=1, device_id={"sp": peer}, device_id_type=MESH)

    n_sends = [0]

    def send(src, dst, peer):
        i = n_sends[0]
        n_sends[0] += 1
        cp = pltpu.make_async_remote_copy(
            src_ref=src, dst_ref=dst, send_sem=send_sem.at[i], recv_sem=recv_sem.at[i],
            device_id={"sp": peer}, device_id_type=MESH)
        cp.start()
        return cp

    def step_ln(i):
        gamma = g_ref[...].reshape(1, C)
        beta = b_ref[...].reshape(1, C)
        lo, size = a_block(i)
        for j in range(size // SB):
            rows = pl.ds(lo + j * SB, SB)
            xf = x[rows, :].astype(F32)
            cen = xf - jnp.mean(xf, axis=-1, keepdims=True)
            inv = lax.rsqrt(jnp.mean(cen * cen, axis=-1, keepdims=True) + LN_EPS)
            xh = cen * inv
            xhat[rows, :] = xh
            istd[rows, :] = jnp.broadcast_to(inv, (SB, LANES))
            u[rows, :] = (xh * gamma + beta).astype(BF16)

    def step_qk(i):
        lo, size = a_block(i)
        rows = pl.ds(lo, size)
        qk = mm(u[rows, :], wqkv[:, : 2 * C]).astype(BF16)
        q[rows, :] = qk[:, :C]
        k[rows, :] = qk[:, C:]

    def step_gram(i):
        lo, size = a_block(i)
        rows = pl.ds(lo, size)
        p0 = mm(q[rows, :256], k[rows, :256], TN)
        p1 = mm(q[rows, 128:], k[rows, 128:], TN)
        if i == 0:
            g0[...], g1[...] = p0, p1
        else:
            g0[...] += p0
            g1[...] += p1
        for r, c0 in ((q, 0), (k, C)):
            part = jnp.zeros((8, C), F32)
            for j in range(size // SB):
                f = r[pl.ds(lo + j * SB, SB), :].astype(F32)
                part += jnp.sum((f * f).reshape(SB // 8, 8, C), axis=0)
            if i == 0:
                sq[:, pl.ds(c0, C)] = part
            else:
                sq[:, pl.ds(c0, C)] += part
        ut[:, rows] = u[rows, :].T

    with jax.named_scope("ln_0"):
        ld_x[0].wait()
        for cp in ld_gb:
            cp.wait()
        step_ln(0)
    ld_wqk.wait()
    for cp in ld_x[1:]:
        cp.wait()
    ld_wo.wait()
    with jax.named_scope("ln_qk"):
        wot[...] = wo[...].T
        for i in range(1, NA + 2):
            if i < NA:
                step_ln(i)
            if 1 <= i <= NA:
                step_qk(i - 1)
            if i >= 2:
                step_gram(i - 2)
    with jax.named_scope("fold_g"):
        fold_windows((g0, g1), pg)
        sums = jnp.sum(sq[...], axis=0, keepdims=True)
        for m in range(6):
            pg[pl.ds(PK + m, 1), :] = sums[:, LANES * m : LANES * (m + 1)]
        pg[pl.ds(PK + 6, 2), :] = jnp.zeros((2, LANES), F32)
    with jax.named_scope("greet"):
        pl.semaphore_wait(barrier, 3)
    s_g1 = send(pg, rg1, sib)

    def step_b(i):
        rows = pl.ds(i * RV, RV)
        v[rows, :] = mm(u[rows, :], wqkv[:, 2 * C :]).astype(BF16)
        do[rows, :] = mm(dy[rows, :], wot[...]).astype(BF16)

    def step_da(i):
        rows = pl.ds(i * RV, RV)
        p0 = mm(do[rows, :256], v[rows, :256], TN)
        p1 = mm(do[rows, 128:], v[rows, 128:], TN)
        if i == 0:
            g0[...], g1[...] = p0, p1
        else:
            g0[...] += p0
            g1[...] += p1

    with jax.named_scope("v_do_1"):
        ld_wv.wait()
        ld_dy.wait()
        ld_tau.wait()
        for i in range(CUT):
            step_b(i)
    with jax.named_scope("sum_g"):
        s_g1.wait()
        sg[...] = pg[...] + rg1[...]
        s_g2 = send(sg, rg2, nbr)
    with jax.named_scope("v_do_2"):
        for i in range(CUT, NV):
            step_b(i)
            for j in range(max(0, i - LAG) if i > CUT else 0, i + 1 - LAG):
                step_da(j)
        for i in range(NV - LAG, NV):
            step_da(i)
    with jax.named_scope("fold_a"):
        fold_windows((g0, g1), pa)
        s_a1 = [
            send(pa.at[1 - core], ra1.at[me], sib),
            send(pa.at[core], ra1.at[me], nbr),
            send(pa.at[1 - core], ra1.at[me], diag),
        ]

    with jax.named_scope("wait_g"):
        s_g2.wait()
    rels = head_rel()
    row = lax.broadcasted_iota(jnp.int32, (HD, LANES), 0)
    with jax.named_scope("softmax"):
        gfull[...] = sg[...] + rg2[...]
        for ref in (a0, a1, e0, e1):
            ref[...] = jnp.zeros_like(ref)
        for h in range(HEADS):
            rel = rels[h]
            valid = rel < HD
            tau = tau_ref[h]
            s_q = jnp.zeros((HD, LANES), F32)
            s_k = jnp.ones((HD, LANES), F32)
            for m in segs_of(h):
                mask = seg_mask(rel, h, m)
                s_q = jnp.where(mask, gfull[pl.ds(PK + m, 1), :], s_q)
                s_k = jnp.where(mask, gfull[pl.ds(PK + 3 + m, 1), :], s_k)
            q_inv = lax.rsqrt(jnp.sum(jnp.where(rel == row, s_q, 0.0), axis=1, keepdims=True))
            k_inv = lax.rsqrt(s_k)
            by_k = packed_head(gfull, h) * k_inv
            top = jnp.max(jnp.where(valid, by_k, -jnp.inf), axis=1, keepdims=True)
            scale = tau * q_inv
            sc = jnp.where(valid, scale * by_k, 0.0)
            inv = jnp.where(valid, q_inv * k_inv, 0.0)
            ex = jnp.where(valid, jnp.exp(sc - scale * top), 0.0)
            at = ex / jnp.sum(ex, axis=1, keepdims=True)
            hr = pl.ds(HD * h, HD)
            score[hr, :] = sc
            qk_inv[hr, :] = inv
            attn[hr, :] = at
            spread_head(at, rels, h, (a0, a1))

    far = pl.ds(pl.multiple_of(2 * OWN * (1 - chip), 16), 2 * OWN)
    near = pl.ds(pl.multiple_of(2 * OWN * chip, 16), 2 * OWN)
    theirs = pl.ds(pl.multiple_of(OWN * (1 - core), 8), OWN)
    mine = pl.ds(pl.multiple_of(OWN * core, 8), OWN)

    def part_rows(lhs_t, rows, rhs, part, r1, slot):
        part[slot] = mm(lhs_t[rows, :], rhs)
        return send(part.at[slot, theirs, :], r1.at[slot], sib)

    def cross(cp, part, r1, s, r2):
        cp.wait()
        s[...] = part[0, mine, :] + r1[0]
        return send(s, r2, nbr)

    with jax.named_scope("dv"):
        for i in range(NB):
            rows = block(i)
            dqkv[rows, 2 * C :] = window_mm(do[rows, :], (a0, a1), NN).astype(BF16)
        f_wv = part_rows(ut, far, dqkv[:, 2 * C :], wv_part, wv_r1, 0)
    with jax.named_scope("sum_a"):
        ra1[me] = pa[core]
        for cp in s_a1:
            cp.wait()
        sa[core] = (ra1[0] + ra1[1]) + (ra1[2] + ra1[3])
        s_a2 = send(sa.at[core], sa.at[core], sib)
    with jax.named_scope("o"):
        for i in range(NB):
            rows = block(i)
            o[rows, :] = window_mm(v[rows, :], (a0, a1), NT).astype(BF16)
            ot[:, rows] = o[rows, :].T
    with jax.named_scope("cross_wv"):
        x_wv = cross(f_wv, wv_part, wv_r1, wv_s, wv_r2)
    with jax.named_scope("dwo_far"):
        f_wo = part_rows(ot, far, dy[...], wo_part, wo_r1, 0)

    with jax.named_scope("wait_a"):
        s_a2.wait()
    with jax.named_scope("softmax_bwd"):
        dsum = [jnp.zeros((1, LANES), F32) for _ in range(6)]
        lane = lax.broadcasted_iota(jnp.int32, (1, LANES), 1)
        d_tau = jnp.zeros((1, LANES), F32)
        for h in range(HEADS):
            rel = rels[h]
            valid = rel < HD
            hr = pl.ds(HD * h, HD)
            at = attn[hr, :]
            d_at = jnp.where(valid, packed_head(sa, h), 0.0).astype(BF16).astype(F32)
            d_sc = at * (d_at - jnp.sum(d_at * at, axis=1, keepdims=True))
            d_sc_inv = d_sc * qk_inv[hr, :]
            d_tau_h = jnp.sum(d_sc_inv * jnp.where(valid, packed_head(gfull, h), 0.0), axis=0, keepdims=True)
            d_tau = jnp.where(lane == h, jnp.sum(d_tau_h, axis=1, keepdims=True), d_tau)
            spread_head(d_sc_inv * tau_ref[h], rels, h, (e0, e1))
            wt = d_sc * score[hr, :]
            over_q = jnp.sum(jnp.where(rel == row, jnp.sum(wt, axis=1, keepdims=True), 0.0), axis=0, keepdims=True)
            over_k = jnp.sum(wt, axis=0, keepdims=True)
            for m in segs_of(h):
                mask = seg_mask(rel, h, m)[:1]
                dsum[m] = jnp.where(mask, over_q, dsum[m])
                dsum[3 + m] = jnp.where(mask, over_k, dsum[3 + m])
        dt_ref[...] = d_tau[:, :HEADS].reshape(HEADS)
        for m in range(6):
            dsq[:, pl.ds(LANES * m, LANES)] = -dsum[m] / gfull[pl.ds(PK + m, 1), :]
    with jax.named_scope("dqk"):
        for i in range(NB):
            rows = block(i)
            dqkv[rows, :C] = (
                window_mm(k[rows, :], (e0, e1), NT) + q[rows, :].astype(F32) * dsq[:, :C]).astype(BF16)
            dqkv[rows, C : 2 * C] = (
                window_mm(q[rows, :], (e0, e1), NN) + k[rows, :].astype(F32) * dsq[:, C:]).astype(BF16)
    with jax.named_scope("cross_wo"):
        x_wo = cross(f_wo, wo_part, wo_r1, wo_s, wo_r2)
    with jax.named_scope("dwq_far"):
        f_wq = part_rows(ut, far, dqkv[:, :C], wq_part, wq_r1, 0)
    with jax.named_scope("dwk_far"):
        f_wk = part_rows(ut, far, dqkv[:, C : 2 * C], wk_part, wk_r1, 0)
    with jax.named_scope("near_v"):
        l_wv = part_rows(ut, near, dqkv[:, 2 * C :], wv_part, wv_r1, 1)
    with jax.named_scope("cross_wq"):
        x_wq = cross(f_wq, wq_part, wq_r1, wq_s, wq_r2)
    with jax.named_scope("near_o"):
        l_wo = part_rows(ot, near, dy[...], wo_part, wo_r1, 1)
    with jax.named_scope("cross_wk"):
        x_wk = cross(f_wk, wk_part, wk_r1, wk_s, wk_r2)
    with jax.named_scope("near_qk"):
        l_wq = part_rows(ut, near, dqkv[:, :C], wq_part, wq_r1, 1)
        l_wk = part_rows(ut, near, dqkv[:, C : 2 * C], wk_part, wk_r1, 1)

    gamma = g_ref[...].reshape(1, C)
    dgam = jnp.zeros((8, C), F32)
    dbet = jnp.zeros((8, C), F32)
    with jax.named_scope("ln_bwd"):
        for i in range(NB):
            rows = block(i)
            du[rows, :] = mm(dqkv[rows, :], wqkv[...], NT).astype(BF16)
            for j in range(RB // SB):
                sub = pl.ds(i * RB + j * SB, SB)
                d = du[sub, :].astype(F32)
                xh = xhat[sub, :]
                dxh = d * xh
                dgam += jnp.sum(dxh.reshape(SB // 8, 8, C), axis=0)
                dbet += jnp.sum(d.reshape(SB // 8, 8, C), axis=0)
                dh = d * gamma
                m1 = jnp.mean(dh, axis=-1, keepdims=True)
                m2 = jnp.mean(dxh * gamma, axis=-1, keepdims=True)
                inv = istd[sub, :]
                term = dh - m1 - xh * m2
                dln = term * jnp.concatenate([inv, inv, inv], axis=1)
                dx[sub, :] = (dy[sub, :].astype(F32) + dln).astype(BF16)
        dgb_all[me] = jnp.concatenate(
            [jnp.sum(dgam, axis=0, keepdims=True), jnp.sum(dbet, axis=0, keepdims=True)], axis=1)
    c_dgb = [send(dgb_all.at[me], dgb_all.at[me], peer) for peer in (sib, nbr, diag)]
    with jax.named_scope("y"):
        for i in range(NB):
            rows = block(i)
            y[rows, :] = (x[rows, :].astype(F32) + mm(o[rows, :], wo[...])).astype(BF16)

    with jax.named_scope("wait_wo"):
        l_wo.wait()
        x_wo.wait()
        dwo_ref[...] = (wo_part[1, mine, :] + wo_r1[1] + wo_r2[...]).astype(BF16)
    with jax.named_scope("wait_wv"):
        l_wv.wait()
        x_wv.wait()
        dwqkv_ref[:, 2 * C :] = (wv_part[1, mine, :] + wv_r1[1] + wv_r2[...]).astype(BF16)
    with jax.named_scope("wait_wq"):
        l_wq.wait()
        x_wq.wait()
        dwqkv_ref[:, :C] = (wq_part[1, mine, :] + wq_r1[1] + wq_r2[...]).astype(BF16)
    with jax.named_scope("wait_dgb"):
        for cp in c_dgb:
            cp.wait()
        total = dgb_all[0] + dgb_all[1] + dgb_all[2] + dgb_all[3]
        dg_ref[...] = total[:, :C].reshape(C)
        db_ref[...] = total[:, C:].reshape(C)
    with jax.named_scope("wait_wqk"):
        l_wk.wait()
        x_wk.wait()
        dwqkv_ref[:, C : 2 * C] = (wk_part[1, mine, :] + wk_r1[1] + wk_r2[...]).astype(BF16)


def write_out(*refs):
    ins, outs, sem = refs[:7], refs[7:14], refs[14]
    pairs = []
    for i in range(2):
        for j in range(PIECES):
            rows = pl.ds(j * (TOK // PIECES), TOK // PIECES)
            pairs.append((ins[i].at[rows, :], outs[i].at[rows, :]))
    pairs += [(ins[i], outs[i]) for i in range(2, 7)]
    copies = [pltpu.make_async_copy(src, dst, sem.at[i]) for i, (src, dst) in enumerate(pairs)]
    for cp in copies:
        cp.start()
    for cp in copies:
        cp.wait()


def xca_local(x_rows, dy_rows, ln_gamma, ln_beta, w_qkv, w_out, temperature):
    vm = pltpu.VMEM
    hbm_spec = pl.BlockSpec(memory_space=pltpu.HBM)
    vmem_spec = pl.BlockSpec(memory_space=pltpu.VMEM)
    results = (
        ((TOK, C), BF16), ((TOK, C), BF16), ((OWN, 3 * C), BF16), ((OWN, C), BF16),
        ((C,), F32), ((C,), F32), ((HEADS,), F32),
    )
    rows_bf = vm((TOK, C), BF16)
    cols_bf = vm((C, TOK), BF16)
    win_f = vm((256, 256), F32)
    win_b = vm((256, 256), BF16)
    pk_g = vm((PK + 8, LANES), F32)
    pk_a = vm((2, HALF, LANES), F32)
    fold = vm((C, LANES), F32)
    scratch = [
        rows_bf, rows_bf, vm((C,), F32), vm((C,), F32), vm((C, 3 * C), BF16), vm((C, C), BF16), vm((C, C), BF16),
        pltpu.SMEM((HEADS,), F32), rows_bf, cols_bf, vm((TOK, C), F32), vm((TOK, LANES), F32),
        rows_bf, rows_bf, rows_bf, rows_bf, rows_bf, cols_bf, vm((TOK, 3 * C), BF16), rows_bf,
        win_f, win_f, vm((8, 2 * C), F32), pk_g, pk_g, pk_g, pk_g, pk_a, vm((4, HALF, LANES), F32), pk_a,
        win_b, win_b, win_b, win_b, fold, fold, fold, pk_g, vm((1, 2 * C), F32),
        *[vm((2, 2 * OWN, C), F32)] * 4, *[vm((2, OWN, C), F32)] * 4, *[vm((OWN, C), F32)] * 8,
        vm((4, 1, 2 * C), F32),
        pltpu.SemaphoreType.DMA((16,)),
        pltpu.SemaphoreType.DMA((24,)), pltpu.SemaphoreType.DMA((24,)),
    ]
    parts = pl.pallas_call(
        kernel,
        name="xca",
        out_shape=tuple(pltpu.VMEM(shape, dtype) for shape, dtype in results),
        in_specs=[hbm_spec] * 7,
        out_specs=[vmem_spec] * 7,
        scratch_shapes=scratch,
        compiler_params=pltpu.CompilerParams(
            collective_id=0, has_side_effects=True, vmem_limit_bytes=60 * 1024 * 1024),
    )(x_rows, dy_rows, ln_gamma, ln_beta, w_qkv, w_out, temperature)
    return pl.pallas_call(
        write_out,
        name="xca_out",
        out_shape=tuple(jax.ShapeDtypeStruct(shape, dtype) for shape, dtype in results),
        in_specs=[vmem_spec] * 7,
        out_specs=[hbm_spec] * 7,
        scratch_shapes=[pltpu.SemaphoreType.DMA((2 * PIECES + 5,))],
        compiler_params=pltpu.CompilerParams(vmem_limit_bytes=1024 * 1024),
    )(*parts)


def solution(mesh):
    row_spec = P(('dp', 'sp'), None)
    full_mat = P(None, None)
    full_vec = P(None)
    part_vec = P('dp')
    return jax.shard_map(
        xca_local, mesh=mesh,
        in_specs=(row_spec, row_spec, full_vec, full_vec, full_mat, full_mat, full_vec),
        out_specs=(row_spec, row_spec, row_spec, row_spec, part_vec, part_vec, part_vec),
        check_vma=False)
```

```python
import jax
import jax.numpy as jnp
from jax import lax
from jax.experimental import pallas as pl
from jax.experimental.pallas import tpu as pltpu
from jax.sharding import PartitionSpec as P

LN_EPS = 1e-6
F32, BF16 = jnp.float32, jnp.bfloat16
MESH = pl.DeviceIdType.MESH

C = 384
HEADS, HD = 8, 48
LANES = 128
TOK = 2048
RB = 512
NB = TOK // RB
A_BLOCKS = (512, 512, 512, 512)
NA = len(A_BLOCKS)
RV = 256
NV = TOK // RV
CUT = 4
LAG = 3
N_SENDS = 23
PIECES = 1
SB = 64
OWN = C // 4
PK = 144
DIRECT = 16
HALF = PK // 2
W0_HEADS = 5

NN = (((1,), (0,)), ((), ()))
NT = (((1,), (1,)), ((), ()))
TN = (((0,), (0,)), ((), ()))


def mm(a, b, dims=NN):
    return lax.dot_general(a, b, dims, preferred_element_type=F32)


def a_block(i):
    return sum(A_BLOCKS[:i]), A_BLOCKS[i]


def head_rel():
    lane = lax.broadcasted_iota(jnp.int32, (HD, LANES), 1)
    return [(lane - HD * h) & (LANES - 1) for h in range(HEADS)]


def seg_mask(rel, h, m):
    chan = rel + HD * h
    return (rel < HD) & (chan >= LANES * m) & (chan < LANES * (m + 1))


def head_window(h):
    if h < W0_HEADS:
        return 0, HD * h, (0, 1)
    return 1, HD * h - LANES, (1, 2)


def segs_of(h):
    return sorted({(HD * h) // LANES, (HD * h + HD - 1) // LANES})


def spare_lanes(g):
    lane = lax.broadcasted_iota(jnp.int32, (HD, LANES), 1)
    return (lane >= 96 - 32 * g) & (lane < 128 - 32 * g)


def fold_windows(win_refs, out_ref):
    rels = head_rel()

    def put(acc, h, where):
        w, row, segs = head_window(h)
        for s, m in enumerate(segs):
            if m in segs_of(h):
                block = win_refs[w][pl.ds(row, HD), pl.ds(LANES * s, LANES)]
                mask = seg_mask(rels[h], h, m)
                acc = jnp.where(mask if where is None else mask & where, block, acc)
        return acc

    for g in range(3):
        acc = put(put(jnp.zeros((HD, LANES), F32), 2 * g, None), 2 * g + 1, None)
        spare = spare_lanes(g)
        put_rows(out_ref, g, put(put(acc, 6, spare), 7, spare))


def put_rows(ref, g, value):
    if len(ref.shape) == 2:
        ref[pl.ds(HD * g, HD), :] = value
    elif g == 1:
        ref[0, pl.ds(HD, HALF - HD), :] = value[: HALF - HD]
        ref[1, pl.ds(0, HALF - HD), :] = value[HALF - HD :]
    else:
        ref[g // 2, pl.ds((HALF - HD) * (g // 2), HD), :] = value


def get_rows(ref, g):
    if len(ref.shape) == 2:
        return ref[pl.ds(HD * g, HD), :]
    if g == 1:
        return jnp.concatenate([ref[0, pl.ds(HD, HALF - HD), :], ref[1, pl.ds(0, HALF - HD), :]], axis=0)
    return ref[g // 2, pl.ds((HALF - HD) * (g // 2), HD), :]


def packed_head(ref, h):
    if h < 6:
        return get_rows(ref, h // 2)
    lane = lax.broadcasted_iota(jnp.int32, (HD, LANES), 1)
    return jnp.where(lane >= 96, get_rows(ref, 0), jnp.where(lane >= 64, get_rows(ref, 1), get_rows(ref, 2)))


def spread_head(value, rels, h, win_refs):
    w, row, segs = head_window(h)
    parts = []
    for m in segs:
        if m in segs_of(h):
            parts.append(jnp.where(seg_mask(rels[h], h, m), value, 0.0))
        else:
            parts.append(jnp.zeros((HD, LANES), F32))
    win_refs[w][pl.ds(row, HD), :] = jnp.concatenate(parts, axis=1).astype(BF16)


def window_mm(a, win_refs, dims):
    r0 = mm(a[:, :256], win_refs[0][...], dims)
    r1 = mm(a[:, 128:], win_refs[1][...], dims)
    return jnp.concatenate([r0[:, :128], r0[:, 128:] + r1[:, :128], r1[:, 128:]], axis=1)


def kernel(
    x_hbm, dy_hbm, g_hbm, b_hbm, wqkv_hbm, wo_hbm, tau_hbm,
    y, dx, dwqkv_ref, dwo_ref, dg_ref, db_ref, dt_ref,
    x, dy, g_ref, b_ref, wqkv, wo, wot, tau_ref, u, ut, xhat, istd, q, k, v, do, o, ot, dqkv, du,
    g0, g1, sq, pg, rg1, sg, rg2, pa, ra1, sa,
    a0, a1, e0, e1, attn, score, qk_inv, gfull, dsq,
    wo_part, wv_part, wq_part, wk_part, wo_r1, wv_r1, wq_r1, wk_r1,
    wo_s, wv_s, wq_s, wk_s, wo_r2, wv_r2, wq_r2, wk_r2, wv_d,
    dgb_all,
    in_sem, send_sem, recv_sem,
):
    me = lax.axis_index("sp")
    core = lax.rem(me, 2)
    chip = me // 2
    sib = me + 1 - 2 * core
    nbr = lax.rem(me + 2, 4)
    diag = lax.rem(sib + 2, 4)

    n_loads = [0]

    def load(src, dst):
        cp = pltpu.make_async_copy(src, dst, in_sem.at[n_loads[0]])
        n_loads[0] += 1
        cp.start()
        return cp

    def block(i):
        return pl.ds(i * RB, RB)

    ld_gb = [load(g_hbm, g_ref), load(b_hbm, b_ref)]
    ld_x = [load(x_hbm.at[pl.ds(*a_block(0)), :], x.at[pl.ds(*a_block(0)), :])]
    ld_wqk = load(wqkv_hbm.at[:, pl.ds(0, 2 * C)], wqkv.at[:, pl.ds(0, 2 * C)])
    ld_x += [load(x_hbm.at[pl.ds(*a_block(i)), :], x.at[pl.ds(*a_block(i)), :]) for i in range(1, NA)]
    ld_wo = load(wo_hbm, wo)
    ld_wv = load(wqkv_hbm.at[:, pl.ds(2 * C, C)], wqkv.at[:, pl.ds(2 * C, C)])
    ld_dy = load(dy_hbm, dy)
    ld_tau = load(tau_hbm, tau_ref)

    barrier = pltpu.get_barrier_semaphore()
    for peer in (sib, nbr, diag):
        pl.semaphore_signal(barrier, inc=1, device_id={"sp": peer}, device_id_type=MESH)

    sends = []

    def send(src, dst, peer):
        i = len(sends)
        cp = pltpu.make_async_remote_copy(
            src_ref=src, dst_ref=dst, send_sem=send_sem.at[i], recv_sem=recv_sem.at[i],
            device_id={"sp": peer}, device_id_type=MESH)
        cp.start()
        sends.append(cp)
        return cp

    def step_ln(i):
        gamma = g_ref[...].reshape(1, C)
        beta = b_ref[...].reshape(1, C)
        lo, size = a_block(i)
        for j in range(size // SB):
            rows = pl.ds(lo + j * SB, SB)
            xf = x[rows, :].astype(F32)
            cen = xf - jnp.mean(xf, axis=-1, keepdims=True)
            inv = lax.rsqrt(jnp.mean(cen * cen, axis=-1, keepdims=True) + LN_EPS)
            xh = cen * inv
            xhat[rows, :] = xh
            istd[rows, :] = jnp.broadcast_to(inv, (SB, LANES))
            u[rows, :] = (xh * gamma + beta).astype(BF16)

    def step_qk(i):
        lo, size = a_block(i)
        rows = pl.ds(lo, size)
        qk = mm(u[rows, :], wqkv[:, : 2 * C]).astype(BF16)
        q[rows, :] = qk[:, :C]
        k[rows, :] = qk[:, C:]

    def step_gram(i):
        lo, size = a_block(i)
        rows = pl.ds(lo, size)
        p0 = mm(q[rows, :256], k[rows, :256], TN)
        p1 = mm(q[rows, 128:], k[rows, 128:], TN)
        if i == 0:
            g0[...], g1[...] = p0, p1
        else:
            g0[...] += p0
            g1[...] += p1
        for r, c0 in ((q, 0), (k, C)):
            part = jnp.zeros((8, C), F32)
            for j in range(size // SB):
                f = r[pl.ds(lo + j * SB, SB), :].astype(F32)
                part += jnp.sum((f * f).reshape(SB // 8, 8, C), axis=0)
            if i == 0:
                sq[:, pl.ds(c0, C)] = part
            else:
                sq[:, pl.ds(c0, C)] += part
        ut[:, rows] = u[rows, :].T

    with jax.named_scope("ln_0"):
        ld_x[0].wait()
        for cp in ld_gb:
            cp.wait()
        step_ln(0)
    ld_wqk.wait()
    for cp in ld_x[1:]:
        cp.wait()
    with jax.named_scope("ln_qk"):
        for i in range(1, NA + 2):
            if i < NA:
                step_ln(i)
            if 1 <= i <= NA:
                step_qk(i - 1)
            if i >= 2:
                step_gram(i - 2)
    with jax.named_scope("fold_g"):
        fold_windows((g0, g1), pg)
        sums = jnp.sum(sq[...], axis=0, keepdims=True)
        for m in range(6):
            pg[pl.ds(PK + m, 1), :] = sums[:, LANES * m : LANES * (m + 1)]
        pg[pl.ds(PK + 6, 2), :] = jnp.zeros((2, LANES), F32)
    with jax.named_scope("greet"):
        pl.semaphore_wait(barrier, 3)
    s_g1 = send(pg, rg1, sib)

    def step_b(i):
        rows = pl.ds(i * RV, RV)
        v[rows, :] = mm(u[rows, :], wqkv[:, 2 * C :]).astype(BF16)
        do[rows, :] = mm(dy[rows, :], wot[...]).astype(BF16)

    def step_da(i):
        rows = pl.ds(i * RV, RV)
        p0 = mm(do[rows, :256], v[rows, :256], TN)
        p1 = mm(do[rows, 128:], v[rows, 128:], TN)
        if i == 0:
            g0[...], g1[...] = p0, p1
        else:
            g0[...] += p0
            g1[...] += p1

    with jax.named_scope("v_do_1"):
        ld_wo.wait()
        ld_wv.wait()
        ld_dy.wait()
        ld_tau.wait()
        wot[...] = wo[...].T
        for i in range(CUT):
            step_b(i)
    with jax.named_scope("sum_g"):
        s_g1.wait_recv()
        sg[...] = pg[...] + rg1[...]
        s_g2 = [
            pltpu.make_async_remote_copy(
                src_ref=sg, dst_ref=rg2, send_sem=send_sem.at[N_SENDS + j], recv_sem=recv_sem.at[N_SENDS],
                device_id={"sp": peer}, device_id_type=MESH)
            for j, peer in enumerate((diag, nbr))
        ]

        @pl.when(core == 1)
        def _():
            for cp in s_g2:
                cp.start()
    with jax.named_scope("v_do_2"):
        for i in range(CUT, NV):
            step_b(i)
            for j in range(max(0, i - LAG) if i > CUT else 0, i + 1 - LAG):
                step_da(j)
        for i in range(NV - LAG, NV):
            step_da(i)
    with jax.named_scope("fold_a"):
        fold_windows((g0, g1), pa)
        s_a1 = [
            send(pa.at[1 - core], ra1.at[me], sib),
            send(pa.at[core], ra1.at[me], nbr),
            send(pa.at[1 - core], ra1.at[me], diag),
        ]

    with jax.named_scope("wait_g"):
        s_g2[0].wait_recv()
    rels = head_rel()
    row = lax.broadcasted_iota(jnp.int32, (HD, LANES), 0)
    with jax.named_scope("softmax"):
        gfull[...] = sg[...] + rg2[...]
        for ref in (a0, a1, e0, e1):
            ref[...] = jnp.zeros_like(ref)
        for h in range(HEADS):
            rel = rels[h]
            valid = rel < HD
            tau = tau_ref[h]
            s_q = jnp.zeros((HD, LANES), F32)
            s_k = jnp.ones((HD, LANES), F32)
            for m in segs_of(h):
                mask = seg_mask(rel, h, m)
                s_q = jnp.where(mask, gfull[pl.ds(PK + m, 1), :], s_q)
                s_k = jnp.where(mask, gfull[pl.ds(PK + 3 + m, 1), :], s_k)
            q_inv = lax.rsqrt(jnp.sum(jnp.where(rel == row, s_q, 0.0), axis=1, keepdims=True))
            k_inv = lax.rsqrt(s_k)
            by_k = packed_head(gfull, h) * k_inv
            top = jnp.max(jnp.where(valid, by_k, -jnp.inf), axis=1, keepdims=True)
            scale = tau * q_inv
            sc = jnp.where(valid, scale * by_k, 0.0)
            inv = jnp.where(valid, q_inv * k_inv, 0.0)
            ex = jnp.where(valid, jnp.exp(sc - scale * top), 0.0)
            at = ex / jnp.sum(ex, axis=1, keepdims=True)
            hr = pl.ds(HD * h, HD)
            score[hr, :] = sc
            qk_inv[hr, :] = inv
            attn[hr, :] = at
            spread_head(at, rels, h, (a0, a1))

    far = pl.ds(pl.multiple_of(2 * OWN * (1 - chip), 16), 2 * OWN)
    near = pl.ds(pl.multiple_of(2 * OWN * chip, 16), 2 * OWN)
    mine = pl.ds(pl.multiple_of(OWN * core, 8), OWN)

    def part_rows(lhs_t, rows, rhs, part, r1, slot, count=OWN):
        part[slot] = mm(lhs_t[rows, :], rhs)
        theirs = pl.ds(pl.multiple_of(OWN * (1 - core), 8), count)
        return send(part.at[slot, theirs, :], r1.at[slot, pl.ds(0, count), :], sib)

    def cross(cp, part, r1, s, r2, count=OWN):
        cp.wait_recv()
        rows = pl.ds(0, count)
        s[rows, :] = part[0, pl.ds(pl.multiple_of(OWN * core, 8), count), :] + r1[0, rows, :]
        return send(s.at[rows, :], r2.at[rows, :], nbr)

    with jax.named_scope("dv"):
        for i in range(NB):
            rows = block(i)
            dqkv[rows, 2 * C :] = window_mm(do[rows, :], (a0, a1), NN).astype(BF16)
        f_wv = part_rows(ut, far, dqkv[:, 2 * C :], wv_part, wv_r1, 0, OWN - DIRECT)
        d_wv = [
            send(wv_part.at[0, pl.ds(pl.multiple_of(OWN * c + OWN - DIRECT, 8), DIRECT), :], wv_d.at[j], peer)
            for j, (c, peer) in enumerate(((1 - core, diag), (core, nbr)))
        ]
    def step_o(i):
        rows = block(i)
        o[rows, :] = window_mm(v[rows, :], (a0, a1), NT).astype(BF16)
        ot[:, rows] = o[rows, :].T

    with jax.named_scope("o_1"):
        for i in range(NB // 2):
            step_o(i)
    with jax.named_scope("sum_a"):
        ra1[me] = pa[core]
        for cp in s_a1:
            cp.wait_recv()
        sa[core] = (ra1[0] + ra1[1]) + (ra1[2] + ra1[3])
        s_a2 = send(sa.at[core], sa.at[core], sib)
    with jax.named_scope("o_2"):
        for i in range(NB // 2, NB):
            step_o(i)
    with jax.named_scope("cross_wv"):
        x_wv = cross(f_wv, wv_part, wv_r1, wv_s, wv_r2, OWN - DIRECT)
    with jax.named_scope("dwo_far"):
        f_wo = part_rows(ot, far, dy[...], wo_part, wo_r1, 0)

    with jax.named_scope("wait_a"):
        s_a2.wait_recv()
    with jax.named_scope("softmax_bwd"):
        dsum = [jnp.zeros((1, LANES), F32) for _ in range(6)]
        lane = lax.broadcasted_iota(jnp.int32, (1, LANES), 1)
        d_tau = jnp.zeros((1, LANES), F32)
        for h in range(HEADS):
            rel = rels[h]
            valid = rel < HD
            hr = pl.ds(HD * h, HD)
            at = attn[hr, :]
            d_at = jnp.where(valid, packed_head(sa, h), 0.0).astype(BF16).astype(F32)
            d_sc = at * (d_at - jnp.sum(d_at * at, axis=1, keepdims=True))
            d_sc_inv = d_sc * qk_inv[hr, :]
            d_tau_h = jnp.sum(d_sc_inv * jnp.where(valid, packed_head(gfull, h), 0.0), axis=0, keepdims=True)
            d_tau = jnp.where(lane == h, jnp.sum(d_tau_h, axis=1, keepdims=True), d_tau)
            spread_head(d_sc_inv * tau_ref[h], rels, h, (e0, e1))
            wt = d_sc * score[hr, :]
            over_q = jnp.sum(jnp.where(rel == row, jnp.sum(wt, axis=1, keepdims=True), 0.0), axis=0, keepdims=True)
            over_k = jnp.sum(wt, axis=0, keepdims=True)
            for m in segs_of(h):
                mask = seg_mask(rel, h, m)[:1]
                dsum[m] = jnp.where(mask, over_q, dsum[m])
                dsum[3 + m] = jnp.where(mask, over_k, dsum[3 + m])
        dt_ref[...] = d_tau[:, :HEADS].reshape(HEADS)
        for m in range(6):
            dsq[:, pl.ds(LANES * m, LANES)] = -dsum[m] / gfull[pl.ds(PK + m, 1), :]
    with jax.named_scope("dqk"):
        for i in range(NB):
            rows = block(i)
            dqkv[rows, :C] = (
                window_mm(k[rows, :], (e0, e1), NT) + q[rows, :].astype(F32) * dsq[:, :C]).astype(BF16)
            dqkv[rows, C : 2 * C] = (
                window_mm(q[rows, :], (e0, e1), NN) + k[rows, :].astype(F32) * dsq[:, C:]).astype(BF16)
    with jax.named_scope("cross_wo"):
        x_wo = cross(f_wo, wo_part, wo_r1, wo_s, wo_r2)
    with jax.named_scope("dwq_far"):
        f_wq = part_rows(ut, far, dqkv[:, :C], wq_part, wq_r1, 0)
    with jax.named_scope("dwk_far"):
        f_wk = part_rows(ut, far, dqkv[:, C : 2 * C], wk_part, wk_r1, 0)
    with jax.named_scope("near_v"):
        l_wv = part_rows(ut, near, dqkv[:, 2 * C :], wv_part, wv_r1, 1)
    with jax.named_scope("cross_wq"):
        x_wq = cross(f_wq, wq_part, wq_r1, wq_s, wq_r2)
    with jax.named_scope("near_o"):
        l_wo = part_rows(ot, near, dy[...], wo_part, wo_r1, 1)
    with jax.named_scope("cross_wk"):
        x_wk = cross(f_wk, wk_part, wk_r1, wk_s, wk_r2)
    with jax.named_scope("near_qk"):
        l_wq = part_rows(ut, near, dqkv[:, :C], wq_part, wq_r1, 1)
        l_wk = part_rows(ut, near, dqkv[:, C : 2 * C], wk_part, wk_r1, 1)

    gamma = g_ref[...].reshape(1, C)
    dgam = jnp.zeros((8, C), F32)
    dbet = jnp.zeros((8, C), F32)
    with jax.named_scope("ln_bwd"):
        for i in range(NB):
            rows = block(i)
            du[rows, :] = mm(dqkv[rows, :], wqkv[...], NT).astype(BF16)
            for j in range(RB // SB):
                sub = pl.ds(i * RB + j * SB, SB)
                d = du[sub, :].astype(F32)
                xh = xhat[sub, :]
                dxh = d * xh
                dgam += jnp.sum(dxh.reshape(SB // 8, 8, C), axis=0)
                dbet += jnp.sum(d.reshape(SB // 8, 8, C), axis=0)
                dh = d * gamma
                m1 = jnp.mean(dh, axis=-1, keepdims=True)
                m2 = jnp.mean(dxh * gamma, axis=-1, keepdims=True)
                inv = istd[sub, :]
                term = dh - m1 - xh * m2
                dln = term * jnp.concatenate([inv, inv, inv], axis=1)
                dx[sub, :] = (dy[sub, :].astype(F32) + dln).astype(BF16)
        dgb_all[me] = jnp.concatenate(
            [jnp.sum(dgam, axis=0, keepdims=True), jnp.sum(dbet, axis=0, keepdims=True)], axis=1)
    c_dgb = [send(dgb_all.at[me], dgb_all.at[me], peer) for peer in (sib, nbr, diag)]
    with jax.named_scope("y"):
        for i in range(NB):
            rows = block(i)
            y[rows, :] = (x[rows, :].astype(F32) + mm(o[rows, :], wo[...])).astype(BF16)

    assert len(sends) <= N_SENDS
    @pl.when(core == 1)
    def _():
        for cp in s_g2:
            cp.wait_send()

    with jax.named_scope("wait_wo"):
        l_wo.wait_recv()
        x_wo.wait_recv()
        dwo_ref[...] = (wo_part[1, mine, :] + wo_r1[1] + wo_r2[...]).astype(BF16)
    with jax.named_scope("wait_wv"):
        l_wv.wait_recv()
        x_wv.wait_recv()
        for cp in d_wv:
            cp.wait_recv()
        cut = OWN - DIRECT
        near_sum = wv_part[1, mine, :] + wv_r1[1]
        far_sum = jnp.concatenate([wv_r2[pl.ds(0, cut), :], wv_d[0] + wv_d[1]], axis=0)
        dwqkv_ref[:, 2 * C :] = (near_sum + far_sum).astype(BF16)
    with jax.named_scope("wait_wq"):
        l_wq.wait_recv()
        x_wq.wait_recv()
        dwqkv_ref[:, :C] = (wq_part[1, mine, :] + wq_r1[1] + wq_r2[...]).astype(BF16)
    with jax.named_scope("wait_dgb"):
        for cp in c_dgb:
            cp.wait_recv()
        total = dgb_all[0] + dgb_all[1] + dgb_all[2] + dgb_all[3]
        dg_ref[...] = total[:, :C].reshape(C)
        db_ref[...] = total[:, C:].reshape(C)
    with jax.named_scope("wait_wqk"):
        l_wk.wait_recv()
        x_wk.wait_recv()
        dwqkv_ref[:, C : 2 * C] = (wk_part[1, mine, :] + wk_r1[1] + wk_r2[...]).astype(BF16)
    for cp in sends:
        cp.wait_send()


def write_out(*refs):
    ins, outs, sem = refs[:7], refs[7:14], refs[14]
    pairs = []
    for i in range(2):
        for j in range(PIECES):
            rows = pl.ds(j * (TOK // PIECES), TOK // PIECES)
            pairs.append((ins[i].at[rows, :], outs[i].at[rows, :]))
    pairs += [(ins[i], outs[i]) for i in range(2, 7)]
    copies = [pltpu.make_async_copy(src, dst, sem.at[i]) for i, (src, dst) in enumerate(pairs)]
    for cp in copies:
        cp.start()
    for cp in copies:
        cp.wait()


def xca_local(x_rows, dy_rows, ln_gamma, ln_beta, w_qkv, w_out, temperature):
    vm = pltpu.VMEM
    hbm_spec = pl.BlockSpec(memory_space=pltpu.HBM)
    vmem_spec = pl.BlockSpec(memory_space=pltpu.VMEM)
    results = (
        ((TOK, C), BF16), ((TOK, C), BF16), ((OWN, 3 * C), BF16), ((OWN, C), BF16),
        ((C,), F32), ((C,), F32), ((HEADS,), F32),
    )
    rows_bf = vm((TOK, C), BF16)
    cols_bf = vm((C, TOK), BF16)
    win_f = vm((256, 256), F32)
    win_b = vm((256, 256), BF16)
    pk_g = vm((PK + 8, LANES), F32)
    pk_a = vm((2, HALF, LANES), F32)
    fold = vm((C, LANES), F32)
    scratch = [
        rows_bf, rows_bf, vm((C,), F32), vm((C,), F32), vm((C, 3 * C), BF16), vm((C, C), BF16), vm((C, C), BF16),
        pltpu.SMEM((HEADS,), F32), rows_bf, cols_bf, vm((TOK, C), F32), vm((TOK, LANES), F32),
        rows_bf, rows_bf, rows_bf, rows_bf, rows_bf, cols_bf, vm((TOK, 3 * C), BF16), rows_bf,
        win_f, win_f, vm((8, 2 * C), F32), pk_g, pk_g, pk_g, pk_g, pk_a, vm((4, HALF, LANES), F32), pk_a,
        win_b, win_b, win_b, win_b, fold, fold, fold, pk_g, vm((1, 2 * C), F32),
        *[vm((2, 2 * OWN, C), F32)] * 4, *[vm((2, OWN, C), F32)] * 4, *[vm((OWN, C), F32)] * 8, vm((2, DIRECT, C), F32),
        vm((4, 1, 2 * C), F32),
        pltpu.SemaphoreType.DMA((16,)),
        pltpu.SemaphoreType.DMA((N_SENDS + 2,)), pltpu.SemaphoreType.DMA((N_SENDS + 1,)),
    ]
    parts = pl.pallas_call(
        kernel,
        name="xca",
        out_shape=tuple(pltpu.VMEM(shape, dtype) for shape, dtype in results),
        in_specs=[hbm_spec] * 7,
        out_specs=[vmem_spec] * 7,
        scratch_shapes=scratch,
        compiler_params=pltpu.CompilerParams(
            collective_id=0, has_side_effects=True, vmem_limit_bytes=60 * 1024 * 1024),
    )(x_rows, dy_rows, ln_gamma, ln_beta, w_qkv, w_out, temperature)
    return pl.pallas_call(
        write_out,
        name="xca_out",
        out_shape=tuple(jax.ShapeDtypeStruct(shape, dtype) for shape, dtype in results),
        in_specs=[vmem_spec] * 7,
        out_specs=[hbm_spec] * 7,
        scratch_shapes=[pltpu.SemaphoreType.DMA((2 * PIECES + 5,))],
        compiler_params=pltpu.CompilerParams(vmem_limit_bytes=1024 * 1024),
    )(*parts)


def solution(mesh):
    row_spec = P(('dp', 'sp'), None)
    full_mat = P(None, None)
    full_vec = P(None)
    part_vec = P('dp')
    return jax.shard_map(
        xca_local, mesh=mesh,
        in_specs=(row_spec, row_spec, full_vec, full_vec, full_mat, full_mat, full_vec),
        out_specs=(row_spec, row_spec, row_spec, row_spec, part_vec, part_vec, part_vec),
        check_vma=False)
```

```python
import jax
import jax.numpy as jnp
from jax import lax
from jax.experimental import pallas as pl
from jax.experimental.pallas import tpu as pltpu
from jax.sharding import PartitionSpec as P

LN_EPS = 1e-6
F32, BF16 = jnp.float32, jnp.bfloat16
MESH = pl.DeviceIdType.MESH

C = 384
HEADS, HD = 8, 48
LANES = 128
TOK = 2048
RB = 512
NB = TOK // RB
A_BLOCKS = (512, 512, 512, 512)
NA = len(A_BLOCKS)
RV = 256
NV = TOK // RV
CUT = 4
LAG = 3
PIECES = 1
SB = 64
OWN = C // 4
PK = 144
LATE = 32
DIRECT = 16
HALF = PK // 2
W0_HEADS = 5

NN = (((1,), (0,)), ((), ()))
NT = (((1,), (1,)), ((), ()))
TN = (((0,), (0,)), ((), ()))


def mm(a, b, dims=NN):
    return lax.dot_general(a, b, dims, preferred_element_type=F32)


def a_block(i):
    return sum(A_BLOCKS[:i]), A_BLOCKS[i]


def head_rel():
    lane = lax.broadcasted_iota(jnp.int32, (HD, LANES), 1)
    return [(lane - HD * h) & (LANES - 1) for h in range(HEADS)]


def seg_mask(rel, h, m):
    chan = rel + HD * h
    return (rel < HD) & (chan >= LANES * m) & (chan < LANES * (m + 1))


def head_window(h):
    if h < W0_HEADS:
        return 0, HD * h, (0, 1)
    return 1, HD * h - LANES, (1, 2)


def segs_of(h):
    return sorted({(HD * h) // LANES, (HD * h + HD - 1) // LANES})


def spare_lanes(g):
    lane = lax.broadcasted_iota(jnp.int32, (HD, LANES), 1)
    return (lane >= 96 - 32 * g) & (lane < 128 - 32 * g)


def fold_windows(win_refs, out_ref):
    rels = head_rel()

    def put(acc, h, where):
        w, row, segs = head_window(h)
        for s, m in enumerate(segs):
            if m in segs_of(h):
                block = win_refs[w][pl.ds(row, HD), pl.ds(LANES * s, LANES)]
                mask = seg_mask(rels[h], h, m)
                acc = jnp.where(mask if where is None else mask & where, block, acc)
        return acc

    for g in range(3):
        acc = put(put(jnp.zeros((HD, LANES), F32), 2 * g, None), 2 * g + 1, None)
        spare = spare_lanes(g)
        put_rows(out_ref, g, put(put(acc, 6, spare), 7, spare))


def put_rows(ref, g, value):
    if len(ref.shape) == 2:
        ref[pl.ds(HD * g, HD), :] = value
    elif g == 1:
        ref[0, pl.ds(HD, HALF - HD), :] = value[: HALF - HD]
        ref[1, pl.ds(0, HALF - HD), :] = value[HALF - HD :]
    else:
        ref[g // 2, pl.ds((HALF - HD) * (g // 2), HD), :] = value


def get_rows(ref, g):
    if len(ref.shape) == 2:
        return ref[pl.ds(HD * g, HD), :]
    if g == 1:
        return jnp.concatenate([ref[0, pl.ds(HD, HALF - HD), :], ref[1, pl.ds(0, HALF - HD), :]], axis=0)
    return ref[g // 2, pl.ds((HALF - HD) * (g // 2), HD), :]


def packed_head(ref, h):
    if h < 6:
        return get_rows(ref, h // 2)
    lane = lax.broadcasted_iota(jnp.int32, (HD, LANES), 1)
    return jnp.where(lane >= 96, get_rows(ref, 0), jnp.where(lane >= 64, get_rows(ref, 1), get_rows(ref, 2)))


def spread_head(value, rels, h, win_refs):
    w, row, segs = head_window(h)
    parts = []
    for m in segs:
        if m in segs_of(h):
            parts.append(jnp.where(seg_mask(rels[h], h, m), value, 0.0))
        else:
            parts.append(jnp.zeros((HD, LANES), F32))
    win_refs[w][pl.ds(row, HD), :] = jnp.concatenate(parts, axis=1).astype(BF16)


def window_mm(a, win_refs, dims):
    r0 = mm(a[:, :256], win_refs[0][...], dims)
    r1 = mm(a[:, 128:], win_refs[1][...], dims)
    return jnp.concatenate([r0[:, :128], r0[:, 128:] + r1[:, :128], r1[:, 128:]], axis=1)


def kernel(
    x_hbm, dy_hbm, g_hbm, b_hbm, wqkv_hbm, wo_hbm, tau_hbm,
    y, dx, dwqkv_ref, dwo_ref, dg_ref, db_ref, dt_ref,
    x, dy, g_ref, b_ref, wqkv, wo, wot, tau_ref, u, ut, xhat, istd, q, k, v, do, o, ot, dqkv, du,
    g0, g1, sq, pg, rg1, sg, rg2, pa, ra1, sa,
    a0, a1, e0, e1, attn, score, qk_inv, gfull, dsq,
    wo_part, wv_part, wq_part, wk_part, wo_r1, wv_r1, wq_r1, wk_r1,
    wo_s, wv_s, wq_s, wk_s, wo_r2, wv_r2, wq_r2, wk_r2, wv_d,
    dgb_all,
    loc_sem, recv_sem,
):
    me = lax.axis_index("sp")
    core = lax.rem(me, 2)
    chip = me // 2
    sib = me + 1 - 2 * core
    nbr = lax.rem(me + 2, 4)
    diag = lax.rem(sib + 2, 4)

    def load(src, dst, slot):
        cp = pltpu.make_async_copy(src, dst, loc_sem.at[slot])
        cp.start()
        return cp

    def block(i):
        return pl.ds(i * RB, RB)

    n0 = A_BLOCKS[0]
    ld_gb = [load(g_hbm, g_ref, 0), load(b_hbm, b_ref, 1)]
    ld_x0 = load(x_hbm.at[pl.ds(0, n0), :], x.at[pl.ds(0, n0), :], 2)
    ld_wqk = load(wqkv_hbm.at[:, pl.ds(0, 2 * C)], wqkv.at[:, pl.ds(0, 2 * C)], 3)
    ld_x1 = load(x_hbm.at[pl.ds(n0, TOK - n0), :], x.at[pl.ds(n0, TOK - n0), :], 4)
    ld_wo = load(wo_hbm, wo, 5)
    ld_wv = load(wqkv_hbm.at[:, pl.ds(2 * C, C)], wqkv.at[:, pl.ds(2 * C, C)], 6)
    ld_dy = load(dy_hbm, dy, 7)
    ld_tau = load(tau_hbm, tau_ref, 8)

    barrier = pltpu.get_barrier_semaphore()
    for peer in (sib, nbr, diag):
        pl.semaphore_signal(barrier, inc=1, device_id={"sp": peer}, device_id_type=MESH)

    busy = {}

    def remote(src, dst, peer, slot, got):
        return pltpu.make_async_remote_copy(
            src_ref=src, dst_ref=dst, send_sem=loc_sem.at[slot], recv_sem=recv_sem.at[got],
            device_id={"sp": peer}, device_id_type=MESH)

    def send(src, dst, peer, slot, got):
        if slot in busy:
            busy[slot].wait_send()
        cp = remote(src, dst, peer, slot, got)
        cp.start()
        busy[slot] = cp
        return cp

    def await_bytes(ref, got):
        remote(ref, ref, sib, 0, got).wait_recv()

    def step_ln(i):
        gamma = g_ref[...].reshape(1, C)
        beta = b_ref[...].reshape(1, C)
        lo, size = a_block(i)
        for j in range(size // SB):
            rows = pl.ds(lo + j * SB, SB)
            xf = x[rows, :].astype(F32)
            cen = xf - jnp.mean(xf, axis=-1, keepdims=True)
            inv = lax.rsqrt(jnp.mean(cen * cen, axis=-1, keepdims=True) + LN_EPS)
            xh = cen * inv
            xhat[rows, :] = xh
            istd[rows, :] = jnp.broadcast_to(inv, (SB, LANES))
            u[rows, :] = (xh * gamma + beta).astype(BF16)

    def step_qk(i):
        lo, size = a_block(i)
        rows = pl.ds(lo, size)
        qk = mm(u[rows, :], wqkv[:, : 2 * C]).astype(BF16)
        q[rows, :] = qk[:, :C]
        k[rows, :] = qk[:, C:]

    def step_gram(i):
        lo, size = a_block(i)
        rows = pl.ds(lo, size)
        p0 = mm(q[rows, :256], k[rows, :256], TN)
        p1 = mm(q[rows, 128:], k[rows, 128:], TN)
        if i == 0:
            g0[...], g1[...] = p0, p1
        else:
            g0[...] += p0
            g1[...] += p1
        for r, c0 in ((q, 0), (k, C)):
            part = jnp.zeros((8, C), F32)
            for j in range(size // SB):
                f = r[pl.ds(lo + j * SB, SB), :].astype(F32)
                part += jnp.sum((f * f).reshape(SB // 8, 8, C), axis=0)
            if i == 0:
                sq[:, pl.ds(c0, C)] = part
            else:
                sq[:, pl.ds(c0, C)] += part

    with jax.named_scope("ln_0"):
        ld_x0.wait()
        for cp in ld_gb:
            cp.wait()
        step_ln(0)
    ld_wqk.wait()
    ld_x1.wait()
    with jax.named_scope("ln_qk"):
        for i in range(1, NA + 2):
            if i < NA:
                step_ln(i)
            if 1 <= i <= NA:
                step_qk(i - 1)
            if i >= 2:
                step_gram(i - 2)
    with jax.named_scope("fold_g"):
        fold_windows((g0, g1), pg)
        sums = jnp.sum(sq[...], axis=0, keepdims=True)
        for m in range(6):
            pg[pl.ds(PK + m, 1), :] = sums[:, LANES * m : LANES * (m + 1)]
        pg[pl.ds(PK + 6, 2), :] = jnp.zeros((2, LANES), F32)
    with jax.named_scope("greet"):
        pl.semaphore_wait(barrier, 3)
    s_g1 = send(pg, rg1, sib, 0, 0)

    def step_b(i):
        rows = pl.ds(i * RV, RV)
        v[rows, :] = mm(u[rows, :], wqkv[:, 2 * C :]).astype(BF16)
        do[rows, :] = mm(dy[rows, :], wot[...]).astype(BF16)

    def step_da(i):
        rows = pl.ds(i * RV, RV)
        p0 = mm(do[rows, :256], v[rows, :256], TN)
        p1 = mm(do[rows, 128:], v[rows, 128:], TN)
        if i == 0:
            g0[...], g1[...] = p0, p1
        else:
            g0[...] += p0
            g1[...] += p1

    with jax.named_scope("v_do_1"):
        ld_wo.wait()
        ld_wv.wait()
        ld_dy.wait()
        ld_tau.wait()
        wot[...] = wo[...].T
        for i in range(CUT):
            step_b(i)
        for i in range(NB):
            ut[:, block(i)] = u[block(i), :].T
    with jax.named_scope("sum_g"):
        s_g1.wait_recv()
        sg[...] = pg[...] + rg1[...]
        s_g2 = [remote(sg, rg2, peer, 1 + j, 1) for j, peer in enumerate((diag, nbr))]

        @pl.when(core == 1)
        def _():
            for cp in s_g2:
                cp.start()
    with jax.named_scope("v_do_2"):
        for i in range(CUT, NV):
            step_b(i)
            for j in range(max(0, i - LAG) if i > CUT else 0, i + 1 - LAG):
                step_da(j)
        for i in range(NV - LAG, NV):
            step_da(i)
    with jax.named_scope("fold_a"):
        fold_windows((g0, g1), pa)
        send(pa.at[1 - core], ra1.at[me], sib, 3, 2)
        send(pa.at[core], ra1.at[me], nbr, 4, 2)
        send(pa.at[1 - core], ra1.at[me], diag, 5, 2)

    with jax.named_scope("wait_g"):
        s_g2[0].wait_recv()
    rels = head_rel()
    row = lax.broadcasted_iota(jnp.int32, (HD, LANES), 0)
    with jax.named_scope("softmax"):
        gfull[...] = sg[...] + rg2[...]
        for ref in (a0, a1, e0, e1):
            ref[...] = jnp.zeros_like(ref)
        for h in range(HEADS):
            rel = rels[h]
            valid = rel < HD
            tau = tau_ref[h]
            s_q = jnp.zeros((HD, LANES), F32)
            s_k = jnp.ones((HD, LANES), F32)
            for m in segs_of(h):
                mask = seg_mask(rel, h, m)
                s_q = jnp.where(mask, gfull[pl.ds(PK + m, 1), :], s_q)
                s_k = jnp.where(mask, gfull[pl.ds(PK + 3 + m, 1), :], s_k)
            q_inv = lax.rsqrt(jnp.sum(jnp.where(rel == row, s_q, 0.0), axis=1, keepdims=True))
            k_inv = lax.rsqrt(s_k)
            by_k = packed_head(gfull, h) * k_inv
            top = jnp.max(jnp.where(valid, by_k, -jnp.inf), axis=1, keepdims=True)
            scale = tau * q_inv
            sc = jnp.where(valid, scale * by_k, 0.0)
            inv = jnp.where(valid, q_inv * k_inv, 0.0)
            ex = jnp.where(valid, jnp.exp(sc - scale * top), 0.0)
            at = ex / jnp.sum(ex, axis=1, keepdims=True)
            hr = pl.ds(HD * h, HD)
            score[hr, :] = sc
            qk_inv[hr, :] = inv
            attn[hr, :] = at
            spread_head(at, rels, h, (a0, a1))

    far = pl.ds(pl.multiple_of(2 * OWN * (1 - chip), 16), 2 * OWN)
    near = pl.ds(pl.multiple_of(2 * OWN * chip, 16), 2 * OWN)
    mine = pl.ds(pl.multiple_of(OWN * core, 8), OWN)

    def part_rows(lhs_t, rows, rhs, part, r1, half, sem, got, count=OWN):
        part[half] = mm(lhs_t[rows, :], rhs)
        theirs = pl.ds(pl.multiple_of(OWN * (1 - core), 8), count)
        return send(part.at[half, theirs, :], r1.at[half, pl.ds(0, count), :], sib, sem, got)

    def cross(cp, part, r1, s, r2, sem, got, count=OWN, first=0):
        if cp is not None:
            cp.wait_recv()
        rows = pl.ds(first, count)
        s[rows, :] = part[0, pl.ds(pl.multiple_of(OWN * core + first, 8), count), :] + r1[0, rows, :]
        send(s.at[rows, :], r2.at[rows, :], nbr, sem, got)

    with jax.named_scope("dv"):
        for i in range(NB):
            rows = block(i)
            dqkv[rows, 2 * C :] = window_mm(do[rows, :], (a0, a1), NN).astype(BF16)
        f_wv = part_rows(ut, far, dqkv[:, 2 * C :], wv_part, wv_r1, 0, 0, 3, OWN - DIRECT)
        @pl.when(core == 1)
        def _():
            for cp in s_g2:
                cp.wait_send()

        for j, (c, peer) in enumerate(((1 - core, diag), (core, nbr))):
            rows = pl.ds(pl.multiple_of(OWN * c + OWN - DIRECT, 8), DIRECT)
            send(wv_part.at[0, rows, :], wv_d.at[j], peer, 1 + j, 4)

    def step_o(i):
        rows = block(i)
        o[rows, :] = window_mm(v[rows, :], (a0, a1), NT).astype(BF16)

    with jax.named_scope("o_1"):
        for i in range(NB // 2):
            step_o(i)
    with jax.named_scope("sum_a"):
        ra1[me] = pa[core]
        await_bytes(ra1.at[pl.ds(0, 3)], 2)
        sa[core] = (ra1[0] + ra1[1]) + (ra1[2] + ra1[3])
        s_a2 = send(sa.at[core], sa.at[core], sib, 3, 5)
    with jax.named_scope("o_2"):
        for i in range(NB // 2, NB):
            step_o(i)
    with jax.named_scope("cross_wv"):
        cross(f_wv, wv_part, wv_r1, wv_s, wv_r2, 6, 10, OWN - DIRECT)
    with jax.named_scope("dwo_far"):
        for i in range(NB):
            ot[:, block(i)] = o[block(i), :].T
        f_wo = part_rows(ot, far, dy[...], wo_part, wo_r1, 0, 0, 6)

    with jax.named_scope("wait_a"):
        s_a2.wait_recv()
    with jax.named_scope("softmax_bwd"):
        dsum = [jnp.zeros((1, LANES), F32) for _ in range(6)]
        lane = lax.broadcasted_iota(jnp.int32, (1, LANES), 1)
        d_tau = jnp.zeros((1, LANES), F32)
        for h in range(HEADS):
            rel = rels[h]
            valid = rel < HD
            hr = pl.ds(HD * h, HD)
            at = attn[hr, :]
            d_at = jnp.where(valid, packed_head(sa, h), 0.0).astype(BF16).astype(F32)
            d_sc = at * (d_at - jnp.sum(d_at * at, axis=1, keepdims=True))
            d_sc_inv = d_sc * qk_inv[hr, :]
            d_tau_h = jnp.sum(d_sc_inv * jnp.where(valid, packed_head(gfull, h), 0.0), axis=0, keepdims=True)
            d_tau = jnp.where(lane == h, jnp.sum(d_tau_h, axis=1, keepdims=True), d_tau)
            spread_head(d_sc_inv * tau_ref[h], rels, h, (e0, e1))
            wt = d_sc * score[hr, :]
            over_q = jnp.sum(jnp.where(rel == row, jnp.sum(wt, axis=1, keepdims=True), 0.0), axis=0, keepdims=True)
            over_k = jnp.sum(wt, axis=0, keepdims=True)
            for m in segs_of(h):
                mask = seg_mask(rel, h, m)[:1]
                dsum[m] = jnp.where(mask, over_q, dsum[m])
                dsum[3 + m] = jnp.where(mask, over_k, dsum[3 + m])
        dt_ref[...] = d_tau[:, :HEADS].reshape(HEADS)
        for m in range(6):
            dsq[:, pl.ds(LANES * m, LANES)] = -dsum[m] / gfull[pl.ds(PK + m, 1), :]
    with jax.named_scope("dqk"):
        for i in range(NB):
            rows = block(i)
            dqkv[rows, :C] = (
                window_mm(k[rows, :], (e0, e1), NT) + q[rows, :].astype(F32) * dsq[:, :C]).astype(BF16)
            dqkv[rows, C : 2 * C] = (
                window_mm(q[rows, :], (e0, e1), NN) + k[rows, :].astype(F32) * dsq[:, C:]).astype(BF16)
    with jax.named_scope("cross_wo"):
        cross(f_wo, wo_part, wo_r1, wo_s, wo_r2, 7, 10)
    with jax.named_scope("dwq_far"):
        f_wq = part_rows(ut, far, dqkv[:, :C], wq_part, wq_r1, 0, 3, 7)
    with jax.named_scope("dwk_far"):
        f_wk = part_rows(ut, far, dqkv[:, C : 2 * C], wk_part, wk_r1, 0, 0, 8)
    with jax.named_scope("near_v"):
        part_rows(ut, near, dqkv[:, 2 * C :], wv_part, wv_r1, 1, 8, 9)
    with jax.named_scope("cross_wq"):
        cross(f_wq, wq_part, wq_r1, wq_s, wq_r2, 4, 10)
    with jax.named_scope("near_o"):
        part_rows(ot, near, dy[...], wo_part, wo_r1, 1, 3, 9)
    with jax.named_scope("cross_wk"):
        cross(f_wk, wk_part, wk_r1, wk_s, wk_r2, 5, 11, OWN - LATE)
    with jax.named_scope("near_qk"):
        part_rows(ut, near, dqkv[:, :C], wq_part, wq_r1, 1, 0, 9)
        part_rows(ut, near, dqkv[:, C : 2 * C], wk_part, wk_r1, 1, 8, 9)

    gamma = g_ref[...].reshape(1, C)
    dgam = jnp.zeros((8, C), F32)
    dbet = jnp.zeros((8, C), F32)
    with jax.named_scope("ln_bwd"):
        for i in range(NB):
            rows = block(i)
            du[rows, :] = mm(dqkv[rows, :], wqkv[...], NT).astype(BF16)
            for j in range(RB // SB):
                sub = pl.ds(i * RB + j * SB, SB)
                d = du[sub, :].astype(F32)
                xh = xhat[sub, :]
                dxh = d * xh
                dgam += jnp.sum(dxh.reshape(SB // 8, 8, C), axis=0)
                dbet += jnp.sum(d.reshape(SB // 8, 8, C), axis=0)
                dh = d * gamma
                m1 = jnp.mean(dh, axis=-1, keepdims=True)
                m2 = jnp.mean(dxh * gamma, axis=-1, keepdims=True)
                inv = istd[sub, :]
                term = dh - m1 - xh * m2
                dln = term * jnp.concatenate([inv, inv, inv], axis=1)
                dx[sub, :] = (dy[sub, :].astype(F32) + dln).astype(BF16)
        dgb_all[me] = jnp.concatenate(
            [jnp.sum(dgam, axis=0, keepdims=True), jnp.sum(dbet, axis=0, keepdims=True)], axis=1)
    for j, peer in enumerate((nbr, diag, sib)):
        send(dgb_all.at[me], dgb_all.at[me], peer, 1 + j, 12)
    cross(None, wk_part, wk_r1, wk_s, wk_r2, 6, 11, LATE, OWN - LATE)
    with jax.named_scope("y"):
        for i in range(NB):
            rows = block(i)
            y[rows, :] = (x[rows, :].astype(F32) + mm(o[rows, :], wo[...])).astype(BF16)

    def rows_of(n):
        return xhat.at[pl.ds(0, n), :]

    with jax.named_scope("wait_wq"):
        await_bytes(rows_of(4 * OWN), 9)
        await_bytes(wv_d, 4)
        await_bytes(rows_of(3 * OWN - DIRECT), 10)
        dwo_ref[...] = (wo_part[1, mine, :] + wo_r1[1] + wo_r2[...]).astype(BF16)
        dwqkv_ref[:, :C] = (wq_part[1, mine, :] + wq_r1[1] + wq_r2[...]).astype(BF16)
        cut = OWN - DIRECT
        near_sum = wv_part[1, mine, :] + wv_r1[1]
        far_sum = jnp.concatenate([wv_r2[pl.ds(0, cut), :], wv_d[0] + wv_d[1]], axis=0)
        dwqkv_ref[:, 2 * C :] = (near_sum + far_sum).astype(BF16)
    with jax.named_scope("wait_dgb"):
        await_bytes(dgb_all.at[pl.ds(0, 3)], 12)
        total = dgb_all[0] + dgb_all[1] + dgb_all[2] + dgb_all[3]
        dg_ref[...] = total[:, :C].reshape(C)
        db_ref[...] = total[:, C:].reshape(C)
    with jax.named_scope("wait_wqk"):
        await_bytes(rows_of(OWN), 11)
        dwqkv_ref[:, C : 2 * C] = (wk_part[1, mine, :] + wk_r1[1] + wk_r2[...]).astype(BF16)
    with jax.named_scope("sends"):
        for cp in busy.values():
            cp.wait_send()


def write_out(*refs):
    ins, outs, sem = refs[:7], refs[7:14], refs[14]
    pairs = []
    for i in range(2):
        for j in range(PIECES):
            rows = pl.ds(j * (TOK // PIECES), TOK // PIECES)
            pairs.append((ins[i].at[rows, :], outs[i].at[rows, :]))
    pairs += [(ins[i], outs[i]) for i in range(2, 7)]
    copies = [pltpu.make_async_copy(src, dst, sem.at[i]) for i, (src, dst) in enumerate(pairs)]
    for cp in copies:
        cp.start()
    for cp in copies:
        cp.wait()


def xca_local(x_rows, dy_rows, ln_gamma, ln_beta, w_qkv, w_out, temperature):
    vm = pltpu.VMEM
    hbm_spec = pl.BlockSpec(memory_space=pltpu.HBM)
    vmem_spec = pl.BlockSpec(memory_space=pltpu.VMEM)
    results = (
        ((TOK, C), BF16), ((TOK, C), BF16), ((OWN, 3 * C), BF16), ((OWN, C), BF16),
        ((C,), F32), ((C,), F32), ((HEADS,), F32),
    )
    rows_bf = vm((TOK, C), BF16)
    cols_bf = vm((C, TOK), BF16)
    win_f = vm((256, 256), F32)
    win_b = vm((256, 256), BF16)
    pk_g = vm((PK + 8, LANES), F32)
    pk_a = vm((2, HALF, LANES), F32)
    fold = vm((C, LANES), F32)
    scratch = [
        rows_bf, rows_bf, vm((C,), F32), vm((C,), F32), vm((C, 3 * C), BF16), vm((C, C), BF16), vm((C, C), BF16),
        pltpu.SMEM((HEADS,), F32), rows_bf, cols_bf, vm((TOK, C), F32), vm((TOK, LANES), F32),
        rows_bf, rows_bf, rows_bf, rows_bf, rows_bf, cols_bf, vm((TOK, 3 * C), BF16), rows_bf,
        win_f, win_f, vm((8, 2 * C), F32), pk_g, pk_g, pk_g, pk_g, pk_a, vm((4, HALF, LANES), F32), pk_a,
        win_b, win_b, win_b, win_b, fold, fold, fold, pk_g, vm((1, 2 * C), F32),
        *[vm((2, 2 * OWN, C), F32)] * 4, *[vm((2, OWN, C), F32)] * 4, *[vm((OWN, C), F32)] * 8, vm((2, DIRECT, C), F32),
        vm((4, 1, 2 * C), F32),
        pltpu.SemaphoreType.DMA((9,)), pltpu.SemaphoreType.DMA((13,)),
    ]
    parts = pl.pallas_call(
        kernel,
        name="xca",
        out_shape=tuple(pltpu.VMEM(shape, dtype) for shape, dtype in results),
        in_specs=[hbm_spec] * 7,
        out_specs=[vmem_spec] * 7,
        scratch_shapes=scratch,
        compiler_params=pltpu.CompilerParams(
            collective_id=0, has_side_effects=True, vmem_limit_bytes=60 * 1024 * 1024),
    )(x_rows, dy_rows, ln_gamma, ln_beta, w_qkv, w_out, temperature)
    return pl.pallas_call(
        write_out,
        name="xca_out",
        out_shape=tuple(jax.ShapeDtypeStruct(shape, dtype) for shape, dtype in results),
        in_specs=[vmem_spec] * 7,
        out_specs=[hbm_spec] * 7,
        scratch_shapes=[pltpu.SemaphoreType.DMA((2 * PIECES + 5,))],
        compiler_params=pltpu.CompilerParams(vmem_limit_bytes=1024 * 1024),
    )(*parts)


def solution(mesh):
    row_spec = P(('dp', 'sp'), None)
    full_mat = P(None, None)
    full_vec = P(None)
    part_vec = P('dp')
    return jax.shard_map(
        xca_local, mesh=mesh,
        in_specs=(row_spec, row_spec, full_vec, full_vec, full_mat, full_mat, full_vec),
        out_specs=(row_spec, row_spec, row_spec, row_spec, part_vec, part_vec, part_vec),
        check_vma=False)
```

```python
import jax
import jax.numpy as jnp
from jax import lax
from jax.experimental import pallas as pl
from jax.experimental.pallas import tpu as pltpu
from jax.sharding import PartitionSpec as P

LN_EPS = 1e-6
F32, BF16 = jnp.float32, jnp.bfloat16
MESH = pl.DeviceIdType.MESH

C = 384
HEADS, HD = 8, 48
LANES = 128
TOK = 2048
RB = 512
NB = TOK // RB
A_BLOCKS = (512, 512, 512, 512)
NA = len(A_BLOCKS)
RV = 256
NV = TOK // RV
CUT = 4
LAG = 3
PIECES = 1
SB = 64
OWN = C // 4
PK = 144
LATE = 48
MOVE = 40
DIRECT = 16
HALF = PK // 2
W0_HEADS = 5

NN = (((1,), (0,)), ((), ()))
NT = (((1,), (1,)), ((), ()))
TN = (((0,), (0,)), ((), ()))


def mm(a, b, dims=NN):
    return lax.dot_general(a, b, dims, preferred_element_type=F32)


def a_block(i):
    return sum(A_BLOCKS[:i]), A_BLOCKS[i]


def head_rel():
    lane = lax.broadcasted_iota(jnp.int32, (HD, LANES), 1)
    return [(lane - HD * h) & (LANES - 1) for h in range(HEADS)]


def seg_mask(rel, h, m):
    chan = rel + HD * h
    return (rel < HD) & (chan >= LANES * m) & (chan < LANES * (m + 1))


def head_window(h):
    if h < W0_HEADS:
        return 0, HD * h, (0, 1)
    return 1, HD * h - LANES, (1, 2)


def segs_of(h):
    return sorted({(HD * h) // LANES, (HD * h + HD - 1) // LANES})


def spare_lanes(g):
    lane = lax.broadcasted_iota(jnp.int32, (HD, LANES), 1)
    return (lane >= 96 - 32 * g) & (lane < 128 - 32 * g)


def fold_windows(win_refs, out_ref):
    rels = head_rel()

    def put(acc, h, where):
        w, row, segs = head_window(h)
        for s, m in enumerate(segs):
            if m in segs_of(h):
                block = win_refs[w][pl.ds(row, HD), pl.ds(LANES * s, LANES)]
                mask = seg_mask(rels[h], h, m)
                acc = jnp.where(mask if where is None else mask & where, block, acc)
        return acc

    for g in range(3):
        acc = put(put(jnp.zeros((HD, LANES), F32), 2 * g, None), 2 * g + 1, None)
        spare = spare_lanes(g)
        put_rows(out_ref, g, put(put(acc, 6, spare), 7, spare))


def put_rows(ref, g, value):
    if len(ref.shape) == 2:
        ref[pl.ds(HD * g, HD), :] = value
    elif g == 1:
        ref[0, pl.ds(HD, HALF - HD), :] = value[: HALF - HD]
        ref[1, pl.ds(0, HALF - HD), :] = value[HALF - HD :]
    else:
        ref[g // 2, pl.ds((HALF - HD) * (g // 2), HD), :] = value


def get_rows(ref, g):
    if len(ref.shape) == 2:
        return ref[pl.ds(HD * g, HD), :]
    if g == 1:
        return jnp.concatenate([ref[0, pl.ds(HD, HALF - HD), :], ref[1, pl.ds(0, HALF - HD), :]], axis=0)
    return ref[g // 2, pl.ds((HALF - HD) * (g // 2), HD), :]


def packed_head(ref, h):
    if h < 6:
        return get_rows(ref, h // 2)
    lane = lax.broadcasted_iota(jnp.int32, (HD, LANES), 1)
    return jnp.where(lane >= 96, get_rows(ref, 0), jnp.where(lane >= 64, get_rows(ref, 1), get_rows(ref, 2)))


def spread_head(value, rels, h, win_refs):
    w, row, segs = head_window(h)
    parts = []
    for m in segs:
        if m in segs_of(h):
            parts.append(jnp.where(seg_mask(rels[h], h, m), value, 0.0))
        else:
            parts.append(jnp.zeros((HD, LANES), F32))
    win_refs[w][pl.ds(row, HD), :] = jnp.concatenate(parts, axis=1).astype(BF16)


def window_mm(a, win_refs, dims):
    r0 = mm(a[:, :256], win_refs[0][...], dims)
    r1 = mm(a[:, 128:], win_refs[1][...], dims)
    return jnp.concatenate([r0[:, :128], r0[:, 128:] + r1[:, :128], r1[:, 128:]], axis=1)


def kernel(
    x_hbm, dy_hbm, g_hbm, b_hbm, wqkv_hbm, wo_hbm, tau_hbm,
    y, dx, dwqkv_ref, dwo_ref, dg_ref, db_ref, dt_ref,
    x, dy, g_ref, b_ref, wqkv, wo, wot, tau_ref, u, ut, xhat, istd, q, k, v, do, o, ot, dqkv, du,
    g0, g1, sq, pg, rg1, sg, rg2, pa, ra1, sa,
    a0, a1, e0, e1, attn, score, qk_inv, gfull, dsq,
    wo_part, wv_part, wq_part, wk_part, wo_r1, wv_r1, wq_r1, wk_r1,
    wo_s, wv_s, wq_s, wk_s, wo_r2, wv_r2, wq_r2, wk_r2, wv_d, wk_x, wk_m,
    dgb_all,
    loc_sem, recv_sem,
):
    me = lax.axis_index("sp")
    core = lax.rem(me, 2)
    chip = me // 2
    sib = me + 1 - 2 * core
    nbr = lax.rem(me + 2, 4)
    diag = lax.rem(sib + 2, 4)

    def load(src, dst, slot):
        cp = pltpu.make_async_copy(src, dst, loc_sem.at[slot])
        cp.start()
        return cp

    def block(i):
        return pl.ds(i * RB, RB)

    n0 = A_BLOCKS[0]
    ld_gb = [load(g_hbm, g_ref, 0), load(b_hbm, b_ref, 1)]
    ld_x0 = load(x_hbm.at[pl.ds(0, n0), :], x.at[pl.ds(0, n0), :], 2)
    ld_wqk = load(wqkv_hbm.at[:, pl.ds(0, 2 * C)], wqkv.at[:, pl.ds(0, 2 * C)], 3)
    ld_x1 = load(x_hbm.at[pl.ds(n0, TOK - n0), :], x.at[pl.ds(n0, TOK - n0), :], 4)
    ld_wo = load(wo_hbm, wo, 5)
    ld_wv = load(wqkv_hbm.at[:, pl.ds(2 * C, C)], wqkv.at[:, pl.ds(2 * C, C)], 6)
    ld_dy = load(dy_hbm, dy, 7)
    ld_tau = load(tau_hbm, tau_ref, 8)

    barrier = pltpu.get_barrier_semaphore()
    for peer in (sib, nbr, diag):
        pl.semaphore_signal(barrier, inc=1, device_id={"sp": peer}, device_id_type=MESH)

    busy = {}

    def remote(src, dst, peer, slot, got):
        return pltpu.make_async_remote_copy(
            src_ref=src, dst_ref=dst, send_sem=loc_sem.at[slot], recv_sem=recv_sem.at[got],
            device_id={"sp": peer}, device_id_type=MESH)

    def send(src, dst, peer, slot, got):
        if slot in busy:
            busy[slot].wait_send()
        cp = remote(src, dst, peer, slot, got)
        cp.start()
        busy[slot] = cp
        return cp

    def await_bytes(ref, got):
        remote(ref, ref, sib, 0, got).wait_recv()

    def step_ln(i):
        gamma = g_ref[...].reshape(1, C)
        beta = b_ref[...].reshape(1, C)
        lo, size = a_block(i)
        for j in range(size // SB):
            rows = pl.ds(lo + j * SB, SB)
            xf = x[rows, :].astype(F32)
            cen = xf - jnp.mean(xf, axis=-1, keepdims=True)
            inv = lax.rsqrt(jnp.mean(cen * cen, axis=-1, keepdims=True) + LN_EPS)
            xh = cen * inv
            xhat[rows, :] = xh
            istd[rows, :] = jnp.broadcast_to(inv, (SB, LANES))
            u[rows, :] = (xh * gamma + beta).astype(BF16)

    def step_qk(i):
        lo, size = a_block(i)
        rows = pl.ds(lo, size)
        qk = mm(u[rows, :], wqkv[:, : 2 * C]).astype(BF16)
        q[rows, :] = qk[:, :C]
        k[rows, :] = qk[:, C:]

    def step_gram(i):
        lo, size = a_block(i)
        rows = pl.ds(lo, size)
        p0 = mm(q[rows, :256], k[rows, :256], TN)
        p1 = mm(q[rows, 128:], k[rows, 128:], TN)
        if i == 0:
            g0[...], g1[...] = p0, p1
        else:
            g0[...] += p0
            g1[...] += p1
        for r, c0 in ((q, 0), (k, C)):
            part = jnp.zeros((8, C), F32)
            for j in range(size // SB):
                f = r[pl.ds(lo + j * SB, SB), :].astype(F32)
                part += jnp.sum((f * f).reshape(SB // 8, 8, C), axis=0)
            if i == 0:
                sq[:, pl.ds(c0, C)] = part
            else:
                sq[:, pl.ds(c0, C)] += part

    with jax.named_scope("ln_0"):
        ld_x0.wait()
        for cp in ld_gb:
            cp.wait()
        step_ln(0)
    ld_wqk.wait()
    ld_x1.wait()
    with jax.named_scope("ln_qk"):
        for i in range(1, NA + 2):
            if i < NA:
                step_ln(i)
            if 1 <= i <= NA:
                step_qk(i - 1)
            if i >= 2:
                step_gram(i - 2)
    with jax.named_scope("fold_g"):
        fold_windows((g0, g1), pg)
        sums = jnp.sum(sq[...], axis=0, keepdims=True)
        for m in range(6):
            pg[pl.ds(PK + m, 1), :] = sums[:, LANES * m : LANES * (m + 1)]
        pg[pl.ds(PK + 6, 2), :] = jnp.zeros((2, LANES), F32)
    with jax.named_scope("greet"):
        pl.semaphore_wait(barrier, 3)
    s_g1 = send(pg, rg1, sib, 0, 0)

    def step_b(i):
        rows = pl.ds(i * RV, RV)
        v[rows, :] = mm(u[rows, :], wqkv[:, 2 * C :]).astype(BF16)
        do[rows, :] = mm(dy[rows, :], wot[...]).astype(BF16)

    def step_da(i):
        rows = pl.ds(i * RV, RV)
        p0 = mm(do[rows, :256], v[rows, :256], TN)
        p1 = mm(do[rows, 128:], v[rows, 128:], TN)
        if i == 0:
            g0[...], g1[...] = p0, p1
        else:
            g0[...] += p0
            g1[...] += p1

    with jax.named_scope("v_do_1"):
        ld_wo.wait()
        ld_wv.wait()
        ld_dy.wait()
        ld_tau.wait()
        wot[...] = wo[...].T
        for i in range(CUT):
            step_b(i)
        for i in range(NB):
            ut[:, block(i)] = u[block(i), :].T
    with jax.named_scope("sum_g"):
        s_g1.wait_recv()
        sg[...] = pg[...] + rg1[...]
        s_g2 = [remote(sg, rg2, peer, 1 + j, 1) for j, peer in enumerate((diag, nbr))]

        @pl.when(core == 1)
        def _():
            for cp in s_g2:
                cp.start()
    with jax.named_scope("v_do_2"):
        for i in range(CUT, NV):
            step_b(i)
            for j in range(max(0, i - LAG) if i > CUT else 0, i + 1 - LAG):
                step_da(j)
        for i in range(NV - LAG, NV):
            step_da(i)
    with jax.named_scope("fold_a"):
        fold_windows((g0, g1), pa)
        send(pa.at[1 - core], ra1.at[me], sib, 3, 2)
        send(pa.at[core], ra1.at[me], nbr, 4, 2)
        send(pa.at[1 - core], ra1.at[me], diag, 5, 2)

    with jax.named_scope("wait_g"):
        s_g2[0].wait_recv()
    rels = head_rel()
    row = lax.broadcasted_iota(jnp.int32, (HD, LANES), 0)
    with jax.named_scope("softmax"):
        gfull[...] = sg[...] + rg2[...]
        for ref in (a0, a1, e0, e1):
            ref[...] = jnp.zeros_like(ref)
        for h in range(HEADS):
            rel = rels[h]
            valid = rel < HD
            tau = tau_ref[h]
            s_q = jnp.zeros((HD, LANES), F32)
            s_k = jnp.ones((HD, LANES), F32)
            for m in segs_of(h):
                mask = seg_mask(rel, h, m)
                s_q = jnp.where(mask, gfull[pl.ds(PK + m, 1), :], s_q)
                s_k = jnp.where(mask, gfull[pl.ds(PK + 3 + m, 1), :], s_k)
            q_inv = lax.rsqrt(jnp.sum(jnp.where(rel == row, s_q, 0.0), axis=1, keepdims=True))
            k_inv = lax.rsqrt(s_k)
            by_k = packed_head(gfull, h) * k_inv
            top = jnp.max(jnp.where(valid, by_k, -jnp.inf), axis=1, keepdims=True)
            scale = tau * q_inv
            sc = jnp.where(valid, scale * by_k, 0.0)
            inv = jnp.where(valid, q_inv * k_inv, 0.0)
            ex = jnp.where(valid, jnp.exp(sc - scale * top), 0.0)
            at = ex / jnp.sum(ex, axis=1, keepdims=True)
            hr = pl.ds(HD * h, HD)
            score[hr, :] = sc
            qk_inv[hr, :] = inv
            attn[hr, :] = at
            spread_head(at, rels, h, (a0, a1))

    far = pl.ds(pl.multiple_of(2 * OWN * (1 - chip), 16), 2 * OWN)
    near = pl.ds(pl.multiple_of(2 * OWN * chip, 16), 2 * OWN)
    mine = pl.ds(pl.multiple_of(OWN * core, 8), OWN)

    def part_rows(lhs_t, rows, rhs, part, r1, half, sem, got, count=OWN):
        part[half] = mm(lhs_t[rows, :], rhs)
        theirs = pl.ds(pl.multiple_of(OWN * (1 - core), 8), count)
        return send(part.at[half, theirs, :], r1.at[half, pl.ds(0, count), :], sib, sem, got)

    def cross(cp, part, r1, s, r2, sem, got, count=OWN):
        cp.wait_recv()
        rows = pl.ds(0, count)
        s[rows, :] = part[0, pl.ds(pl.multiple_of(OWN * core, 8), count), :] + r1[0, rows, :]
        send(s.at[rows, :], r2.at[rows, :], nbr, sem, got)

    with jax.named_scope("dv"):
        for i in range(NB):
            rows = block(i)
            dqkv[rows, 2 * C :] = window_mm(do[rows, :], (a0, a1), NN).astype(BF16)
        f_wv = part_rows(ut, far, dqkv[:, 2 * C :], wv_part, wv_r1, 0, 0, 3, OWN - DIRECT)
        @pl.when(core == 1)
        def _():
            for cp in s_g2:
                cp.wait_send()

        for j, (c, peer) in enumerate(((1 - core, diag), (core, nbr))):
            rows = pl.ds(pl.multiple_of(OWN * c + OWN - DIRECT, 8), DIRECT)
            send(wv_part.at[0, rows, :], wv_d.at[j], peer, 1 + j, 4)

    def step_o(i):
        rows = block(i)
        o[rows, :] = window_mm(v[rows, :], (a0, a1), NT).astype(BF16)

    with jax.named_scope("o_1"):
        for i in range(NB // 2):
            step_o(i)
    with jax.named_scope("sum_a"):
        ra1[me] = pa[core]
        await_bytes(ra1.at[pl.ds(0, 3)], 2)
        sa[core] = (ra1[0] + ra1[1]) + (ra1[2] + ra1[3])
        s_a2 = send(sa.at[core], sa.at[core], sib, 3, 5)
    with jax.named_scope("o_2"):
        for i in range(NB // 2, NB):
            step_o(i)
    with jax.named_scope("cross_wv"):
        cross(f_wv, wv_part, wv_r1, wv_s, wv_r2, 6, 10, OWN - DIRECT)
    with jax.named_scope("dwo_far"):
        for i in range(NB):
            ot[:, block(i)] = o[block(i), :].T
        f_wo = part_rows(ot, far, dy[...], wo_part, wo_r1, 0, 0, 6)

    with jax.named_scope("wait_a"):
        s_a2.wait_recv()
    with jax.named_scope("softmax_bwd"):
        dsum = [jnp.zeros((1, LANES), F32) for _ in range(6)]
        lane = lax.broadcasted_iota(jnp.int32, (1, LANES), 1)
        d_tau = jnp.zeros((1, LANES), F32)
        for h in range(HEADS):
            rel = rels[h]
            valid = rel < HD
            hr = pl.ds(HD * h, HD)
            at = attn[hr, :]
            d_at = jnp.where(valid, packed_head(sa, h), 0.0).astype(BF16).astype(F32)
            d_sc = at * (d_at - jnp.sum(d_at * at, axis=1, keepdims=True))
            d_sc_inv = d_sc * qk_inv[hr, :]
            d_tau_h = jnp.sum(d_sc_inv * jnp.where(valid, packed_head(gfull, h), 0.0), axis=0, keepdims=True)
            d_tau = jnp.where(lane == h, jnp.sum(d_tau_h, axis=1, keepdims=True), d_tau)
            spread_head(d_sc_inv * tau_ref[h], rels, h, (e0, e1))
            wt = d_sc * score[hr, :]
            over_q = jnp.sum(jnp.where(rel == row, jnp.sum(wt, axis=1, keepdims=True), 0.0), axis=0, keepdims=True)
            over_k = jnp.sum(wt, axis=0, keepdims=True)
            for m in segs_of(h):
                mask = seg_mask(rel, h, m)[:1]
                dsum[m] = jnp.where(mask, over_q, dsum[m])
                dsum[3 + m] = jnp.where(mask, over_k, dsum[3 + m])
        dt_ref[...] = d_tau[:, :HEADS].reshape(HEADS)
        for m in range(6):
            dsq[:, pl.ds(LANES * m, LANES)] = -dsum[m] / gfull[pl.ds(PK + m, 1), :]
    with jax.named_scope("dqk"):
        for i in range(NB):
            rows = block(i)
            dqkv[rows, :C] = (
                window_mm(k[rows, :], (e0, e1), NT) + q[rows, :].astype(F32) * dsq[:, :C]).astype(BF16)
            dqkv[rows, C : 2 * C] = (
                window_mm(q[rows, :], (e0, e1), NN) + k[rows, :].astype(F32) * dsq[:, C:]).astype(BF16)
    with jax.named_scope("cross_wo"):
        cross(f_wo, wo_part, wo_r1, wo_s, wo_r2, 7, 10)
    with jax.named_scope("dwq_far"):
        f_wq = part_rows(ut, far, dqkv[:, :C], wq_part, wq_r1, 0, 3, 7)
    with jax.named_scope("dwk_far"):
        f_wk = part_rows(ut, far, dqkv[:, C : 2 * C], wk_part, wk_r1, 0, 0, 8)
        last = pl.ds(OWN - MOVE, MOVE)
        hand = remote(wk_part.at[0, last, :], wk_x, sib, 9, 13)

        @pl.when(core == 0)
        def _():
            hand.start()

    with jax.named_scope("near_v"):
        part_rows(ut, near, dqkv[:, 2 * C :], wv_part, wv_r1, 1, 8, 9)
    with jax.named_scope("cross_wq"):
        cross(f_wq, wq_part, wq_r1, wq_s, wq_r2, 4, 10)
    with jax.named_scope("near_o"):
        part_rows(ot, near, dy[...], wo_part, wo_r1, 1, 3, 9)
    with jax.named_scope("cross_wk"):
        cross(f_wk, wk_part, wk_r1, wk_s, wk_r2, 5, 11, OWN - LATE)
    with jax.named_scope("near_qk"):
        part_rows(ut, near, dqkv[:, :C], wq_part, wq_r1, 1, 0, 9)
        part_rows(ut, near, dqkv[:, C : 2 * C], wk_part, wk_r1, 1, 8, 9)

    gamma = g_ref[...].reshape(1, C)
    dgam = jnp.zeros((8, C), F32)
    dbet = jnp.zeros((8, C), F32)
    with jax.named_scope("ln_bwd"):
        for i in range(NB):
            rows = block(i)
            du[rows, :] = mm(dqkv[rows, :], wqkv[...], NT).astype(BF16)
            for j in range(RB // SB):
                sub = pl.ds(i * RB + j * SB, SB)
                d = du[sub, :].astype(F32)
                xh = xhat[sub, :]
                dxh = d * xh
                dgam += jnp.sum(dxh.reshape(SB // 8, 8, C), axis=0)
                dbet += jnp.sum(d.reshape(SB // 8, 8, C), axis=0)
                dh = d * gamma
                m1 = jnp.mean(dh, axis=-1, keepdims=True)
                m2 = jnp.mean(dxh * gamma, axis=-1, keepdims=True)
                inv = istd[sub, :]
                term = dh - m1 - xh * m2
                dln = term * jnp.concatenate([inv, inv, inv], axis=1)
                dx[sub, :] = (dy[sub, :].astype(F32) + dln).astype(BF16)
        dgb_all[me] = jnp.concatenate(
            [jnp.sum(dgam, axis=0, keepdims=True), jnp.sum(dbet, axis=0, keepdims=True)], axis=1)
    for j, peer in enumerate((nbr, diag, sib)):
        send(dgb_all.at[me], dgb_all.at[me], peer, 1 + j, 12)
    late = pl.ds(OWN - LATE, LATE)
    wk_s[late, :] = wk_part[0, pl.ds(pl.multiple_of(OWN * core + OWN - LATE, 8), LATE), :] + wk_r1[0, late, :]
    busy.pop(6).wait_send()

    def late_copy(count):
        rows = pl.ds(OWN - LATE, count)
        return remote(wk_s.at[rows, :], wk_r2.at[rows, :], nbr, 6, 11)

    moved = remote(wk_m, wk_r2.at[last, :], diag, 9, 11)

    @pl.when(core == 0)
    def _():
        late_copy(LATE - MOVE).start()

    @pl.when(core == 1)
    def _():
        hand.wait_recv()
        wk_m[...] = wk_part[0, last, :] + wk_x[...]
        moved.start()
        late_copy(LATE).start()

    with jax.named_scope("y"):
        for i in range(NB):
            rows = block(i)
            y[rows, :] = (x[rows, :].astype(F32) + mm(o[rows, :], wo[...])).astype(BF16)

    def rows_of(n):
        return xhat.at[pl.ds(0, n), :]

    with jax.named_scope("wait_wq"):
        await_bytes(rows_of(4 * OWN), 9)
        await_bytes(wv_d, 4)
        await_bytes(rows_of(3 * OWN - DIRECT), 10)
        dwo_ref[...] = (wo_part[1, mine, :] + wo_r1[1] + wo_r2[...]).astype(BF16)
        dwqkv_ref[:, :C] = (wq_part[1, mine, :] + wq_r1[1] + wq_r2[...]).astype(BF16)
        cut = OWN - DIRECT
        near_sum = wv_part[1, mine, :] + wv_r1[1]
        far_sum = jnp.concatenate([wv_r2[pl.ds(0, cut), :], wv_d[0] + wv_d[1]], axis=0)
        dwqkv_ref[:, 2 * C :] = (near_sum + far_sum).astype(BF16)
    with jax.named_scope("wait_dgb"):
        await_bytes(dgb_all.at[pl.ds(0, 3)], 12)
        total = dgb_all[0] + dgb_all[1] + dgb_all[2] + dgb_all[3]
        dg_ref[...] = total[:, :C].reshape(C)
        db_ref[...] = total[:, C:].reshape(C)
    with jax.named_scope("wait_wqk"):
        await_bytes(rows_of(OWN), 11)
        dwqkv_ref[:, C : 2 * C] = (wk_part[1, mine, :] + wk_r1[1] + wk_r2[...]).astype(BF16)
    with jax.named_scope("sends"):
        for cp in busy.values():
            cp.wait_send()

        @pl.when(core == 0)
        def _():
            hand.wait_send()
            late_copy(LATE - MOVE).wait_send()

        @pl.when(core == 1)
        def _():
            moved.wait_send()
            late_copy(LATE).wait_send()


def write_out(*refs):
    ins, outs, sem = refs[:7], refs[7:14], refs[14]
    pairs = []
    for i in range(2):
        for j in range(PIECES):
            rows = pl.ds(j * (TOK // PIECES), TOK // PIECES)
            pairs.append((ins[i].at[rows, :], outs[i].at[rows, :]))
    pairs += [(ins[i], outs[i]) for i in range(2, 7)]
    copies = [pltpu.make_async_copy(src, dst, sem.at[i]) for i, (src, dst) in enumerate(pairs)]
    for cp in copies:
        cp.start()
    for cp in copies:
        cp.wait()


def xca_local(x_rows, dy_rows, ln_gamma, ln_beta, w_qkv, w_out, temperature):
    vm = pltpu.VMEM
    hbm_spec = pl.BlockSpec(memory_space=pltpu.HBM)
    vmem_spec = pl.BlockSpec(memory_space=pltpu.VMEM)
    results = (
        ((TOK, C), BF16), ((TOK, C), BF16), ((OWN, 3 * C), BF16), ((OWN, C), BF16),
        ((C,), F32), ((C,), F32), ((HEADS,), F32),
    )
    rows_bf = vm((TOK, C), BF16)
    cols_bf = vm((C, TOK), BF16)
    win_f = vm((256, 256), F32)
    win_b = vm((256, 256), BF16)
    pk_g = vm((PK + 8, LANES), F32)
    pk_a = vm((2, HALF, LANES), F32)
    fold = vm((C, LANES), F32)
    scratch = [
        rows_bf, rows_bf, vm((C,), F32), vm((C,), F32), vm((C, 3 * C), BF16), vm((C, C), BF16), vm((C, C), BF16),
        pltpu.SMEM((HEADS,), F32), rows_bf, cols_bf, vm((TOK, C), F32), vm((TOK, LANES), F32),
        rows_bf, rows_bf, rows_bf, rows_bf, rows_bf, cols_bf, vm((TOK, 3 * C), BF16), rows_bf,
        win_f, win_f, vm((8, 2 * C), F32), pk_g, pk_g, pk_g, pk_g, pk_a, vm((4, HALF, LANES), F32), pk_a,
        win_b, win_b, win_b, win_b, fold, fold, fold, pk_g, vm((1, 2 * C), F32),
        *[vm((2, 2 * OWN, C), F32)] * 4, *[vm((2, OWN, C), F32)] * 4, *[vm((OWN, C), F32)] * 8, vm((2, DIRECT, C), F32), vm((MOVE, C), F32), vm((MOVE, C), F32),
        vm((4, 1, 2 * C), F32),
        pltpu.SemaphoreType.DMA((10,)), pltpu.SemaphoreType.DMA((14,)),
    ]
    parts = pl.pallas_call(
        kernel,
        name="xca",
        out_shape=tuple(pltpu.VMEM(shape, dtype) for shape, dtype in results),
        in_specs=[hbm_spec] * 7,
        out_specs=[vmem_spec] * 7,
        scratch_shapes=scratch,
        compiler_params=pltpu.CompilerParams(
            collective_id=0, has_side_effects=True, vmem_limit_bytes=60 * 1024 * 1024),
    )(x_rows, dy_rows, ln_gamma, ln_beta, w_qkv, w_out, temperature)
    return pl.pallas_call(
        write_out,
        name="xca_out",
        out_shape=tuple(jax.ShapeDtypeStruct(shape, dtype) for shape, dtype in results),
        in_specs=[vmem_spec] * 7,
        out_specs=[hbm_spec] * 7,
        scratch_shapes=[pltpu.SemaphoreType.DMA((2 * PIECES + 5,))],
        compiler_params=pltpu.CompilerParams(vmem_limit_bytes=1024 * 1024),
    )(*parts)


def solution(mesh):
    row_spec = P(('dp', 'sp'), None)
    full_mat = P(None, None)
    full_vec = P(None)
    part_vec = P('dp')
    return jax.shard_map(
        xca_local, mesh=mesh,
        in_specs=(row_spec, row_spec, full_vec, full_vec, full_mat, full_mat, full_vec),
        out_specs=(row_spec, row_spec, row_spec, row_spec, part_vec, part_vec, part_vec),
        check_vma=False)
```

```python
import jax
import jax.numpy as jnp
from jax import lax
from jax.experimental import pallas as pl
from jax.experimental.pallas import tpu as pltpu
from jax.sharding import PartitionSpec as P

LN_EPS = 1e-6
F32, BF16 = jnp.float32, jnp.bfloat16
MESH = pl.DeviceIdType.MESH

C = 384
HEADS, HD = 8, 48
LANES = 128
TOK = 2048
RB = 512
NB = TOK // RB
A_BLOCKS = (512, 512, 512, 512)
NA = len(A_BLOCKS)
RV = 256
NV = TOK // RV
CUT = 4
LAG = 3
PIECES = 1
SB = 64
OWN = C // 4
PK = 144
LATE = 64
MOVE = 48
DIRECT = 16
HALF = PK // 2
W0_HEADS = 5

NN = (((1,), (0,)), ((), ()))
NT = (((1,), (1,)), ((), ()))
TN = (((0,), (0,)), ((), ()))


def mm(a, b, dims=NN):
    return lax.dot_general(a, b, dims, preferred_element_type=F32)


def a_block(i):
    return sum(A_BLOCKS[:i]), A_BLOCKS[i]


def head_rel():
    lane = lax.broadcasted_iota(jnp.int32, (HD, LANES), 1)
    return [(lane - HD * h) & (LANES - 1) for h in range(HEADS)]


def seg_mask(rel, h, m):
    chan = rel + HD * h
    return (rel < HD) & (chan >= LANES * m) & (chan < LANES * (m + 1))


def head_window(h):
    if h < W0_HEADS:
        return 0, HD * h, (0, 1)
    return 1, HD * h - LANES, (1, 2)


def segs_of(h):
    return sorted({(HD * h) // LANES, (HD * h + HD - 1) // LANES})


def spare_lanes(g):
    lane = lax.broadcasted_iota(jnp.int32, (HD, LANES), 1)
    return (lane >= 96 - 32 * g) & (lane < 128 - 32 * g)


def fold_windows(win_refs, out_ref):
    rels = head_rel()

    def put(acc, h, where):
        w, row, segs = head_window(h)
        for s, m in enumerate(segs):
            if m in segs_of(h):
                block = win_refs[w][pl.ds(row, HD), pl.ds(LANES * s, LANES)]
                mask = seg_mask(rels[h], h, m)
                acc = jnp.where(mask if where is None else mask & where, block, acc)
        return acc

    for g in range(3):
        acc = put(put(jnp.zeros((HD, LANES), F32), 2 * g, None), 2 * g + 1, None)
        spare = spare_lanes(g)
        put_rows(out_ref, g, put(put(acc, 6, spare), 7, spare))


def put_rows(ref, g, value):
    if len(ref.shape) == 2:
        ref[pl.ds(HD * g, HD), :] = value
    elif g == 1:
        ref[0, pl.ds(HD, HALF - HD), :] = value[: HALF - HD]
        ref[1, pl.ds(0, HALF - HD), :] = value[HALF - HD :]
    else:
        ref[g // 2, pl.ds((HALF - HD) * (g // 2), HD), :] = value


def get_rows(ref, g):
    if len(ref.shape) == 2:
        return ref[pl.ds(HD * g, HD), :]
    if g == 1:
        return jnp.concatenate([ref[0, pl.ds(HD, HALF - HD), :], ref[1, pl.ds(0, HALF - HD), :]], axis=0)
    return ref[g // 2, pl.ds((HALF - HD) * (g // 2), HD), :]


def packed_head(ref, h):
    if h < 6:
        return get_rows(ref, h // 2)
    lane = lax.broadcasted_iota(jnp.int32, (HD, LANES), 1)
    return jnp.where(lane >= 96, get_rows(ref, 0), jnp.where(lane >= 64, get_rows(ref, 1), get_rows(ref, 2)))


def spread_head(value, rels, h, win_refs):
    w, row, segs = head_window(h)
    parts = []
    for m in segs:
        if m in segs_of(h):
            parts.append(jnp.where(seg_mask(rels[h], h, m), value, 0.0))
        else:
            parts.append(jnp.zeros((HD, LANES), F32))
    win_refs[w][pl.ds(row, HD), :] = jnp.concatenate(parts, axis=1).astype(BF16)


def window_mm(a, win_refs, dims):
    r0 = mm(a[:, :256], win_refs[0][...], dims)
    r1 = mm(a[:, 128:], win_refs[1][...], dims)
    return jnp.concatenate([r0[:, :128], r0[:, 128:] + r1[:, :128], r1[:, 128:]], axis=1)


def kernel(
    x_hbm, dy_hbm, g_hbm, b_hbm, wqkv_hbm, wo_hbm, tau_hbm,
    y, dx, dwqkv_ref, dwo_ref, dg_ref, db_ref, dt_ref,
    x, dy, g_ref, b_ref, wqkv, wo, wot, tau_ref, u, ut, xhat, istd, q, k, v, do, o, ot, dqkv, du,
    g0, g1, sq, pg, rg1, sg, rg2, pa, ra1, sa,
    a0, a1, e0, e1, attn, score, qk_inv, gfull, dsq,
    wo_part, wv_part, wq_part, wk_part, wo_r1, wv_r1, wq_r1, wk_r1,
    wo_s, wv_s, wq_s, wk_s, wo_r2, wv_r2, wq_r2, wk_r2, wv_d, wk_x, wk_m,
    dgb_all,
    loc_sem, recv_sem,
):
    me = lax.axis_index("sp")
    core = lax.rem(me, 2)
    chip = me // 2
    sib = me + 1 - 2 * core
    nbr = lax.rem(me + 2, 4)
    diag = lax.rem(sib + 2, 4)

    def load(src, dst, slot):
        cp = pltpu.make_async_copy(src, dst, loc_sem.at[slot])
        cp.start()
        return cp

    def block(i):
        return pl.ds(i * RB, RB)

    n0 = A_BLOCKS[0]
    ld_gb = [load(g_hbm, g_ref, 0), load(b_hbm, b_ref, 1)]
    ld_x0 = load(x_hbm.at[pl.ds(0, n0), :], x.at[pl.ds(0, n0), :], 2)
    ld_wqk = load(wqkv_hbm.at[:, pl.ds(0, 2 * C)], wqkv.at[:, pl.ds(0, 2 * C)], 3)
    ld_x1 = load(x_hbm.at[pl.ds(n0, TOK - n0), :], x.at[pl.ds(n0, TOK - n0), :], 4)
    ld_wo = load(wo_hbm, wo, 5)
    ld_wv = load(wqkv_hbm.at[:, pl.ds(2 * C, C)], wqkv.at[:, pl.ds(2 * C, C)], 6)
    ld_dy = load(dy_hbm, dy, 7)
    ld_tau = load(tau_hbm, tau_ref, 8)

    barrier = pltpu.get_barrier_semaphore()
    for peer in (sib, nbr, diag):
        pl.semaphore_signal(barrier, inc=1, device_id={"sp": peer}, device_id_type=MESH)

    busy = {}

    def remote(src, dst, peer, slot, got):
        return pltpu.make_async_remote_copy(
            src_ref=src, dst_ref=dst, send_sem=loc_sem.at[slot], recv_sem=recv_sem.at[got],
            device_id={"sp": peer}, device_id_type=MESH)

    def send(src, dst, peer, slot, got):
        if slot in busy:
            busy[slot].wait_send()
        cp = remote(src, dst, peer, slot, got)
        cp.start()
        busy[slot] = cp
        return cp

    def await_bytes(ref, got):
        remote(ref, ref, sib, 0, got).wait_recv()

    def step_ln(i):
        gamma = g_ref[...].reshape(1, C)
        beta = b_ref[...].reshape(1, C)
        lo, size = a_block(i)
        for j in range(size // SB):
            rows = pl.ds(lo + j * SB, SB)
            xf = x[rows, :].astype(F32)
            cen = xf - jnp.mean(xf, axis=-1, keepdims=True)
            inv = lax.rsqrt(jnp.mean(cen * cen, axis=-1, keepdims=True) + LN_EPS)
            xh = cen * inv
            xhat[rows, :] = xh
            istd[rows, :] = jnp.broadcast_to(inv, (SB, LANES))
            u[rows, :] = (xh * gamma + beta).astype(BF16)

    def step_qk(i):
        lo, size = a_block(i)
        rows = pl.ds(lo, size)
        qk = mm(u[rows, :], wqkv[:, : 2 * C]).astype(BF16)
        q[rows, :] = qk[:, :C]
        k[rows, :] = qk[:, C:]

    def step_gram(i):
        lo, size = a_block(i)
        rows = pl.ds(lo, size)
        p0 = mm(q[rows, :256], k[rows, :256], TN)
        p1 = mm(q[rows, 128:], k[rows, 128:], TN)
        if i == 0:
            g0[...], g1[...] = p0, p1
        else:
            g0[...] += p0
            g1[...] += p1
        for r, c0 in ((q, 0), (k, C)):
            part = jnp.zeros((8, C), F32)
            for j in range(size // SB):
                f = r[pl.ds(lo + j * SB, SB), :].astype(F32)
                part += jnp.sum((f * f).reshape(SB // 8, 8, C), axis=0)
            if i == 0:
                sq[:, pl.ds(c0, C)] = part
            else:
                sq[:, pl.ds(c0, C)] += part

    with jax.named_scope("ln_0"):
        ld_x0.wait()
        for cp in ld_gb:
            cp.wait()
        step_ln(0)
    ld_wqk.wait()
    ld_x1.wait()
    with jax.named_scope("ln_qk"):
        for i in range(1, NA + 2):
            if i < NA:
                step_ln(i)
            if 1 <= i <= NA:
                step_qk(i - 1)
            if i >= 2:
                step_gram(i - 2)
    with jax.named_scope("fold_g"):
        fold_windows((g0, g1), pg)
        sums = jnp.sum(sq[...], axis=0, keepdims=True)
        for m in range(6):
            pg[pl.ds(PK + m, 1), :] = sums[:, LANES * m : LANES * (m + 1)]
        pg[pl.ds(PK + 6, 2), :] = jnp.zeros((2, LANES), F32)
    with jax.named_scope("greet"):
        pl.semaphore_wait(barrier, 3)
    s_g1 = send(pg, rg1, sib, 0, 0)

    def step_b(i):
        rows = pl.ds(i * RV, RV)
        v[rows, :] = mm(u[rows, :], wqkv[:, 2 * C :]).astype(BF16)
        do[rows, :] = mm(dy[rows, :], wot[...]).astype(BF16)

    def step_da(i):
        rows = pl.ds(i * RV, RV)
        p0 = mm(do[rows, :256], v[rows, :256], TN)
        p1 = mm(do[rows, 128:], v[rows, 128:], TN)
        if i == 0:
            g0[...], g1[...] = p0, p1
        else:
            g0[...] += p0
            g1[...] += p1

    with jax.named_scope("v_do_1"):
        ld_wo.wait()
        ld_wv.wait()
        ld_dy.wait()
        ld_tau.wait()
        wot[...] = wo[...].T
        for i in range(CUT):
            step_b(i)
        for i in range(NB):
            ut[:, block(i)] = u[block(i), :].T
    with jax.named_scope("sum_g"):
        s_g1.wait_recv()
        sg[...] = pg[...] + rg1[...]
        s_g2 = [remote(sg, rg2, peer, 1 + j, 1) for j, peer in enumerate((diag, nbr))]

        @pl.when(core == 1)
        def _():
            for cp in s_g2:
                cp.start()
    with jax.named_scope("v_do_2"):
        for i in range(CUT, NV):
            step_b(i)
            for j in range(max(0, i - LAG) if i > CUT else 0, i + 1 - LAG):
                step_da(j)
        for i in range(NV - LAG, NV):
            step_da(i)
    with jax.named_scope("fold_a"):
        fold_windows((g0, g1), pa)
        send(pa.at[1 - core], ra1.at[me], sib, 3, 2)
        send(pa.at[core], ra1.at[me], nbr, 4, 2)
        send(pa.at[1 - core], ra1.at[me], diag, 5, 2)

    with jax.named_scope("wait_g"):
        s_g2[0].wait_recv()
    rels = head_rel()
    row = lax.broadcasted_iota(jnp.int32, (HD, LANES), 0)
    with jax.named_scope("softmax"):
        gfull[...] = sg[...] + rg2[...]
        for ref in (a0, a1, e0, e1):
            ref[...] = jnp.zeros_like(ref)
        for h in range(HEADS):
            rel = rels[h]
            valid = rel < HD
            tau = tau_ref[h]
            s_q = jnp.zeros((HD, LANES), F32)
            s_k = jnp.ones((HD, LANES), F32)
            for m in segs_of(h):
                mask = seg_mask(rel, h, m)
                s_q = jnp.where(mask, gfull[pl.ds(PK + m, 1), :], s_q)
                s_k = jnp.where(mask, gfull[pl.ds(PK + 3 + m, 1), :], s_k)
            q_inv = lax.rsqrt(jnp.sum(jnp.where(rel == row, s_q, 0.0), axis=1, keepdims=True))
            k_inv = lax.rsqrt(s_k)
            by_k = packed_head(gfull, h) * k_inv
            top = jnp.max(jnp.where(valid, by_k, -jnp.inf), axis=1, keepdims=True)
            scale = tau * q_inv
            sc = jnp.where(valid, scale * by_k, 0.0)
            inv = jnp.where(valid, q_inv * k_inv, 0.0)
            ex = jnp.where(valid, jnp.exp(sc - scale * top), 0.0)
            at = ex / jnp.sum(ex, axis=1, keepdims=True)
            hr = pl.ds(HD * h, HD)
            score[hr, :] = sc
            qk_inv[hr, :] = inv
            attn[hr, :] = at
            spread_head(at, rels, h, (a0, a1))

    far = pl.ds(pl.multiple_of(2 * OWN * (1 - chip), 16), 2 * OWN)
    near = pl.ds(pl.multiple_of(2 * OWN * chip, 16), 2 * OWN)
    mine = pl.ds(pl.multiple_of(OWN * core, 8), OWN)

    def part_rows(lhs_t, rows, rhs, part, r1, half, sem, got, count=OWN):
        part[half] = mm(lhs_t[rows, :], rhs)
        theirs = pl.ds(pl.multiple_of(OWN * (1 - core), 8), count)
        return send(part.at[half, theirs, :], r1.at[half, pl.ds(0, count), :], sib, sem, got)

    def cross(cp, part, r1, s, r2, sem, got, count=OWN):
        cp.wait_recv()
        rows = pl.ds(0, count)
        s[rows, :] = part[0, pl.ds(pl.multiple_of(OWN * core, 8), count), :] + r1[0, rows, :]
        send(s.at[rows, :], r2.at[rows, :], nbr, sem, got)

    with jax.named_scope("dv"):
        for i in range(NB):
            rows = block(i)
            dqkv[rows, 2 * C :] = window_mm(do[rows, :], (a0, a1), NN).astype(BF16)
        f_wv = part_rows(ut, far, dqkv[:, 2 * C :], wv_part, wv_r1, 0, 0, 3, OWN - DIRECT)
        @pl.when(core == 1)
        def _():
            for cp in s_g2:
                cp.wait_send()

        for j, (c, peer) in enumerate(((1 - core, diag), (core, nbr))):
            rows = pl.ds(pl.multiple_of(OWN * c + OWN - DIRECT, 8), DIRECT)
            send(wv_part.at[0, rows, :], wv_d.at[j], peer, 1 + j, 4)

    def step_o(i):
        rows = block(i)
        o[rows, :] = window_mm(v[rows, :], (a0, a1), NT).astype(BF16)

    with jax.named_scope("o_1"):
        for i in range(NB // 2):
            step_o(i)
    with jax.named_scope("sum_a"):
        ra1[me] = pa[core]
        await_bytes(ra1.at[pl.ds(0, 3)], 2)
        sa[core] = (ra1[0] + ra1[1]) + (ra1[2] + ra1[3])
        s_a2 = send(sa.at[core], sa.at[core], sib, 3, 5)
    with jax.named_scope("o_2"):
        for i in range(NB // 2, NB - 1):
            step_o(i)
    with jax.named_scope("cross_wv"):
        cross(f_wv, wv_part, wv_r1, wv_s, wv_r2, 6, 10, OWN - DIRECT)
    with jax.named_scope("dwo_far"):
        step_o(NB - 1)
        for i in range(NB):
            ot[:, block(i)] = o[block(i), :].T
        f_wo = part_rows(ot, far, dy[...], wo_part, wo_r1, 0, 0, 6)

    with jax.named_scope("wait_a"):
        s_a2.wait_recv()
    with jax.named_scope("softmax_bwd"):
        dsum = [jnp.zeros((1, LANES), F32) for _ in range(6)]
        lane = lax.broadcasted_iota(jnp.int32, (1, LANES), 1)
        d_tau = jnp.zeros((1, LANES), F32)
        for h in range(HEADS):
            rel = rels[h]
            valid = rel < HD
            hr = pl.ds(HD * h, HD)
            at = attn[hr, :]
            d_at = jnp.where(valid, packed_head(sa, h), 0.0).astype(BF16).astype(F32)
            d_sc = at * (d_at - jnp.sum(d_at * at, axis=1, keepdims=True))
            d_sc_inv = d_sc * qk_inv[hr, :]
            d_tau_h = jnp.sum(d_sc_inv * jnp.where(valid, packed_head(gfull, h), 0.0), axis=0, keepdims=True)
            d_tau = jnp.where(lane == h, jnp.sum(d_tau_h, axis=1, keepdims=True), d_tau)
            spread_head(d_sc_inv * tau_ref[h], rels, h, (e0, e1))
            wt = d_sc * score[hr, :]
            over_q = jnp.sum(jnp.where(rel == row, jnp.sum(wt, axis=1, keepdims=True), 0.0), axis=0, keepdims=True)
            over_k = jnp.sum(wt, axis=0, keepdims=True)
            for m in segs_of(h):
                mask = seg_mask(rel, h, m)[:1]
                dsum[m] = jnp.where(mask, over_q, dsum[m])
                dsum[3 + m] = jnp.where(mask, over_k, dsum[3 + m])
        dt_ref[...] = d_tau[:, :HEADS].reshape(HEADS)
        for m in range(6):
            dsq[:, pl.ds(LANES * m, LANES)] = -dsum[m] / gfull[pl.ds(PK + m, 1), :]
    with jax.named_scope("dqk"):
        for i in range(NB):
            rows = block(i)
            dqkv[rows, :C] = (
                window_mm(k[rows, :], (e0, e1), NT) + q[rows, :].astype(F32) * dsq[:, :C]).astype(BF16)
            dqkv[rows, C : 2 * C] = (
                window_mm(q[rows, :], (e0, e1), NN) + k[rows, :].astype(F32) * dsq[:, C:]).astype(BF16)
    with jax.named_scope("cross_wo"):
        cross(f_wo, wo_part, wo_r1, wo_s, wo_r2, 7, 10)
    with jax.named_scope("dwq_far"):
        f_wq = part_rows(ut, far, dqkv[:, :C], wq_part, wq_r1, 0, 3, 7)
    with jax.named_scope("dwk_far"):
        f_wk = part_rows(ut, far, dqkv[:, C : 2 * C], wk_part, wk_r1, 0, 0, 8)
        last = pl.ds(OWN - MOVE, MOVE)
        hand = remote(wk_part.at[0, last, :], wk_x, sib, 9, 13)

        @pl.when(core == 0)
        def _():
            hand.start()

    with jax.named_scope("near_v"):
        part_rows(ut, near, dqkv[:, 2 * C :], wv_part, wv_r1, 1, 8, 9)
    with jax.named_scope("cross_wq"):
        cross(f_wq, wq_part, wq_r1, wq_s, wq_r2, 4, 10)
    with jax.named_scope("near_o"):
        part_rows(ot, near, dy[...], wo_part, wo_r1, 1, 3, 9)
    with jax.named_scope("cross_wk"):
        cross(f_wk, wk_part, wk_r1, wk_s, wk_r2, 5, 11, OWN - LATE)
    gamma = g_ref[...].reshape(1, C)
    dgam = jnp.zeros((8, C), F32)
    dbet = jnp.zeros((8, C), F32)
    with jax.named_scope("ln_bwd"):
        for i in range(NB):
            rows = block(i)
            du[rows, :] = mm(dqkv[rows, :], wqkv[...], NT).astype(BF16)
            for j in range(RB // SB):
                sub = pl.ds(i * RB + j * SB, SB)
                d = du[sub, :].astype(F32)
                xh = xhat[sub, :]
                dxh = d * xh
                dgam += jnp.sum(dxh.reshape(SB // 8, 8, C), axis=0)
                dbet += jnp.sum(d.reshape(SB // 8, 8, C), axis=0)
                dh = d * gamma
                m1 = jnp.mean(dh, axis=-1, keepdims=True)
                m2 = jnp.mean(dxh * gamma, axis=-1, keepdims=True)
                inv = istd[sub, :]
                term = dh - m1 - xh * m2
                dln = term * jnp.concatenate([inv, inv, inv], axis=1)
                dx[sub, :] = (dy[sub, :].astype(F32) + dln).astype(BF16)
        dgb_all[me] = jnp.concatenate(
            [jnp.sum(dgam, axis=0, keepdims=True), jnp.sum(dbet, axis=0, keepdims=True)], axis=1)
    for j, peer in enumerate((nbr, diag, sib)):
        send(dgb_all.at[me], dgb_all.at[me], peer, 1 + j, 12)
    late = pl.ds(OWN - LATE, LATE)
    wk_s[late, :] = wk_part[0, pl.ds(pl.multiple_of(OWN * core + OWN - LATE, 8), LATE), :] + wk_r1[0, late, :]
    busy.pop(6).wait_send()

    def late_copy(count):
        rows = pl.ds(OWN - LATE, count)
        return remote(wk_s.at[rows, :], wk_r2.at[rows, :], nbr, 6, 11)

    moved = remote(wk_m, wk_r2.at[last, :], diag, 9, 11)

    @pl.when(core == 0)
    def _():
        late_copy(LATE - MOVE).start()

    @pl.when(core == 1)
    def _():
        hand.wait_recv()
        wk_m[...] = wk_part[0, last, :] + wk_x[...]
        moved.start()
        late_copy(LATE).start()

    with jax.named_scope("near_qk"):
        part_rows(ut, near, dqkv[:, :C], wq_part, wq_r1, 1, 0, 9)
        part_rows(ut, near, dqkv[:, C : 2 * C], wk_part, wk_r1, 1, 8, 9)
    with jax.named_scope("y"):
        for i in range(NB):
            rows = block(i)
            y[rows, :] = (x[rows, :].astype(F32) + mm(o[rows, :], wo[...])).astype(BF16)

    def rows_of(n):
        return xhat.at[pl.ds(0, n), :]

    with jax.named_scope("wait_wq"):
        await_bytes(rows_of(4 * OWN), 9)
        await_bytes(wv_d, 4)
        await_bytes(rows_of(3 * OWN - DIRECT), 10)
        dwo_ref[...] = (wo_part[1, mine, :] + wo_r1[1] + wo_r2[...]).astype(BF16)
        dwqkv_ref[:, :C] = (wq_part[1, mine, :] + wq_r1[1] + wq_r2[...]).astype(BF16)
        cut = OWN - DIRECT
        near_sum = wv_part[1, mine, :] + wv_r1[1]
        far_sum = jnp.concatenate([wv_r2[pl.ds(0, cut), :], wv_d[0] + wv_d[1]], axis=0)
        dwqkv_ref[:, 2 * C :] = (near_sum + far_sum).astype(BF16)
    with jax.named_scope("wait_dgb"):
        await_bytes(dgb_all.at[pl.ds(0, 3)], 12)
        total = dgb_all[0] + dgb_all[1] + dgb_all[2] + dgb_all[3]
        dg_ref[...] = total[:, :C].reshape(C)
        db_ref[...] = total[:, C:].reshape(C)
    with jax.named_scope("wait_wqk"):
        await_bytes(rows_of(OWN), 11)
        dwqkv_ref[:, C : 2 * C] = (wk_part[1, mine, :] + wk_r1[1] + wk_r2[...]).astype(BF16)
    with jax.named_scope("sends"):
        for cp in busy.values():
            cp.wait_send()

        @pl.when(core == 0)
        def _():
            hand.wait_send()
            late_copy(LATE - MOVE).wait_send()

        @pl.when(core == 1)
        def _():
            moved.wait_send()
            late_copy(LATE).wait_send()


def write_out(*refs):
    ins, outs, sem = refs[:7], refs[7:14], refs[14]
    pairs = []
    for i in range(2):
        for j in range(PIECES):
            rows = pl.ds(j * (TOK // PIECES), TOK // PIECES)
            pairs.append((ins[i].at[rows, :], outs[i].at[rows, :]))
    pairs += [(ins[i], outs[i]) for i in range(2, 7)]
    copies = [pltpu.make_async_copy(src, dst, sem.at[i]) for i, (src, dst) in enumerate(pairs)]
    for cp in copies:
        cp.start()
    for cp in copies:
        cp.wait()


def xca_local(x_rows, dy_rows, ln_gamma, ln_beta, w_qkv, w_out, temperature):
    vm = pltpu.VMEM
    hbm_spec = pl.BlockSpec(memory_space=pltpu.HBM)
    vmem_spec = pl.BlockSpec(memory_space=pltpu.VMEM)
    results = (
        ((TOK, C), BF16), ((TOK, C), BF16), ((OWN, 3 * C), BF16), ((OWN, C), BF16),
        ((C,), F32), ((C,), F32), ((HEADS,), F32),
    )
    rows_bf = vm((TOK, C), BF16)
    cols_bf = vm((C, TOK), BF16)
    win_f = vm((256, 256), F32)
    win_b = vm((256, 256), BF16)
    pk_g = vm((PK + 8, LANES), F32)
    pk_a = vm((2, HALF, LANES), F32)
    fold = vm((C, LANES), F32)
    scratch = [
        rows_bf, rows_bf, vm((C,), F32), vm((C,), F32), vm((C, 3 * C), BF16), vm((C, C), BF16), vm((C, C), BF16),
        pltpu.SMEM((HEADS,), F32), rows_bf, cols_bf, vm((TOK, C), F32), vm((TOK, LANES), F32),
        rows_bf, rows_bf, rows_bf, rows_bf, rows_bf, cols_bf, vm((TOK, 3 * C), BF16), rows_bf,
        win_f, win_f, vm((8, 2 * C), F32), pk_g, pk_g, pk_g, pk_g, pk_a, vm((4, HALF, LANES), F32), pk_a,
        win_b, win_b, win_b, win_b, fold, fold, fold, pk_g, vm((1, 2 * C), F32),
        *[vm((2, 2 * OWN, C), F32)] * 4, *[vm((2, OWN, C), F32)] * 4, *[vm((OWN, C), F32)] * 8, vm((2, DIRECT, C), F32), vm((MOVE, C), F32), vm((MOVE, C), F32),
        vm((4, 1, 2 * C), F32),
        pltpu.SemaphoreType.DMA((10,)), pltpu.SemaphoreType.DMA((14,)),
    ]
    parts = pl.pallas_call(
        kernel,
        name="xca",
        out_shape=tuple(pltpu.VMEM(shape, dtype) for shape, dtype in results),
        in_specs=[hbm_spec] * 7,
        out_specs=[vmem_spec] * 7,
        scratch_shapes=scratch,
        compiler_params=pltpu.CompilerParams(
            collective_id=0, has_side_effects=True, vmem_limit_bytes=60 * 1024 * 1024),
    )(x_rows, dy_rows, ln_gamma, ln_beta, w_qkv, w_out, temperature)
    return pl.pallas_call(
        write_out,
        name="xca_out",
        out_shape=tuple(jax.ShapeDtypeStruct(shape, dtype) for shape, dtype in results),
        in_specs=[vmem_spec] * 7,
        out_specs=[hbm_spec] * 7,
        scratch_shapes=[pltpu.SemaphoreType.DMA((2 * PIECES + 5,))],
        compiler_params=pltpu.CompilerParams(vmem_limit_bytes=1024 * 1024),
    )(*parts)


def solution(mesh):
    row_spec = P(('dp', 'sp'), None)
    full_mat = P(None, None)
    full_vec = P(None)
    part_vec = P('dp')
    return jax.shard_map(
        xca_local, mesh=mesh,
        in_specs=(row_spec, row_spec, full_vec, full_vec, full_mat, full_mat, full_vec),
        out_specs=(row_spec, row_spec, row_spec, row_spec, part_vec, part_vec, part_vec),
        check_vma=False)
```

```python
import jax
import jax.numpy as jnp
from jax import lax
from jax.experimental import pallas as pl
from jax.experimental.pallas import tpu as pltpu
from jax.sharding import PartitionSpec as P

LN_EPS = 1e-6
F32, BF16 = jnp.float32, jnp.bfloat16
MESH = pl.DeviceIdType.MESH

C = 384
HEADS, HD = 8, 48
LANES = 128
TOK = 2048
RB = 512
NB = TOK // RB
A_BLOCKS = (512, 512, 512, 512)
NA = len(A_BLOCKS)
RV = 256
NV = TOK // RV
CUT = 4
LAG = 3
PIECES = 1
SB = 64
OWN = C // 4
PK = 144
LATE = 48
MOVE = 40
DIRECT = 16
HALF = PK // 2
W0_HEADS = 5

NN = (((1,), (0,)), ((), ()))
NT = (((1,), (1,)), ((), ()))
TN = (((0,), (0,)), ((), ()))


def mm(a, b, dims=NN):
    return lax.dot_general(a, b, dims, preferred_element_type=F32)


def a_block(i):
    return sum(A_BLOCKS[:i]), A_BLOCKS[i]


def head_rel():
    lane = lax.broadcasted_iota(jnp.int32, (HD, LANES), 1)
    return [(lane - HD * h) & (LANES - 1) for h in range(HEADS)]


def seg_mask(rel, h, m):
    chan = rel + HD * h
    return (rel < HD) & (chan >= LANES * m) & (chan < LANES * (m + 1))


def head_window(h):
    if h < W0_HEADS:
        return 0, HD * h, (0, 1)
    return 1, HD * h - LANES, (1, 2)


def segs_of(h):
    return sorted({(HD * h) // LANES, (HD * h + HD - 1) // LANES})


def spare_lanes(g):
    lane = lax.broadcasted_iota(jnp.int32, (HD, LANES), 1)
    return (lane >= 96 - 32 * g) & (lane < 128 - 32 * g)


def fold_windows(win_refs, out_ref):
    rels = head_rel()

    def put(acc, h, where):
        w, row, segs = head_window(h)
        for s, m in enumerate(segs):
            if m in segs_of(h):
                block = win_refs[w][pl.ds(row, HD), pl.ds(LANES * s, LANES)]
                mask = seg_mask(rels[h], h, m)
                acc = jnp.where(mask if where is None else mask & where, block, acc)
        return acc

    for g in range(3):
        acc = put(put(jnp.zeros((HD, LANES), F32), 2 * g, None), 2 * g + 1, None)
        spare = spare_lanes(g)
        put_rows(out_ref, g, put(put(acc, 6, spare), 7, spare))


def put_rows(ref, g, value):
    if len(ref.shape) == 2:
        ref[pl.ds(HD * g, HD), :] = value
    elif g == 1:
        ref[0, pl.ds(HD, HALF - HD), :] = value[: HALF - HD]
        ref[1, pl.ds(0, HALF - HD), :] = value[HALF - HD :]
    else:
        ref[g // 2, pl.ds((HALF - HD) * (g // 2), HD), :] = value


def get_rows(ref, g):
    if len(ref.shape) == 2:
        return ref[pl.ds(HD * g, HD), :]
    if g == 1:
        return jnp.concatenate([ref[0, pl.ds(HD, HALF - HD), :], ref[1, pl.ds(0, HALF - HD), :]], axis=0)
    return ref[g // 2, pl.ds((HALF - HD) * (g // 2), HD), :]


def packed_head(ref, h):
    if h < 6:
        return get_rows(ref, h // 2)
    lane = lax.broadcasted_iota(jnp.int32, (HD, LANES), 1)
    return jnp.where(lane >= 96, get_rows(ref, 0), jnp.where(lane >= 64, get_rows(ref, 1), get_rows(ref, 2)))


def spread_head(value, rels, h, win_refs):
    w, row, segs = head_window(h)
    parts = []
    for m in segs:
        if m in segs_of(h):
            parts.append(jnp.where(seg_mask(rels[h], h, m), value, 0.0))
        else:
            parts.append(jnp.zeros((HD, LANES), F32))
    win_refs[w][pl.ds(row, HD), :] = jnp.concatenate(parts, axis=1).astype(BF16)


def window_mm(a, win_refs, dims):
    r0 = mm(a[:, :256], win_refs[0][...], dims)
    r1 = mm(a[:, 128:], win_refs[1][...], dims)
    return jnp.concatenate([r0[:, :128], r0[:, 128:] + r1[:, :128], r1[:, 128:]], axis=1)


def kernel(
    x_hbm, dy_hbm, g_hbm, b_hbm, wqkv_hbm, wo_hbm, tau_hbm,
    y, dx, dwqkv_ref, dwo_ref, dg_ref, db_ref, dt_ref,
    x, dy, g_ref, b_ref, wqkv, wo, wot, tau_ref, u, ut, xhat, istd, q, k, v, do, o, ot, dqkv, du,
    g0, g1, sq, pg, rg1, sg, rg2, pa, ra1, sa,
    a0, a1, e0, e1, attn, score, qk_inv, gfull, dsq,
    wo_part, wv_part, wq_part, wk_part, wo_r1, wv_r1, wq_r1, wk_r1,
    wo_s, wv_s, wq_s, wk_s, wo_r2, wv_r2, wq_r2, wk_r2, wv_d, wk_x, wk_m,
    dgb_all,
    loc_sem, recv_sem,
):
    me = lax.axis_index("sp")
    core = lax.rem(me, 2)
    chip = me // 2
    sib = me + 1 - 2 * core
    nbr = lax.rem(me + 2, 4)
    diag = lax.rem(sib + 2, 4)

    def load(src, dst, slot):
        cp = pltpu.make_async_copy(src, dst, loc_sem.at[slot])
        cp.start()
        return cp

    def block(i):
        return pl.ds(i * RB, RB)

    n0 = A_BLOCKS[0]
    ld_gb = [load(g_hbm, g_ref, 0), load(b_hbm, b_ref, 1)]
    ld_x0 = load(x_hbm.at[pl.ds(0, n0), :], x.at[pl.ds(0, n0), :], 2)
    ld_wqk = load(wqkv_hbm.at[:, pl.ds(0, 2 * C)], wqkv.at[:, pl.ds(0, 2 * C)], 3)
    ld_x1 = load(x_hbm.at[pl.ds(n0, TOK - n0), :], x.at[pl.ds(n0, TOK - n0), :], 4)
    ld_wo = load(wo_hbm, wo, 5)
    ld_wv = load(wqkv_hbm.at[:, pl.ds(2 * C, C)], wqkv.at[:, pl.ds(2 * C, C)], 6)
    ld_dy = load(dy_hbm, dy, 7)
    ld_tau = load(tau_hbm, tau_ref, 8)

    barrier = pltpu.get_barrier_semaphore()
    for peer in (sib, nbr, diag):
        pl.semaphore_signal(barrier, inc=1, device_id={"sp": peer}, device_id_type=MESH)

    busy = {}

    def remote(src, dst, peer, slot, got):
        return pltpu.make_async_remote_copy(
            src_ref=src, dst_ref=dst, send_sem=loc_sem.at[slot], recv_sem=recv_sem.at[got],
            device_id={"sp": peer}, device_id_type=MESH)

    def send(src, dst, peer, slot, got):
        if slot in busy:
            busy[slot].wait_send()
        cp = remote(src, dst, peer, slot, got)
        cp.start()
        busy[slot] = cp
        return cp

    def await_bytes(ref, got):
        remote(ref, ref, sib, 0, got).wait_recv()

    def step_ln(i):
        gamma = g_ref[...].reshape(1, C)
        beta = b_ref[...].reshape(1, C)
        lo, size = a_block(i)
        for j in range(size // SB):
            rows = pl.ds(lo + j * SB, SB)
            xf = x[rows, :].astype(F32)
            cen = xf - jnp.mean(xf, axis=-1, keepdims=True)
            inv = lax.rsqrt(jnp.mean(cen * cen, axis=-1, keepdims=True) + LN_EPS)
            xh = cen * inv
            xhat[rows, :] = xh
            istd[rows, :] = jnp.broadcast_to(inv, (SB, LANES))
            u[rows, :] = (xh * gamma + beta).astype(BF16)

    def step_qk(i):
        lo, size = a_block(i)
        rows = pl.ds(lo, size)
        qk = mm(u[rows, :], wqkv[:, : 2 * C]).astype(BF16)
        q[rows, :] = qk[:, :C]
        k[rows, :] = qk[:, C:]

    def step_gram(i):
        lo, size = a_block(i)
        rows = pl.ds(lo, size)
        p0 = mm(q[rows, :256], k[rows, :256], TN)
        p1 = mm(q[rows, 128:], k[rows, 128:], TN)
        if i == 0:
            g0[...], g1[...] = p0, p1
        else:
            g0[...] += p0
            g1[...] += p1
        for r, c0 in ((q, 0), (k, C)):
            part = jnp.zeros((8, C), F32)
            for j in range(size // SB):
                f = r[pl.ds(lo + j * SB, SB), :].astype(F32)
                part += jnp.sum((f * f).reshape(SB // 8, 8, C), axis=0)
            if i == 0:
                sq[:, pl.ds(c0, C)] = part
            else:
                sq[:, pl.ds(c0, C)] += part

    with jax.named_scope("ln_0"):
        ld_x0.wait()
        for cp in ld_gb:
            cp.wait()
        step_ln(0)
    ld_wqk.wait()
    ld_x1.wait()
    with jax.named_scope("ln_qk"):
        for i in range(1, NA + 2):
            if i < NA:
                step_ln(i)
            if 1 <= i <= NA:
                step_qk(i - 1)
            if i >= 2:
                step_gram(i - 2)
    with jax.named_scope("fold_g"):
        fold_windows((g0, g1), pg)
        sums = jnp.sum(sq[...], axis=0, keepdims=True)
        for m in range(6):
            pg[pl.ds(PK + m, 1), :] = sums[:, LANES * m : LANES * (m + 1)]
        pg[pl.ds(PK + 6, 2), :] = jnp.zeros((2, LANES), F32)
    with jax.named_scope("greet"):
        pl.semaphore_wait(barrier, 3)
    s_g1 = send(pg, rg1, sib, 0, 0)

    def step_b(i):
        rows = pl.ds(i * RV, RV)
        v[rows, :] = mm(u[rows, :], wqkv[:, 2 * C :]).astype(BF16)
        do[rows, :] = mm(dy[rows, :], wot[...]).astype(BF16)

    def step_da(i):
        rows = pl.ds(i * RV, RV)
        p0 = mm(do[rows, :256], v[rows, :256], TN)
        p1 = mm(do[rows, 128:], v[rows, 128:], TN)
        if i == 0:
            g0[...], g1[...] = p0, p1
        else:
            g0[...] += p0
            g1[...] += p1

    with jax.named_scope("v_do_1"):
        ld_wo.wait()
        ld_wv.wait()
        ld_dy.wait()
        ld_tau.wait()
        wot[...] = wo[...].T
        for i in range(CUT):
            step_b(i)
        for i in range(NB):
            ut[:, block(i)] = u[block(i), :].T
    with jax.named_scope("sum_g"):
        s_g1.wait_recv()
        sg[...] = pg[...] + rg1[...]
        s_g2 = [remote(sg, rg2, peer, 1 + j, 1) for j, peer in enumerate((diag, nbr))]

        @pl.when(core == 1)
        def _():
            for cp in s_g2:
                cp.start()
    with jax.named_scope("v_do_2"):
        for i in range(CUT, NV):
            step_b(i)
            for j in range(max(0, i - LAG) if i > CUT else 0, i + 1 - LAG):
                step_da(j)
        for i in range(NV - LAG, NV):
            step_da(i)
    with jax.named_scope("fold_a"):
        fold_windows((g0, g1), pa)
        send(pa.at[1 - core], ra1.at[me], sib, 3, 2)
        send(pa.at[core], ra1.at[me], nbr, 4, 2)
        send(pa.at[1 - core], ra1.at[me], diag, 5, 2)

    with jax.named_scope("wait_g"):
        s_g2[0].wait_recv()
    rels = head_rel()
    row = lax.broadcasted_iota(jnp.int32, (HD, LANES), 0)
    with jax.named_scope("softmax"):
        gfull[...] = sg[...] + rg2[...]
        for ref in (a0, a1, e0, e1):
            ref[...] = jnp.zeros_like(ref)
        for h in range(HEADS):
            rel = rels[h]
            valid = rel < HD
            tau = tau_ref[h]
            s_q = jnp.zeros((HD, LANES), F32)
            s_k = jnp.ones((HD, LANES), F32)
            for m in segs_of(h):
                mask = seg_mask(rel, h, m)
                s_q = jnp.where(mask, gfull[pl.ds(PK + m, 1), :], s_q)
                s_k = jnp.where(mask, gfull[pl.ds(PK + 3 + m, 1), :], s_k)
            q_inv = lax.rsqrt(jnp.sum(jnp.where(rel == row, s_q, 0.0), axis=1, keepdims=True))
            k_inv = lax.rsqrt(s_k)
            by_k = packed_head(gfull, h) * k_inv
            top = jnp.max(jnp.where(valid, by_k, -jnp.inf), axis=1, keepdims=True)
            scale = tau * q_inv
            sc = jnp.where(valid, scale * by_k, 0.0)
            inv = jnp.where(valid, q_inv * k_inv, 0.0)
            ex = jnp.where(valid, jnp.exp(sc - scale * top), 0.0)
            at = ex / jnp.sum(ex, axis=1, keepdims=True)
            hr = pl.ds(HD * h, HD)
            score[hr, :] = sc
            qk_inv[hr, :] = inv
            attn[hr, :] = at
            spread_head(at, rels, h, (a0, a1))

    far = pl.ds(pl.multiple_of(2 * OWN * (1 - chip), 16), 2 * OWN)
    near = pl.ds(pl.multiple_of(2 * OWN * chip, 16), 2 * OWN)
    mine = pl.ds(pl.multiple_of(OWN * core, 8), OWN)

    def part_rows(lhs_t, rows, rhs, part, r1, half, sem, got, count=OWN):
        part[half] = mm(lhs_t[rows, :], rhs)
        theirs = pl.ds(pl.multiple_of(OWN * (1 - core), 8), count)
        return send(part.at[half, theirs, :], r1.at[half, pl.ds(0, count), :], sib, sem, got)

    def cross(cp, part, r1, s, r2, sem, got, count=OWN):
        cp.wait_recv()
        rows = pl.ds(0, count)
        s[rows, :] = part[0, pl.ds(pl.multiple_of(OWN * core, 8), count), :] + r1[0, rows, :]
        send(s.at[rows, :], r2.at[rows, :], nbr, sem, got)

    with jax.named_scope("dv"):
        for i in range(NB):
            rows = block(i)
            dqkv[rows, 2 * C :] = window_mm(do[rows, :], (a0, a1), NN).astype(BF16)
        f_wv = part_rows(ut, far, dqkv[:, 2 * C :], wv_part, wv_r1, 0, 0, 3, OWN - DIRECT)
        @pl.when(core == 1)
        def _():
            for cp in s_g2:
                cp.wait_send()

        for j, (c, peer) in enumerate(((1 - core, diag), (core, nbr))):
            rows = pl.ds(pl.multiple_of(OWN * c + OWN - DIRECT, 8), DIRECT)
            send(wv_part.at[0, rows, :], wv_d.at[j], peer, 1 + j, 9)

    def step_o(i):
        rows = block(i)
        o[rows, :] = window_mm(v[rows, :], (a0, a1), NT).astype(BF16)

    with jax.named_scope("o_1"):
        for i in range(NB // 2):
            step_o(i)
    with jax.named_scope("sum_a"):
        ra1[me] = pa[core]
        await_bytes(ra1.at[pl.ds(0, 3)], 2)
        sa[core] = (ra1[0] + ra1[1]) + (ra1[2] + ra1[3])
        s_a2 = send(sa.at[core], sa.at[core], sib, 3, 5)
    with jax.named_scope("o_2"):
        for i in range(NB // 2, NB):
            step_o(i)
    with jax.named_scope("cross_wv"):
        cross(f_wv, wv_part, wv_r1, wv_s, wv_r2, 6, 9, OWN - DIRECT)
    with jax.named_scope("dwo_far"):
        for i in range(NB):
            ot[:, block(i)] = o[block(i), :].T
        f_wo = part_rows(ot, far, dy[...], wo_part, wo_r1, 0, 0, 6)

    with jax.named_scope("wait_a"):
        s_a2.wait_recv()
    with jax.named_scope("softmax_bwd"):
        dsum = [jnp.zeros((1, LANES), F32) for _ in range(6)]
        lane = lax.broadcasted_iota(jnp.int32, (1, LANES), 1)
        d_tau = jnp.zeros((1, LANES), F32)
        for h in range(HEADS):
            rel = rels[h]
            valid = rel < HD
            hr = pl.ds(HD * h, HD)
            at = attn[hr, :]
            d_at = jnp.where(valid, packed_head(sa, h), 0.0).astype(BF16).astype(F32)
            d_sc = at * (d_at - jnp.sum(d_at * at, axis=1, keepdims=True))
            d_sc_inv = d_sc * qk_inv[hr, :]
            d_tau_h = jnp.sum(d_sc_inv * jnp.where(valid, packed_head(gfull, h), 0.0), axis=0, keepdims=True)
            d_tau = jnp.where(lane == h, jnp.sum(d_tau_h, axis=1, keepdims=True), d_tau)
            spread_head(d_sc_inv * tau_ref[h], rels, h, (e0, e1))
            wt = d_sc * score[hr, :]
            over_q = jnp.sum(jnp.where(rel == row, jnp.sum(wt, axis=1, keepdims=True), 0.0), axis=0, keepdims=True)
            over_k = jnp.sum(wt, axis=0, keepdims=True)
            for m in segs_of(h):
                mask = seg_mask(rel, h, m)[:1]
                dsum[m] = jnp.where(mask, over_q, dsum[m])
                dsum[3 + m] = jnp.where(mask, over_k, dsum[3 + m])
        dt_ref[...] = d_tau[:, :HEADS].reshape(HEADS)
        for m in range(6):
            dsq[:, pl.ds(LANES * m, LANES)] = -dsum[m] / gfull[pl.ds(PK + m, 1), :]
    with jax.named_scope("dqk"):
        for i in range(NB):
            rows = block(i)
            dqkv[rows, :C] = (
                window_mm(k[rows, :], (e0, e1), NT) + q[rows, :].astype(F32) * dsq[:, :C]).astype(BF16)
            dqkv[rows, C : 2 * C] = (
                window_mm(q[rows, :], (e0, e1), NN) + k[rows, :].astype(F32) * dsq[:, C:]).astype(BF16)
    with jax.named_scope("cross_wo"):
        cross(f_wo, wo_part, wo_r1, wo_s, wo_r2, 7, 9)
    with jax.named_scope("dwq_far"):
        f_wq = part_rows(ut, far, dqkv[:, :C], wq_part, wq_r1, 0, 3, 7)
    with jax.named_scope("dwk_far"):
        f_wk = part_rows(ut, far, dqkv[:, C : 2 * C], wk_part, wk_r1, 0, 0, 8)
        last = pl.ds(OWN - MOVE, MOVE)
        hand = remote(wk_part.at[0, last, :], wk_x, sib, 9, 4)

        @pl.when(core == 0)
        def _():
            hand.start()

    with jax.named_scope("near_v"):
        part_rows(ut, near, dqkv[:, 2 * C :], wv_part, wv_r1, 1, 8, 9)
    with jax.named_scope("cross_wq"):
        cross(f_wq, wq_part, wq_r1, wq_s, wq_r2, 4, 9)
    with jax.named_scope("near_o"):
        part_rows(ot, near, dy[...], wo_part, wo_r1, 1, 3, 9)
    with jax.named_scope("cross_wk"):
        cross(f_wk, wk_part, wk_r1, wk_s, wk_r2, 5, 11, OWN - LATE)
    with jax.named_scope("near_qk"):
        part_rows(ut, near, dqkv[:, :C], wq_part, wq_r1, 1, 0, 9)
        part_rows(ut, near, dqkv[:, C : 2 * C], wk_part, wk_r1, 1, 8, 9)

    gamma = g_ref[...].reshape(1, C)
    dgam = jnp.zeros((8, C), F32)
    dbet = jnp.zeros((8, C), F32)
    with jax.named_scope("ln_bwd"):
        for i in range(NB):
            rows = block(i)
            du[rows, :] = mm(dqkv[rows, :], wqkv[...], NT).astype(BF16)
            for j in range(RB // SB):
                sub = pl.ds(i * RB + j * SB, SB)
                d = du[sub, :].astype(F32)
                xh = xhat[sub, :]
                dxh = d * xh
                dgam += jnp.sum(dxh.reshape(SB // 8, 8, C), axis=0)
                dbet += jnp.sum(d.reshape(SB // 8, 8, C), axis=0)
                dh = d * gamma
                m1 = jnp.mean(dh, axis=-1, keepdims=True)
                m2 = jnp.mean(dxh * gamma, axis=-1, keepdims=True)
                inv = istd[sub, :]
                term = dh - m1 - xh * m2
                dln = term * jnp.concatenate([inv, inv, inv], axis=1)
                dx[sub, :] = (dy[sub, :].astype(F32) + dln).astype(BF16)
        dgb_all[me] = jnp.concatenate(
            [jnp.sum(dgam, axis=0, keepdims=True), jnp.sum(dbet, axis=0, keepdims=True)], axis=1)
    for j, peer in enumerate((nbr, diag, sib)):
        send(dgb_all.at[me], dgb_all.at[me], peer, 1 + j, 10)
    late = pl.ds(OWN - LATE, LATE)
    wk_s[late, :] = wk_part[0, pl.ds(pl.multiple_of(OWN * core + OWN - LATE, 8), LATE), :] + wk_r1[0, late, :]
    busy.pop(6).wait_send()

    def late_copy(count):
        rows = pl.ds(OWN - LATE, count)
        return remote(wk_s.at[rows, :], wk_r2.at[rows, :], nbr, 6, 11)

    moved = remote(wk_m, wk_r2.at[last, :], diag, 9, 11)

    @pl.when(core == 0)
    def _():
        late_copy(LATE - MOVE).start()

    @pl.when(core == 1)
    def _():
        hand.wait_recv()
        wk_m[...] = wk_part[0, last, :] + wk_x[...]
        moved.start()
        late_copy(LATE).start()

    with jax.named_scope("y"):
        for i in range(NB):
            rows = block(i)
            y[rows, :] = (x[rows, :].astype(F32) + mm(o[rows, :], wo[...])).astype(BF16)

    def rows_of(n):
        return xhat.at[pl.ds(0, n), :]

    with jax.named_scope("wait_wq"):
        await_bytes(rows_of(7 * OWN + DIRECT), 9)
        dwo_ref[...] = (wo_part[1, mine, :] + wo_r1[1] + wo_r2[...]).astype(BF16)
        dwqkv_ref[:, :C] = (wq_part[1, mine, :] + wq_r1[1] + wq_r2[...]).astype(BF16)
        cut = OWN - DIRECT
        near_sum = wv_part[1, mine, :] + wv_r1[1]
        far_sum = jnp.concatenate([wv_r2[pl.ds(0, cut), :], wv_d[0] + wv_d[1]], axis=0)
        dwqkv_ref[:, 2 * C :] = (near_sum + far_sum).astype(BF16)
    with jax.named_scope("wait_dgb"):
        await_bytes(dgb_all.at[pl.ds(0, 3)], 10)
        total = dgb_all[0] + dgb_all[1] + dgb_all[2] + dgb_all[3]
        dg_ref[...] = total[:, :C].reshape(C)
        db_ref[...] = total[:, C:].reshape(C)
    with jax.named_scope("wait_wqk"):
        await_bytes(rows_of(OWN), 11)
        dwqkv_ref[:, C : 2 * C] = (wk_part[1, mine, :] + wk_r1[1] + wk_r2[...]).astype(BF16)
    with jax.named_scope("sends"):
        for cp in busy.values():
            cp.wait_send()

        @pl.when(core == 0)
        def _():
            hand.wait_send()
            late_copy(LATE - MOVE).wait_send()

        @pl.when(core == 1)
        def _():
            moved.wait_send()
            late_copy(LATE).wait_send()


def write_out(*refs):
    ins, outs, sem = refs[:7], refs[7:14], refs[14]
    pairs = []
    for i in range(2):
        for j in range(PIECES):
            rows = pl.ds(j * (TOK // PIECES), TOK // PIECES)
            pairs.append((ins[i].at[rows, :], outs[i].at[rows, :]))
    pairs += [(ins[i], outs[i]) for i in range(2, 7)]
    copies = [pltpu.make_async_copy(src, dst, sem.at[i]) for i, (src, dst) in enumerate(pairs)]
    for cp in copies:
        cp.start()
    for cp in copies:
        cp.wait()


def xca_local(x_rows, dy_rows, ln_gamma, ln_beta, w_qkv, w_out, temperature):
    vm = pltpu.VMEM
    hbm_spec = pl.BlockSpec(memory_space=pltpu.HBM)
    vmem_spec = pl.BlockSpec(memory_space=pltpu.VMEM)
    results = (
        ((TOK, C), BF16), ((TOK, C), BF16), ((OWN, 3 * C), BF16), ((OWN, C), BF16),
        ((C,), F32), ((C,), F32), ((HEADS,), F32),
    )
    rows_bf = vm((TOK, C), BF16)
    cols_bf = vm((C, TOK), BF16)
    win_f = vm((256, 256), F32)
    win_b = vm((256, 256), BF16)
    pk_g = vm((PK + 8, LANES), F32)
    pk_a = vm((2, HALF, LANES), F32)
    fold = vm((C, LANES), F32)
    scratch = [
        rows_bf, rows_bf, vm((C,), F32), vm((C,), F32), vm((C, 3 * C), BF16), vm((C, C), BF16), vm((C, C), BF16),
        pltpu.SMEM((HEADS,), F32), rows_bf, cols_bf, vm((TOK, C), F32), vm((TOK, LANES), F32),
        rows_bf, rows_bf, rows_bf, rows_bf, rows_bf, cols_bf, vm((TOK, 3 * C), BF16), rows_bf,
        win_f, win_f, vm((8, 2 * C), F32), pk_g, pk_g, pk_g, pk_g, pk_a, vm((4, HALF, LANES), F32), pk_a,
        win_b, win_b, win_b, win_b, fold, fold, fold, pk_g, vm((1, 2 * C), F32),
        *[vm((2, 2 * OWN, C), F32)] * 4, *[vm((2, OWN, C), F32)] * 4, *[vm((OWN, C), F32)] * 8, vm((2, DIRECT, C), F32), vm((MOVE, C), F32), vm((MOVE, C), F32),
        vm((4, 1, 2 * C), F32),
        pltpu.SemaphoreType.DMA((10,)), pltpu.SemaphoreType.DMA((12,)),
    ]
    parts = pl.pallas_call(
        kernel,
        name="xca",
        out_shape=tuple(pltpu.VMEM(shape, dtype) for shape, dtype in results),
        in_specs=[hbm_spec] * 7,
        out_specs=[vmem_spec] * 7,
        scratch_shapes=scratch,
        compiler_params=pltpu.CompilerParams(
            collective_id=0, has_side_effects=True, vmem_limit_bytes=60 * 1024 * 1024),
    )(x_rows, dy_rows, ln_gamma, ln_beta, w_qkv, w_out, temperature)
    return pl.pallas_call(
        write_out,
        name="xca_out",
        out_shape=tuple(jax.ShapeDtypeStruct(shape, dtype) for shape, dtype in results),
        in_specs=[vmem_spec] * 7,
        out_specs=[hbm_spec] * 7,
        scratch_shapes=[pltpu.SemaphoreType.DMA((2 * PIECES + 5,))],
        compiler_params=pltpu.CompilerParams(vmem_limit_bytes=1024 * 1024),
    )(*parts)


def solution(mesh):
    row_spec = P(('dp', 'sp'), None)
    full_mat = P(None, None)
    full_vec = P(None)
    part_vec = P('dp')
    return jax.shard_map(
        xca_local, mesh=mesh,
        in_specs=(row_spec, row_spec, full_vec, full_vec, full_mat, full_mat, full_vec),
        out_specs=(row_spec, row_spec, row_spec, row_spec, part_vec, part_vec, part_vec),
        check_vma=False)
```
